32 devices in a mesh: dp: 1 (over z), tp: 4 (over y), sq: 8 (over x, core).
Axes of the slice: x: 4, y: 4, z: 1, core: 2. Of those that a mesh axis runs over, the one named last changes fastest.
The devices are a block of a 4x4x8 slice.
Arguments:
- hidden: bfloat16 [256, 6144], P('dp')
- cache_lens: int32 [256], P('dp')
- k_cache: bfloat16 [256, 2048, 128], P('dp', 'sq')
- v_cache: bfloat16 [256, 2048, 128], P('dp', 'sq')
- ln_gain: float32 [6144], replicated
- ln_bias: float32 [6144], replicated
- w_query: bfloat16 [6144, 6144], P(None, 'tp')
- b_query: float32 [6144], P('tp')
- w_kv: bfloat16 [6144, 256], replicated
- b_kv: float32 [256], replicated
- w_out: bfloat16 [6144, 6144], P('tp')
- b_out: float32 [6144], replicated
Outputs:
- output 1: bfloat16 [256, 6144], P('dp')
- output 2: bfloat16 [256, 2048, 128], P('dp', 'sq')
- output 3: bfloat16 [256, 2048, 128], P('dp', 'sq')
All inputs are finite; a program needn't handle non-finite values.
Results may differ from the reference program's by a relative error of at most 0.00348177.
Values sent between devices are 32-bit elements.
A program may use at most 768 MiB of HBM per device.

```python
import math
import jax
import jax.numpy as jnp
from jax import lax

BATCH = 256
CACHE_LEN = 2048
D_MODEL = 6144
HEADS = 48
HEAD_DIM = 128


def layer_norm(x_rows, ln_gain, ln_bias):
    x_wide = x_rows.astype(jnp.float32)
    mean_val = jnp.mean(x_wide, axis=-1, keepdims=True)
    centered = x_wide - mean_val
    variance = jnp.mean(centered * centered, axis=-1, keepdims=True)
    normed = centered * lax.rsqrt(variance + 1e-5)
    return (normed * ln_gain + ln_bias).astype(jnp.bfloat16)


def setup_inputs(seed: int = 0, part: int = 0) -> dict:
    own_keys = jax.random.split(jax.random.fold_in(jax.random.key(seed), part), 5)
    shared_keys = jax.random.split(jax.random.key(seed + 1), 10)
    q_width = HEADS * HEAD_DIM
    score_var = max(1.0, math.log(CACHE_LEN / 32.0))
    key_scale = math.sqrt(score_var / 2.0)
    self_bias = (math.log(0.6 * CACHE_LEN) + 0.5 * score_var) / math.sqrt(HEAD_DIM)
    hidden = jax.random.normal(own_keys[0], (BATCH, D_MODEL), jnp.float32).astype(jnp.bfloat16)
    drawn = CACHE_LEN - 1 - jax.random.randint(own_keys[1], (BATCH,), 0, CACHE_LEN // 2)
    order = jax.random.permutation(own_keys[2], BATCH)
    seq_ids = jnp.arange(BATCH)
    cache_lens = jnp.where(seq_ids == order[0], CACHE_LEN - 1, jnp.where(seq_ids == order[1], 1, drawn)).astype(jnp.int32)
    k_cache = (key_scale * jax.random.normal(own_keys[3], (BATCH, CACHE_LEN, HEAD_DIM), jnp.float32)).astype(jnp.bfloat16)
    v_cache = jax.random.normal(own_keys[4], (BATCH, CACHE_LEN, HEAD_DIM), jnp.float32).astype(jnp.bfloat16)
    ln_gain = 1.0 + 0.3 * jax.random.normal(shared_keys[0], (D_MODEL,), jnp.float32)
    ln_bias = 0.3 * jax.random.normal(shared_keys[1], (D_MODEL,), jnp.float32)
    w_query = (jax.random.normal(shared_keys[2], (D_MODEL, q_width), jnp.float32) * D_MODEL ** -0.5).astype(jnp.bfloat16)
    shared_dir = jax.random.normal(shared_keys[3], (HEAD_DIM,), jnp.float32)
    b_query = jnp.tile(shared_dir, HEADS) + 0.2 * jax.random.normal(shared_keys[4], (q_width,), jnp.float32)
    w_kv = (jax.random.normal(shared_keys[5], (D_MODEL, 2 * HEAD_DIM), jnp.float32) * D_MODEL ** -0.5).astype(jnp.bfloat16)
    key_bias = self_bias * shared_dir + 0.2 * jax.random.normal(shared_keys[6], (HEAD_DIM,), jnp.float32)
    val_bias = 0.5 * jax.random.normal(shared_keys[7], (HEAD_DIM,), jnp.float32)
    b_kv = jnp.concatenate([key_bias, val_bias])
    w_out = (jax.random.normal(shared_keys[8], (q_width, D_MODEL), jnp.float32) * q_width ** -0.5).astype(jnp.bfloat16)
    b_out = 0.3 * jax.random.normal(shared_keys[9], (D_MODEL,), jnp.float32)
    return {"hidden": hidden, "cache_lens": cache_lens, "k_cache": k_cache, "v_cache": v_cache, "ln_gain": ln_gain, "ln_bias": ln_bias, "w_query": w_query, "b_query": b_query, "w_kv": w_kv, "b_kv": b_kv, "w_out": w_out, "b_out": b_out}


def reference(hidden, cache_lens, k_cache, v_cache, ln_gain, ln_bias, w_query, b_query, w_kv, b_kv, w_out, b_out):
    normed = layer_norm(hidden, ln_gain, ln_bias)
    query = (jnp.dot(normed, w_query, preferred_element_type=jnp.float32) + b_query).astype(jnp.bfloat16)
    query = query.reshape(BATCH, HEADS, HEAD_DIM)
    key_val = (jnp.dot(normed, w_kv, preferred_element_type=jnp.float32) + b_kv).astype(jnp.bfloat16)
    positions = jnp.arange(CACHE_LEN, dtype=jnp.int32)
    at_slot = (positions[None, :] == cache_lens[:, None])[:, :, None]
    key_new = jnp.where(at_slot, key_val[:, None, :HEAD_DIM], k_cache)
    val_new = jnp.where(at_slot, key_val[:, None, HEAD_DIM:], v_cache)

    def one_sequence(packed):
        query_row, key_rows, val_rows, length = packed
        scores = jnp.einsum("nd,td->nt", query_row.astype(jnp.float32), key_rows.astype(jnp.float32)) * (HEAD_DIM ** -0.5)
        valid = positions <= length
        scores = jnp.where(valid[None, :], scores, -jnp.inf)
        weights = jax.nn.softmax(scores, axis=-1)
        return jnp.einsum("nt,td->nd", weights, val_rows.astype(jnp.float32)).astype(jnp.bfloat16)

    attended = lax.map(one_sequence, (query, key_new, val_new, cache_lens))
    projected = jnp.dot(attended.reshape(BATCH, HEADS * HEAD_DIM), w_out, preferred_element_type=jnp.float32)
    out_hidden = (hidden.astype(jnp.float32) + projected + b_out).astype(jnp.bfloat16)
    return (out_hidden, key_new, val_new)
```

```python
import functools

import jax
import jax.numpy as jnp
from jax import lax
from jax.experimental import pallas as pl
from jax.experimental.pallas import tpu as pltpu
from jax.sharding import PartitionSpec as P

MESH = pl.DeviceIdType.MESH
LANES = 128
NEG = -1e30


def layer_norm(x_rows, ln_gain, ln_bias):
    x_wide = x_rows.astype(jnp.float32)
    mean_val = jnp.mean(x_wide, axis=-1, keepdims=True)
    centered = x_wide - mean_val
    variance = jnp.mean(centered * centered, axis=-1, keepdims=True)
    normed = centered * lax.rsqrt(variance + 1e-5)
    return (normed * ln_gain + ln_bias).astype(jnp.bfloat16)


def merge_into(dst, part_a, part_b, heads):
    width = heads * LANES
    stat_a, stat_b = part_a[:, width:], part_b[:, width:]
    top = jnp.maximum(stat_a, stat_b)
    exp_a, exp_b = jnp.exp(stat_a - top), jnp.exp(stat_b - top)
    sums = stat_a * pltpu.roll(exp_a, 64, 1) + stat_b * pltpu.roll(exp_b, 64, 1)
    lane = lax.broadcasted_iota(jnp.int32, top.shape, 1)
    dst[:, width:] = jnp.where(lane < 64, top, sums)
    for n in range(heads):
        cols = slice(n * LANES, (n + 1) * LANES)
        dst[:, cols] = part_a[:, cols] * exp_a[:, n : n + 1] + part_b[:, cols] * exp_b[:, n : n + 1]


def finish_kernel(
    dims,
    part_ref,
    b_out_ref,
    hidden_ref,
    w_out_ref,
    out_ref,
    w_buf,
    pair_buf,
    merge_buf,
    x_buf,
    att_buf,
    proj_buf,
    y_buf,
    hid_buf,
    gather_buf,
    w_sem,
    hid_sem,
    pair_send,
    pair_recv,
    x_send,
    x_recv,
    y_send,
    y_recv,
    g_send,
    g_recv,
    d_send,
    d_recv,
):
    nx, ny, heads, rows, cols = dims
    half = cols // 2
    width = heads * LANES
    sq = lax.axis_index("sq")
    y = lax.axis_index("tp")
    x = sq // 2
    core = sq % 2
    step = 1 - 2 * core

    def wrap(value, size):
        return lax.rem(value + 2 * size, size)

    x_fwd, x_bwd, x_opp = wrap(x + step, nx), wrap(x - step, nx), wrap(x + 2, nx)
    y_fwd, y_bwd, y_opp = wrap(y + step, ny), wrap(y - step, ny), wrap(y + 2, ny)
    to_pair = {"sq": x * 2 + 1 - core}
    to_x_fwd, to_x_bwd = {"sq": x_fwd * 2 + core}, {"sq": x_bwd * 2 + core}
    to_y_fwd, to_y_bwd = {"tp": y_fwd}, {"tp": y_bwd}

    barrier = pltpu.get_barrier_semaphore()
    for peer in (to_pair, to_x_fwd, to_x_bwd, to_y_fwd, to_y_bwd):
        pl.semaphore_signal(barrier, inc=1, device_id=peer, device_id_type=MESH)

    y_order = (y_opp, y_bwd, y_fwd, y)
    w_copies = []
    for k, target in enumerate(y_order):
        src = w_out_ref.at[:, pl.ds(pl.multiple_of(target * cols, cols), cols)]
        w_copies.append(pltpu.make_async_copy(src, w_buf.at[k], w_sem.at[k]))
    my_row = pl.multiple_of(sq * rows, rows)
    my_col = pl.multiple_of(y * cols, cols)
    hid_copy = pltpu.make_async_copy(hidden_ref.at[pl.ds(my_row, rows), pl.ds(my_col, cols)], hid_buf, hid_sem)
    pl.semaphore_wait(barrier, 5)

    sends = []

    def send(src, dst, ssem, rsem, peer):
        copy = pltpu.make_async_remote_copy(
            src_ref=src, dst_ref=dst, send_sem=ssem, recv_sem=rsem, device_id=peer, device_id_type=MESH
        )
        copy.start()
        sends.append(copy)
        return copy

    def part_rows(xt, ct):
        return pl.ds(pl.multiple_of((xt * 2 + ct) * rows, rows), rows)

    pair = []
    for k, xt in enumerate((x_opp, x_fwd, x_bwd, x)):
        pair.append(send(part_ref.at[part_rows(xt, 1 - core), :], pair_buf.at[k], pair_send.at[k], pair_recv.at[k], to_pair))
    for copy in w_copies:
        copy.start()
    hid_copy.start()

    pair[0].wait_recv()
    merge_into(merge_buf.at[0], part_ref[part_rows(x_opp, core), :], pair_buf[0], heads)
    x_o = send(merge_buf.at[0], x_buf.at[0], x_send.at[0], x_recv.at[0], to_x_fwd)
    pair[1].wait_recv()
    merge_into(merge_buf.at[1], part_ref[part_rows(x_bwd, core), :], pair_buf[1], heads)
    x_b = send(merge_buf.at[1], x_buf.at[1], x_send.at[1], x_recv.at[1], to_x_bwd)
    pair[2].wait_recv()
    merge_into(merge_buf.at[2], part_ref[part_rows(x_fwd, core), :], pair_buf[2], heads)
    x_o.wait_recv()
    merge_into(merge_buf.at[3], merge_buf[2], x_buf[0], heads)
    x_a = send(merge_buf.at[3], x_buf.at[2], x_send.at[2], x_recv.at[2], to_x_fwd)
    pair[3].wait_recv()
    merge_into(merge_buf.at[4], part_ref[part_rows(x, core), :], pair_buf[3], heads)
    x_b.wait_recv()
    merge_into(merge_buf.at[5], merge_buf[4], x_buf[1], heads)
    x_a.wait_recv()
    merge_into(merge_buf.at[6], merge_buf[5], x_buf[2], heads)
    stat = merge_buf[6, :, width:]
    for n in range(heads):
        block = slice(n * LANES, (n + 1) * LANES)
        att_buf[:, block] = (merge_buf[6, :, block] / stat[:, 64 + n : 65 + n]).astype(jnp.bfloat16)

    for copy in w_copies:
        copy.wait()
    hid_copy.wait()

    def project(k, h):
        return jnp.dot(att_buf[...], w_buf[k, :, h * half : (h + 1) * half], preferred_element_type=jnp.float32)

    y_o, y_b, y_a = [None, None], [None, None], [None, None]
    for h in range(2):
        proj_buf[0, h] = project(0, h)
        y_o[h] = send(proj_buf.at[0, h], y_buf.at[0, h], y_send.at[0, h], y_recv.at[0, h], to_y_fwd)
    for h in range(2):
        proj_buf[1, h] = project(1, h)
        y_b[h] = send(proj_buf.at[1, h], y_buf.at[1, h], y_send.at[1, h], y_recv.at[1, h], to_y_bwd)
        fwd_part = project(2, h)
        y_o[h].wait_recv()
        proj_buf[2, h] = fwd_part + y_buf[0, h]
        y_a[h] = send(proj_buf.at[2, h], y_buf.at[2, h], y_send.at[2, h], y_recv.at[2, h], to_y_fwd)
        own_cols = pl.ds(pl.multiple_of(y * cols + h * half, half), half)
        own = project(3, h) + hid_buf[:, h * half : (h + 1) * half].astype(jnp.float32) + b_out_ref[:, own_cols]
        proj_buf[3, h] = own

    def place(xt, yt, ct, h):
        row = pl.multiple_of((xt * 2 + ct) * rows, rows)
        col = pl.multiple_of(yt * cols + h * half, half)
        return pl.ds(row, rows), pl.ds(col, half)

    xs = (x, x_bwd, x_fwd, x_opp)
    ys = (y, y_bwd, y_fwd, y_opp)
    x_peers, y_peers = (to_x_fwd, to_x_bwd), (to_y_fwd, to_y_bwd)
    gathers = {}
    pairs = {}

    def spot(h, first, second, ct=None):
        ct = core if ct is None else ct
        if h == 0:
            return place(xs[first], ys[second], ct, h)
        return place(xs[second], ys[first], ct, h)

    def piece(h, first, second):
        return gather_buf.at[spot(h, first, second)]

    def ring_send(h, first, second, slot, phase):
        peers = (x_peers, y_peers) if h == 0 else (y_peers, x_peers)
        peer = peers[phase][1 if slot == 2 else 0]
        index = slot - 1 if phase == 0 else 3 + first * 3 + slot - 1
        key = (h, phase, first if phase else 0, slot)
        ref = piece(h, first, second)
        gathers[key] = send(ref, ref, g_send.at[h, index], g_recv.at[h, index], peer)

    def pair_forward(h, first, second):
        ref = piece(h, first, second)
        index = first * 4 + second
        pairs[(h, first, second)] = send(ref, ref, d_send.at[h, index], d_recv.at[h, index], to_pair)

    def convert(where):
        out_ref[where] = gather_buf[where].astype(jnp.bfloat16)

    def mirrored(slot):
        return (0, 2, 1, 3)[slot]

    todo = []

    def drain(limit):
        while len(todo) > limit:
            h, first, second = todo.pop(0)
            pairs[(h, first, second)].wait_recv()
            convert(spot(h, mirrored(first), mirrored(second), 1 - core))

    def have(h, first, second):
        pair_forward(h, first, second)
        convert(spot(h, first, second))
        todo.append((h, first, second))
        drain(2)

    for h in range(2):
        y_b[h].wait_recv()
        part = proj_buf[3, h] + y_buf[1, h]
        y_a[h].wait_recv()
        gather_buf[spot(h, 0, 0)] = part + y_buf[2, h]
        ring_send(h, 0, 0, 1, 0)
        ring_send(h, 0, 0, 2, 0)
        pair_forward(h, 0, 0)
    for h in range(2):
        ring_send(h, 0, 0, 1, 1)
        ring_send(h, 0, 0, 2, 1)
        convert(spot(h, 0, 0))
        todo.append((h, 0, 0))

    def arrived(h, first, second):
        if second == 0:
            gathers[(h, 0, 0, first)].wait_recv()
            if first == 1:
                ring_send(h, 1, 0, 3, 0)
            ring_send(h, first, 0, 1, 1)
            ring_send(h, first, 0, 2, 1)
        else:
            gathers[(h, 1, first, second)].wait_recv()
            if second == 1:
                ring_send(h, first, 1, 3, 1)
        have(h, first, second)

    order = [(1, 0), (2, 0), (0, 1), (0, 2), (3, 0), (1, 1), (0, 3), (2, 1), (1, 2), (1, 3), (2, 2), (3, 1), (2, 3), (3, 2), (3, 3)]
    for first, second in order:
        for h in range(2):
            arrived(h, first, second)
    drain(0)
    for copy in sends:
        copy.wait_send()


def finish(parts, hidden, w_out, b_out, nx, ny):
    batch, width = parts.shape
    heads = width // LANES - 1
    depth, d_model = w_out.shape
    rows, cols = batch // (2 * nx), d_model // ny
    half = cols // 2
    f32, dma = jnp.float32, pltpu.SemaphoreType.DMA
    return pl.pallas_call(
        functools.partial(finish_kernel, (nx, ny, heads, rows, cols)),
        out_shape=jax.ShapeDtypeStruct((batch, d_model), jnp.bfloat16),
        in_specs=[
            pl.BlockSpec(memory_space=pltpu.VMEM),
            pl.BlockSpec(memory_space=pltpu.VMEM),
            pl.BlockSpec(memory_space=pl.ANY),
            pl.BlockSpec(memory_space=pl.ANY),
        ],
        out_specs=pl.BlockSpec(memory_space=pltpu.VMEM),
        scratch_shapes=[
            pltpu.VMEM((4, depth, cols), jnp.bfloat16),
            pltpu.VMEM((4, rows, width), f32),
            pltpu.VMEM((7, rows, width), f32),
            pltpu.VMEM((3, rows, width), f32),
            pltpu.VMEM((rows, heads * LANES), jnp.bfloat16),
            pltpu.VMEM((4, 2, rows, half), f32),
            pltpu.VMEM((3, 2, rows, half), f32),
            pltpu.VMEM((rows, cols), jnp.bfloat16),
            pltpu.VMEM((batch, d_model), f32),
            dma((4,)),
            dma,
            dma((4,)),
            dma((4,)),
            dma((3,)),
            dma((3,)),
            dma((3, 2)),
            dma((3, 2)),
            dma((2, 15)),
            dma((2, 15)),
            dma((2, 16)),
            dma((2, 16)),
        ],
        compiler_params=pltpu.CompilerParams(collective_id=0, has_side_effects=True, vmem_limit_bytes=48 * 1024 * 1024),
        name="finish",
    )(parts, b_out.reshape(1, d_model), hidden, w_out)


def solution(mesh):
    nx, ny = mesh.shape["sq"] // 2, mesh.shape["tp"]

    def local_step(hidden, cache_lens, k_cache, v_cache, ln_gain, ln_bias, w_query, b_query, w_kv, b_kv, w_out, b_out):
        batch, pos_local, head_dim = k_cache.shape
        heads_local = w_query.shape[1] // head_dim
        normed = layer_norm(hidden, ln_gain, ln_bias)
        query = (jnp.dot(normed, w_query, preferred_element_type=jnp.float32) + b_query).astype(jnp.bfloat16)
        query = query.reshape(batch, heads_local, head_dim)
        key_val = (jnp.dot(normed, w_kv, preferred_element_type=jnp.float32) + b_kv).astype(jnp.bfloat16)
        first_pos = lax.axis_index("sq") * pos_local
        positions = first_pos + lax.broadcasted_iota(jnp.int32, (1, pos_local), 1)
        at_slot = (positions == cache_lens[:, None])[:, :, None]
        key_new = jnp.where(at_slot, key_val[:, None, :head_dim], k_cache)
        val_new = jnp.where(at_slot, key_val[:, None, head_dim:], v_cache)
        scores = jnp.einsum("bnd,btd->bnt", query, key_new, preferred_element_type=jnp.float32) * (head_dim ** -0.5)
        valid = (positions <= cache_lens[:, None])[:, None, :]
        scores = jnp.where(valid, scores, NEG)
        local_max = jnp.max(scores, axis=-1, keepdims=True)
        weights = jnp.where(valid, jnp.exp(scores - local_max), 0.0)
        local_sum = jnp.sum(weights, axis=-1)
        numerator = jnp.einsum("bnt,btd->bnd", weights.astype(jnp.bfloat16), val_new, preferred_element_type=jnp.float32)
        pad = ((0, 0), (0, 64 - heads_local))
        parts = jnp.concatenate(
            [numerator.reshape(batch, heads_local * head_dim), jnp.pad(local_max[..., 0], pad), jnp.pad(local_sum, pad)], axis=1
        )
        out_hidden = finish(parts, hidden, w_out, b_out, nx, ny)
        return out_hidden, key_new, val_new

    cache_spec = P("dp", "sq", None)
    row_spec = P("dp", None)
    in_specs = (row_spec, P("dp"), cache_spec, cache_spec, P(None), P(None), P(None, "tp"), P("tp"), P(None, None), P(None), P("tp", None), P(None))
    out_specs = (row_spec, cache_spec, cache_spec)
    return jax.shard_map(local_step, mesh=mesh, in_specs=in_specs, out_specs=out_specs, check_vma=False)
```

```python
import functools

import jax
import jax.numpy as jnp
from jax import lax
from jax.experimental import pallas as pl
from jax.experimental.pallas import tpu as pltpu
from jax.sharding import PartitionSpec as P

MESH = pl.DeviceIdType.MESH
LANES = 128


def merge_into(dst, part_a, part_b, heads):
    width = heads * LANES
    stat_a, stat_b = part_a[:, width:], part_b[:, width:]
    top = jnp.maximum(stat_a, stat_b)
    exp_a, exp_b = jnp.exp(stat_a - top), jnp.exp(stat_b - top)
    sums = stat_a * pltpu.roll(exp_a, 64, 1) + stat_b * pltpu.roll(exp_b, 64, 1)
    lane = lax.broadcasted_iota(jnp.int32, top.shape, 1)
    dst[:, width:] = jnp.where(lane < 64, top, sums)
    for n in range(heads):
        cols = slice(n * LANES, (n + 1) * LANES)
        dst[:, cols] = part_a[:, cols] * exp_a[:, n : n + 1] + part_b[:, cols] * exp_b[:, n : n + 1]


def finish_kernel(
    dims,
    part_ref,
    b_out_ref,
    hidden_ref,
    w_out_ref,
    out_ref,
    w_buf,
    pair_buf,
    merge_buf,
    x_buf,
    att_buf,
    proj_buf,
    y_buf,
    hid_buf,
    gather_buf,
    w_sem,
    hid_sem,
    pair_send,
    pair_recv,
    x_send,
    x_recv,
    y_send,
    y_recv,
    g_send,
    g_recv,
    d_send,
    d_recv,
):
    nx, ny, heads, rows, cols = dims
    half = cols // 2
    width = heads * LANES
    sq = lax.axis_index("sq")
    y = lax.axis_index("tp")
    x = sq // 2
    core = sq % 2
    step = 1 - 2 * core

    def wrap(value, size):
        return lax.rem(value + 2 * size, size)

    x_fwd, x_bwd, x_opp = wrap(x + step, nx), wrap(x - step, nx), wrap(x + 2, nx)
    y_fwd, y_bwd, y_opp = wrap(y + step, ny), wrap(y - step, ny), wrap(y + 2, ny)
    to_pair = {"sq": x * 2 + 1 - core}
    to_x_fwd, to_x_bwd = {"sq": x_fwd * 2 + core}, {"sq": x_bwd * 2 + core}
    to_y_fwd, to_y_bwd = {"tp": y_fwd}, {"tp": y_bwd}

    barrier = pltpu.get_barrier_semaphore()
    for peer in (to_pair, to_x_fwd, to_x_bwd, to_y_fwd, to_y_bwd):
        pl.semaphore_signal(barrier, inc=1, device_id=peer, device_id_type=MESH)

    y_order = (y_opp, y_bwd, y_fwd, y)
    w_copies = []
    for k, target in enumerate(y_order):
        src = w_out_ref.at[:, pl.ds(pl.multiple_of(target * cols, cols), cols)]
        w_copies.append(pltpu.make_async_copy(src, w_buf.at[k], w_sem.at[k]))
    my_row = pl.multiple_of(sq * rows, rows)
    my_col = pl.multiple_of(y * cols, cols)
    hid_copy = pltpu.make_async_copy(hidden_ref.at[pl.ds(my_row, rows), pl.ds(my_col, cols)], hid_buf, hid_sem)
    pl.semaphore_wait(barrier, 5)

    sends = []

    def send(src, dst, ssem, rsem, peer):
        copy = pltpu.make_async_remote_copy(
            src_ref=src, dst_ref=dst, send_sem=ssem, recv_sem=rsem, device_id=peer, device_id_type=MESH
        )
        copy.start()
        sends.append(copy)
        return copy

    def part_rows(xt, ct):
        return pl.ds(pl.multiple_of((xt * 2 + ct) * rows, rows), rows)

    pair = []
    for k, xt in enumerate((x_opp, x_fwd, x_bwd, x)):
        pair.append(send(part_ref.at[part_rows(xt, 1 - core), :], pair_buf.at[k], pair_send.at[k], pair_recv.at[k], to_pair))
    for copy in w_copies:
        copy.start()
    hid_copy.start()

    pair[0].wait_recv()
    merge_into(merge_buf.at[0], part_ref[part_rows(x_opp, core), :], pair_buf[0], heads)
    x_o = send(merge_buf.at[0], x_buf.at[0], x_send.at[0], x_recv.at[0], to_x_fwd)
    pair[1].wait_recv()
    merge_into(merge_buf.at[1], part_ref[part_rows(x_bwd, core), :], pair_buf[1], heads)
    x_b = send(merge_buf.at[1], x_buf.at[1], x_send.at[1], x_recv.at[1], to_x_bwd)
    pair[2].wait_recv()
    merge_into(merge_buf.at[2], part_ref[part_rows(x_fwd, core), :], pair_buf[2], heads)
    x_o.wait_recv()
    merge_into(merge_buf.at[3], merge_buf[2], x_buf[0], heads)
    x_a = send(merge_buf.at[3], x_buf.at[2], x_send.at[2], x_recv.at[2], to_x_fwd)
    pair[3].wait_recv()
    merge_into(merge_buf.at[4], part_ref[part_rows(x, core), :], pair_buf[3], heads)
    x_b.wait_recv()
    merge_into(merge_buf.at[5], merge_buf[4], x_buf[1], heads)
    x_a.wait_recv()
    merge_into(merge_buf.at[6], merge_buf[5], x_buf[2], heads)
    stat = merge_buf[6, :, width:]
    for n in range(heads):
        block = slice(n * LANES, (n + 1) * LANES)
        att_buf[:, block] = (merge_buf[6, :, block] / stat[:, 64 + n : 65 + n]).astype(jnp.bfloat16)

    for copy in w_copies:
        copy.wait()
    hid_copy.wait()

    def project(k, h):
        return jnp.dot(att_buf[...], w_buf[k, :, h * half : (h + 1) * half], preferred_element_type=jnp.float32)

    y_o, y_b, y_a = [None, None], [None, None], [None, None]
    for h in range(2):
        proj_buf[0, h] = project(0, h)
        y_o[h] = send(proj_buf.at[0, h], y_buf.at[0, h], y_send.at[0, h], y_recv.at[0, h], to_y_fwd)
    for h in range(2):
        proj_buf[1, h] = project(1, h)
        y_b[h] = send(proj_buf.at[1, h], y_buf.at[1, h], y_send.at[1, h], y_recv.at[1, h], to_y_bwd)
        fwd_part = project(2, h)
        y_o[h].wait_recv()
        proj_buf[2, h] = fwd_part + y_buf[0, h]
        y_a[h] = send(proj_buf.at[2, h], y_buf.at[2, h], y_send.at[2, h], y_recv.at[2, h], to_y_fwd)
        own_cols = pl.ds(pl.multiple_of(y * cols + h * half, half), half)
        own = project(3, h) + hid_buf[:, h * half : (h + 1) * half].astype(jnp.float32) + b_out_ref[:, own_cols]
        proj_buf[3, h] = own

    def place(xt, yt, ct, h):
        row = pl.multiple_of((xt * 2 + ct) * rows, rows)
        col = pl.multiple_of(yt * cols + h * half, half)
        return pl.ds(row, rows), pl.ds(col, half)

    xs = (x, x_bwd, x_fwd, x_opp)
    ys = (y, y_bwd, y_fwd, y_opp)
    x_peers, y_peers = (to_x_fwd, to_x_bwd), (to_y_fwd, to_y_bwd)
    gathers = {}
    pairs = {}

    def spot(h, first, second, ct=None):
        ct = core if ct is None else ct
        if h == 0:
            return place(xs[first], ys[second], ct, h)
        return place(xs[second], ys[first], ct, h)

    def piece(h, first, second):
        return gather_buf.at[spot(h, first, second)]

    def ring_send(h, first, second, slot, phase):
        peers = (x_peers, y_peers) if h == 0 else (y_peers, x_peers)
        peer = peers[phase][1 if slot == 2 else 0]
        index = slot - 1 if phase == 0 else 3 + first * 3 + slot - 1
        key = (h, phase, first if phase else 0, slot)
        ref = piece(h, first, second)
        gathers[key] = send(ref, ref, g_send.at[h, index], g_recv.at[h, index], peer)

    def pair_forward(h, first, second):
        ref = piece(h, first, second)
        index = first * 4 + second
        pairs[(h, first, second)] = send(ref, ref, d_send.at[h, index], d_recv.at[h, index], to_pair)

    def convert(where):
        out_ref[where] = gather_buf[where].astype(jnp.bfloat16)

    def mirrored(slot):
        return (0, 2, 1, 3)[slot]

    todo = []

    def drain(limit):
        while len(todo) > limit:
            h, first, second = todo.pop(0)
            pairs[(h, first, second)].wait_recv()
            convert(spot(h, mirrored(first), mirrored(second), 1 - core))

    def have(h, first, second):
        pair_forward(h, first, second)
        convert(spot(h, first, second))
        todo.append((h, first, second))
        drain(2)

    for h in range(2):
        y_b[h].wait_recv()
        part = proj_buf[3, h] + y_buf[1, h]
        y_a[h].wait_recv()
        gather_buf[spot(h, 0, 0)] = part + y_buf[2, h]
        ring_send(h, 0, 0, 1, 0)
        ring_send(h, 0, 0, 2, 0)
        pair_forward(h, 0, 0)
    for h in range(2):
        ring_send(h, 0, 0, 1, 1)
        ring_send(h, 0, 0, 2, 1)
        convert(spot(h, 0, 0))
        todo.append((h, 0, 0))

    def arrived(h, first, second):
        if second == 0:
            gathers[(h, 0, 0, first)].wait_recv()
            if first == 1:
                ring_send(h, 1, 0, 3, 0)
            ring_send(h, first, 0, 1, 1)
            ring_send(h, first, 0, 2, 1)
        else:
            gathers[(h, 1, first, second)].wait_recv()
            if second == 1:
                ring_send(h, first, 1, 3, 1)
        have(h, first, second)

    order = [(1, 0), (2, 0), (0, 1), (0, 2), (3, 0), (1, 1), (0, 3), (2, 1), (1, 2), (1, 3), (2, 2), (3, 1), (2, 3), (3, 2), (3, 3)]
    for first, second in order:
        for h in range(2):
            arrived(h, first, second)
    drain(0)
    for copy in sends:
        copy.wait_send()


def finish(parts, hidden, w_out, b_out, nx, ny):
    batch, width = parts.shape
    heads = width // LANES - 1
    depth, d_model = w_out.shape
    rows, cols = batch // (2 * nx), d_model // ny
    half = cols // 2
    f32, dma = jnp.float32, pltpu.SemaphoreType.DMA
    return pl.pallas_call(
        functools.partial(finish_kernel, (nx, ny, heads, rows, cols)),
        out_shape=jax.ShapeDtypeStruct((batch, d_model), jnp.bfloat16),
        in_specs=[
            pl.BlockSpec(memory_space=pltpu.VMEM),
            pl.BlockSpec(memory_space=pltpu.VMEM),
            pl.BlockSpec(memory_space=pl.ANY),
            pl.BlockSpec(memory_space=pl.ANY),
        ],
        out_specs=pl.BlockSpec(memory_space=pltpu.VMEM),
        scratch_shapes=[
            pltpu.VMEM((4, depth, cols), jnp.bfloat16),
            pltpu.VMEM((4, rows, width), f32),
            pltpu.VMEM((7, rows, width), f32),
            pltpu.VMEM((3, rows, width), f32),
            pltpu.VMEM((rows, heads * LANES), jnp.bfloat16),
            pltpu.VMEM((4, 2, rows, half), f32),
            pltpu.VMEM((3, 2, rows, half), f32),
            pltpu.VMEM((rows, cols), jnp.bfloat16),
            pltpu.VMEM((batch, d_model), f32),
            dma((4,)),
            dma,
            dma((4,)),
            dma((4,)),
            dma((3,)),
            dma((3,)),
            dma((3, 2)),
            dma((3, 2)),
            dma((2, 15)),
            dma((2, 15)),
            dma((2, 16)),
            dma((2, 16)),
        ],
        compiler_params=pltpu.CompilerParams(collective_id=0, has_side_effects=True, vmem_limit_bytes=48 * 1024 * 1024),
        name="finish",
    )(parts, b_out.reshape(1, d_model), hidden, w_out)


ATTEND_SEQS = 16
WIDE = 256
W_SLOTS = 5


def attend_kernel(
    dims,
    lens_ref,
    hidden_ref,
    gain_ref,
    bias_ref,
    b_query_ref,
    b_kv_ref,
    w_query_ref,
    w_kv_ref,
    k_ref,
    v_ref,
    part_ref,
    k_out_ref,
    v_out_ref,
    h_buf,
    w_buf,
    q_buf,
    kv_buf,
    k_buf,
    v_buf,
    o_buf,
    h_sem,
    w_sem,
    in_sem,
    out_sem,
):
    batch, d_model, heads, pos_local = dims
    hd, seqs = LANES, ATTEND_SEQS
    steps = batch // seqs
    blocks = heads * hd // WIDE
    first_pos = lax.axis_index("sq") * pos_local
    scale = hd ** -0.5
    lowest = float(jnp.finfo(jnp.float32).min)

    def w_copy(k):
        src = w_kv_ref if k == 0 else w_query_ref.at[:, (k - 1) * WIDE : k * WIDE]
        return pltpu.make_async_copy(src, w_buf.at[k % W_SLOTS], w_sem.at[k])

    def rows_of(c):
        return pl.ds(pl.multiple_of(c * seqs, seqs), seqs)

    def read(c):
        return (
            pltpu.make_async_copy(k_ref.at[rows_of(c)], k_buf.at[rows_of(c)], in_sem.at[0, c]),
            pltpu.make_async_copy(v_ref.at[rows_of(c)], v_buf.at[rows_of(c)], in_sem.at[1, c]),
        )

    def write(c):
        return (
            pltpu.make_async_copy(k_buf.at[rows_of(c)], k_out_ref.at[rows_of(c)], out_sem.at[0, c]),
            pltpu.make_async_copy(v_buf.at[rows_of(c)], v_out_ref.at[rows_of(c)], out_sem.at[1, c]),
        )

    h_copy = pltpu.make_async_copy(hidden_ref, h_buf, h_sem)
    h_copy.start()
    for k in range(W_SLOTS):
        w_copy(k).start()
    q_buf[...] = jnp.zeros_like(q_buf)
    h_copy.wait()

    def norm_rows(r, _):
        at = pl.ds(pl.multiple_of(r * 16, 16), 16)
        x_wide = h_buf[at, :].astype(jnp.float32)
        mean_val = jnp.sum(x_wide, axis=-1, keepdims=True) * (1.0 / d_model)
        centered = x_wide - mean_val
        variance = jnp.sum(centered * centered, axis=-1, keepdims=True) * (1.0 / d_model)
        normed = centered * lax.rsqrt(variance + 1e-5)
        h_buf[at, :] = (normed * gain_ref[...] + bias_ref[...]).astype(jnp.bfloat16)
        return 0

    lax.fori_loop(0, batch // 16, norm_rows, 0)

    for k in range(blocks + 1):
        w_copy(k).wait()
        acc = jnp.dot(h_buf[...], w_buf[k % W_SLOTS], preferred_element_type=jnp.float32)
        if k == 0:
            acc = (acc + b_kv_ref[...]).astype(jnp.bfloat16).astype(jnp.float32)
            kv_buf[0] = acc[:, :hd]
            kv_buf[1] = acc[:, hd:]
        else:
            acc = (acc + b_query_ref[:, (k - 1) * WIDE : k * WIDE]).astype(jnp.bfloat16).astype(jnp.float32)
            for e in range(WIDE // hd):
                n = (k - 1) * (WIDE // hd) + e
                q_buf[pl.ds(n, batch, stride=16), :] = acc[:, e * hd : (e + 1) * hd]
        if k + W_SLOTS <= blocks:
            w_copy(k + W_SLOTS).start()
        if k + W_SLOTS == blocks:
            for c in range(steps):
                for copy in read(c):
                    copy.start()

    def attend(c, _):
        for copy in read(c):
            copy.wait()
        sub = lax.broadcasted_iota(jnp.int32, (16, hd), 0)
        for i in range(seqs):
            b = c * seqs + i
            pos = lens_ref[b] - first_pos
            base = pl.multiple_of(lax.div(jnp.clip(pos, 0, pos_local - 1), 16) * 16, 16)
            here = sub + base == pos
            for which, buf in enumerate((k_buf, v_buf)):
                old = buf[b, pl.ds(base, 16), :].astype(jnp.float32)
                new = kv_buf[which, pl.ds(b, 1), :]
                buf[b, pl.ds(base, 16), :] = jnp.where(here, new, old).astype(jnp.bfloat16)
        for copy in write(c):
            copy.start()
        zero = jnp.zeros((16, hd), jnp.bfloat16)
        at_pos = lax.broadcasted_iota(jnp.int32, (16, pos_local), 1) + first_pos
        row = lax.broadcasted_iota(jnp.int32, (16, hd), 0)
        lane = lax.broadcasted_iota(jnp.int32, (16, hd), 1)
        pick_m = (lane == row) & (row < heads)
        pick_l = (lane == row + 64) & (row < heads)
        for i in range(0, seqs, 2):
            b = c * seqs + i
            q0 = q_buf[pl.ds(pl.multiple_of(b * 16, 16), 16), :].astype(jnp.bfloat16)
            q1 = q_buf[pl.ds(pl.multiple_of(b * 16 + 16, 16), 16), :].astype(jnp.bfloat16)
            q2 = jnp.concatenate([jnp.concatenate([q0, zero], axis=1), jnp.concatenate([zero, q1], axis=1)], axis=0)
            k2 = jnp.concatenate([k_buf[b], k_buf[b + 1]], axis=1)
            v2 = jnp.concatenate([v_buf[b], v_buf[b + 1]], axis=1)
            s2 = lax.dot_general(q2, k2, (((1,), (1,)), ((), ())), preferred_element_type=jnp.float32) * scale
            valid = jnp.concatenate([at_pos <= lens_ref[b], at_pos <= lens_ref[b + 1]], axis=0)
            s2 = jnp.where(valid, s2, lowest)
            top = jnp.max(s2, axis=-1, keepdims=True)
            p2 = jnp.where(valid, jnp.exp(s2 - top), 0.0)
            total = jnp.sum(p2, axis=-1, keepdims=True)
            o2 = jnp.dot(p2.astype(jnp.bfloat16), v2, preferred_element_type=jnp.float32)
            for e in range(2):
                half = slice(e * 16, e * 16 + 16)
                stat = jnp.where(pick_m, top[half], 0.0) + jnp.where(pick_l, total[half], 0.0)
                stat = jnp.sum(stat, axis=0, keepdims=True)
                o_buf[(i + e) * 16 : (i + e) * 16 + 16, :] = jnp.where(row == heads, stat, o2[half, e * hd : (e + 1) * hd])
        for n in range(heads + 1):
            part_ref[rows_of(c), n * hd : (n + 1) * hd] = o_buf[pl.ds(n, seqs, stride=16), :]
        return 0

    lax.fori_loop(0, steps, attend, 0)

    def drain(c, _):
        for copy in write(c):
            copy.wait()
        return 0

    lax.fori_loop(0, steps, drain, 0)


def attend(hidden, cache_lens, k_cache, v_cache, ln_gain, ln_bias, w_query, b_query, w_kv, b_kv):
    batch, pos_local, hd = k_cache.shape
    d_model, q_width = w_query.shape
    heads = q_width // hd
    blocks, steps = q_width // WIDE, batch // ATTEND_SEQS
    f32, bf16, dma = jnp.float32, jnp.bfloat16, pltpu.SemaphoreType.DMA
    vmem, hbm = pl.BlockSpec(memory_space=pltpu.VMEM), pl.BlockSpec(memory_space=pl.ANY)
    return pl.pallas_call(
        functools.partial(attend_kernel, (batch, d_model, heads, pos_local)),
        out_shape=[
            jax.ShapeDtypeStruct((batch, (heads + 1) * hd), f32),
            jax.ShapeDtypeStruct(k_cache.shape, bf16),
            jax.ShapeDtypeStruct(v_cache.shape, bf16),
        ],
        in_specs=[pl.BlockSpec(memory_space=pltpu.SMEM), hbm, vmem, vmem, vmem, vmem, hbm, hbm, hbm, hbm],
        out_specs=[vmem, hbm, hbm],
        scratch_shapes=[
            pltpu.VMEM((batch, d_model), bf16),
            pltpu.VMEM((W_SLOTS, d_model, WIDE), bf16),
            pltpu.VMEM((batch * 16, hd), f32),
            pltpu.VMEM((2, batch, hd), f32),
            pltpu.VMEM(k_cache.shape, bf16),
            pltpu.VMEM(v_cache.shape, bf16),
            pltpu.VMEM((ATTEND_SEQS * 16, hd), f32),
            dma,
            dma((blocks + 1,)),
            dma((2, steps)),
            dma((2, steps)),
        ],
        compiler_params=pltpu.CompilerParams(vmem_limit_bytes=62 * 1024 * 1024),
        name="attend",
    )(
        cache_lens,
        hidden,
        ln_gain.reshape(1, d_model),
        ln_bias.reshape(1, d_model),
        b_query.reshape(1, q_width),
        b_kv.reshape(1, 2 * hd),
        w_query,
        w_kv,
        k_cache,
        v_cache,
    )


def solution(mesh):
    nx, ny = mesh.shape["sq"] // 2, mesh.shape["tp"]

    def local_step(hidden, cache_lens, k_cache, v_cache, ln_gain, ln_bias, w_query, b_query, w_kv, b_kv, w_out, b_out):
        parts, key_new, val_new = attend(hidden, cache_lens, k_cache, v_cache, ln_gain, ln_bias, w_query, b_query, w_kv, b_kv)
        out_hidden = finish(parts, hidden, w_out, b_out, nx, ny)
        return out_hidden, key_new, val_new

    cache_spec = P("dp", "sq", None)
    row_spec = P("dp", None)
    in_specs = (row_spec, P("dp"), cache_spec, cache_spec, P(None), P(None), P(None, "tp"), P("tp"), P(None, None), P(None), P("tp", None), P(None))
    out_specs = (row_spec, cache_spec, cache_spec)
    return jax.shard_map(local_step, mesh=mesh, in_specs=in_specs, out_specs=out_specs, check_vma=False)
```

```python
import functools

import jax
import jax.numpy as jnp
from jax import lax
from jax.experimental import pallas as pl
from jax.experimental.pallas import tpu as pltpu
from jax.sharding import PartitionSpec as P

MESH = pl.DeviceIdType.MESH
LANES = 128


def merge_into(dst, part_a, part_b, heads):
    width = heads * LANES
    stat_a, stat_b = part_a[:, width:], part_b[:, width:]
    top = jnp.maximum(stat_a, stat_b)
    exp_a, exp_b = jnp.exp(stat_a - top), jnp.exp(stat_b - top)
    sums = stat_a * pltpu.roll(exp_a, 64, 1) + stat_b * pltpu.roll(exp_b, 64, 1)
    lane = lax.broadcasted_iota(jnp.int32, top.shape, 1)
    dst[:, width:] = jnp.where(lane < 64, top, sums)
    for n in range(heads):
        cols = slice(n * LANES, (n + 1) * LANES)
        dst[:, cols] = part_a[:, cols] * exp_a[:, n : n + 1] + part_b[:, cols] * exp_b[:, n : n + 1]


def finish_kernel(
    dims,
    part_ref,
    b_out_ref,
    hidden_ref,
    w_out_ref,
    out_ref,
    w_buf,
    pair_buf,
    merge_buf,
    x_buf,
    att_buf,
    proj_buf,
    y_buf,
    hid_buf,
    gather_buf,
    w_sem,
    hid_sem,
    pair_send,
    pair_recv,
    x_send,
    x_recv,
    y_send,
    y_recv,
    g_send,
    g_recv,
    d_send,
    d_recv,
):
    nx, ny, heads, rows, cols = dims
    half = cols // 2
    width = heads * LANES
    sq = lax.axis_index("sq")
    y = lax.axis_index("tp")
    x = sq // 2
    core = sq % 2
    step = 1 - 2 * core

    def wrap(value, size):
        return lax.rem(value + 2 * size, size)

    x_fwd, x_bwd, x_opp = wrap(x + step, nx), wrap(x - step, nx), wrap(x + 2, nx)
    y_fwd, y_bwd, y_opp = wrap(y + step, ny), wrap(y - step, ny), wrap(y + 2, ny)
    to_pair = {"sq": x * 2 + 1 - core}
    to_x_fwd, to_x_bwd = {"sq": x_fwd * 2 + core}, {"sq": x_bwd * 2 + core}
    to_y_fwd, to_y_bwd = {"tp": y_fwd}, {"tp": y_bwd}

    barrier = pltpu.get_barrier_semaphore()
    for peer in (to_pair, to_x_fwd, to_x_bwd, to_y_fwd, to_y_bwd):
        pl.semaphore_signal(barrier, inc=1, device_id=peer, device_id_type=MESH)

    y_order = (y_opp, y_bwd, y_fwd, y)
    w_copies = []
    for k, target in enumerate(y_order):
        src = w_out_ref.at[:, pl.ds(pl.multiple_of(target * cols, cols), cols)]
        w_copies.append(pltpu.make_async_copy(src, w_buf.at[k], w_sem.at[k]))
    my_row = pl.multiple_of(sq * rows, rows)
    my_col = pl.multiple_of(y * cols, cols)
    hid_copy = pltpu.make_async_copy(hidden_ref.at[pl.ds(my_row, rows), pl.ds(my_col, cols)], hid_buf, hid_sem)
    pl.semaphore_wait(barrier, 5)

    sends = []

    def send(src, dst, ssem, rsem, peer):
        copy = pltpu.make_async_remote_copy(
            src_ref=src, dst_ref=dst, send_sem=ssem, recv_sem=rsem, device_id=peer, device_id_type=MESH
        )
        copy.start()
        sends.append(copy)
        return copy

    def part_rows(xt, ct):
        return pl.ds(pl.multiple_of((xt * 2 + ct) * rows, rows), rows)

    pair = []
    for k, xt in enumerate((x_opp, x_fwd, x_bwd, x)):
        pair.append(send(part_ref.at[part_rows(xt, 1 - core), :], pair_buf.at[k], pair_send.at[k], pair_recv.at[k], to_pair))
    for copy in w_copies:
        copy.start()
    hid_copy.start()

    pair[0].wait_recv()
    merge_into(merge_buf.at[0], part_ref[part_rows(x_opp, core), :], pair_buf[0], heads)
    x_o = send(merge_buf.at[0], x_buf.at[0], x_send.at[0], x_recv.at[0], to_x_fwd)
    pair[1].wait_recv()
    merge_into(merge_buf.at[1], part_ref[part_rows(x_bwd, core), :], pair_buf[1], heads)
    x_b = send(merge_buf.at[1], x_buf.at[1], x_send.at[1], x_recv.at[1], to_x_bwd)
    pair[2].wait_recv()
    merge_into(merge_buf.at[2], part_ref[part_rows(x_fwd, core), :], pair_buf[2], heads)
    x_o.wait_recv()
    merge_into(merge_buf.at[3], merge_buf[2], x_buf[0], heads)
    x_a = send(merge_buf.at[3], x_buf.at[2], x_send.at[2], x_recv.at[2], to_x_fwd)
    pair[3].wait_recv()
    merge_into(merge_buf.at[4], part_ref[part_rows(x, core), :], pair_buf[3], heads)
    x_b.wait_recv()
    merge_into(merge_buf.at[5], merge_buf[4], x_buf[1], heads)
    x_a.wait_recv()
    merge_into(merge_buf.at[6], merge_buf[5], x_buf[2], heads)
    stat = merge_buf[6, :, width:]
    for n in range(heads):
        block = slice(n * LANES, (n + 1) * LANES)
        att_buf[:, block] = (merge_buf[6, :, block] / stat[:, 64 + n : 65 + n]).astype(jnp.bfloat16)

    for copy in w_copies:
        copy.wait()
    hid_copy.wait()

    def project(k, h):
        return jnp.dot(att_buf[...], w_buf[k, :, h * half : (h + 1) * half], preferred_element_type=jnp.float32)

    y_o, y_b, y_a = [None, None], [None, None], [None, None]
    for h in range(2):
        proj_buf[0, h] = project(0, h)
        y_o[h] = send(proj_buf.at[0, h], y_buf.at[0, h], y_send.at[0, h], y_recv.at[0, h], to_y_fwd)
    for h in range(2):
        proj_buf[1, h] = project(1, h)
        y_b[h] = send(proj_buf.at[1, h], y_buf.at[1, h], y_send.at[1, h], y_recv.at[1, h], to_y_bwd)
        fwd_part = project(2, h)
        y_o[h].wait_recv()
        proj_buf[2, h] = fwd_part + y_buf[0, h]
        y_a[h] = send(proj_buf.at[2, h], y_buf.at[2, h], y_send.at[2, h], y_recv.at[2, h], to_y_fwd)
        own_cols = pl.ds(pl.multiple_of(y * cols + h * half, half), half)
        own = project(3, h) + hid_buf[:, h * half : (h + 1) * half].astype(jnp.float32) + b_out_ref[:, own_cols]
        proj_buf[3, h] = own

    def place(xt, yt, ct, h):
        row = pl.multiple_of((xt * 2 + ct) * rows, rows)
        col = pl.multiple_of(yt * cols + h * half, half)
        return pl.ds(row, rows), pl.ds(col, half)

    xs = (x, x_bwd, x_fwd, x_opp)
    ys = (y, y_bwd, y_fwd, y_opp)
    x_peers, y_peers = (to_x_fwd, to_x_bwd), (to_y_fwd, to_y_bwd)
    gathers = {}
    pairs = {}

    def spot(h, first, second, ct=None):
        ct = core if ct is None else ct
        if h == 0:
            return place(xs[first], ys[second], ct, h)
        return place(xs[second], ys[first], ct, h)

    def piece(h, first, second):
        return gather_buf.at[spot(h, first, second)]

    def ring_send(h, first, second, slot, phase):
        peers = (x_peers, y_peers) if h == 0 else (y_peers, x_peers)
        peer = peers[phase][1 if slot == 2 else 0]
        index = slot - 1 if phase == 0 else 3 + first * 3 + slot - 1
        key = (h, phase, first if phase else 0, slot)
        ref = piece(h, first, second)
        gathers[key] = send(ref, ref, g_send.at[h, index], g_recv.at[h, index], peer)

    def pair_forward(h, first, second):
        ref = piece(h, first, second)
        index = first * 4 + second
        pairs[(h, first, second)] = send(ref, ref, d_send.at[h, index], d_recv.at[h, index], to_pair)

    def convert(where):
        out_ref[where] = gather_buf[where].astype(jnp.bfloat16)

    def mirrored(slot):
        return (0, 2, 1, 3)[slot]

    todo = []

    def drain(limit):
        while len(todo) > limit:
            h, first, second = todo.pop(0)
            pairs[(h, first, second)].wait_recv()
            convert(spot(h, mirrored(first), mirrored(second), 1 - core))

    def have(h, first, second):
        pair_forward(h, first, second)
        convert(spot(h, first, second))
        todo.append((h, first, second))
        drain(2)

    for h in range(2):
        y_b[h].wait_recv()
        part = proj_buf[3, h] + y_buf[1, h]
        y_a[h].wait_recv()
        gather_buf[spot(h, 0, 0)] = part + y_buf[2, h]
        ring_send(h, 0, 0, 1, 0)
        ring_send(h, 0, 0, 2, 0)
        pair_forward(h, 0, 0)
    for h in range(2):
        ring_send(h, 0, 0, 1, 1)
        ring_send(h, 0, 0, 2, 1)
        convert(spot(h, 0, 0))
        todo.append((h, 0, 0))

    def arrived(h, first, second):
        if second == 0:
            gathers[(h, 0, 0, first)].wait_recv()
            if first == 1:
                ring_send(h, 1, 0, 3, 0)
            ring_send(h, first, 0, 1, 1)
            ring_send(h, first, 0, 2, 1)
        else:
            gathers[(h, 1, first, second)].wait_recv()
            if second == 1:
                ring_send(h, first, 1, 3, 1)
        have(h, first, second)

    order = [(1, 0), (2, 0), (0, 1), (0, 2), (3, 0), (1, 1), (0, 3), (2, 1), (1, 2), (1, 3), (2, 2), (3, 1), (2, 3), (3, 2), (3, 3)]
    for first, second in order:
        for h in range(2):
            arrived(h, first, second)
    drain(0)
    for copy in sends:
        copy.wait_send()


def finish(parts, hidden, w_out, b_out, nx, ny):
    batch, width = parts.shape
    heads = width // LANES - 1
    depth, d_model = w_out.shape
    rows, cols = batch // (2 * nx), d_model // ny
    half = cols // 2
    f32, dma = jnp.float32, pltpu.SemaphoreType.DMA
    return pl.pallas_call(
        functools.partial(finish_kernel, (nx, ny, heads, rows, cols)),
        out_shape=jax.ShapeDtypeStruct((batch, d_model), jnp.bfloat16),
        in_specs=[
            pl.BlockSpec(memory_space=pltpu.VMEM),
            pl.BlockSpec(memory_space=pltpu.VMEM),
            pl.BlockSpec(memory_space=pl.ANY),
            pl.BlockSpec(memory_space=pl.ANY),
        ],
        out_specs=pl.BlockSpec(memory_space=pltpu.VMEM),
        scratch_shapes=[
            pltpu.VMEM((4, depth, cols), jnp.bfloat16),
            pltpu.VMEM((4, rows, width), f32),
            pltpu.VMEM((7, rows, width), f32),
            pltpu.VMEM((3, rows, width), f32),
            pltpu.VMEM((rows, heads * LANES), jnp.bfloat16),
            pltpu.VMEM((4, 2, rows, half), f32),
            pltpu.VMEM((3, 2, rows, half), f32),
            pltpu.VMEM((rows, cols), jnp.bfloat16),
            pltpu.VMEM((batch, d_model), f32),
            dma((4,)),
            dma,
            dma((4,)),
            dma((4,)),
            dma((3,)),
            dma((3,)),
            dma((3, 2)),
            dma((3, 2)),
            dma((2, 15)),
            dma((2, 15)),
            dma((2, 16)),
            dma((2, 16)),
        ],
        compiler_params=pltpu.CompilerParams(collective_id=0, has_side_effects=True, vmem_limit_bytes=48 * 1024 * 1024),
        name="finish",
    )(parts, b_out.reshape(1, d_model), hidden, w_out)


ATTEND_SEQS = 16
WIDE = 256
W_SLOTS = 5


def project_kernel(
    dims, hidden_ref, gain_ref, bias_ref, b_query_ref, b_kv_ref, w_query_ref, w_kv_ref, q_buf, kv_buf, h_buf, w_buf, h_sem, w_sem
):
    batch, d_model, heads = dims
    hd = LANES
    blocks = heads * hd // WIDE

    def w_copy(k):
        src = w_kv_ref if k == 0 else w_query_ref.at[:, (k - 1) * WIDE : k * WIDE]
        return pltpu.make_async_copy(src, w_buf.at[k % W_SLOTS], w_sem.at[k])

    h_copy = pltpu.make_async_copy(hidden_ref, h_buf, h_sem)
    h_copy.start()
    for k in range(W_SLOTS):
        w_copy(k).start()
    q_buf[...] = jnp.zeros_like(q_buf)
    h_copy.wait()

    def norm_rows(r, _):
        at = pl.ds(pl.multiple_of(r * 16, 16), 16)
        x_wide = h_buf[at, :].astype(jnp.float32)
        mean_val = jnp.sum(x_wide, axis=-1, keepdims=True) * (1.0 / d_model)
        centered = x_wide - mean_val
        variance = jnp.sum(centered * centered, axis=-1, keepdims=True) * (1.0 / d_model)
        normed = centered * lax.rsqrt(variance + 1e-5)
        h_buf[at, :] = (normed * gain_ref[...] + bias_ref[...]).astype(jnp.bfloat16)
        return 0

    lax.fori_loop(0, batch // 16, norm_rows, 0)

    for k in range(blocks + 1):
        w_copy(k).wait()
        acc = jnp.dot(h_buf[...], w_buf[k % W_SLOTS], preferred_element_type=jnp.float32)
        if k == 0:
            acc = (acc + b_kv_ref[...]).astype(jnp.bfloat16).astype(jnp.float32)
            kv_buf[0] = acc[:, :hd]
            kv_buf[1] = acc[:, hd:]
        else:
            acc = (acc + b_query_ref[:, (k - 1) * WIDE : k * WIDE]).astype(jnp.bfloat16).astype(jnp.float32)
            for e in range(WIDE // hd):
                n = (k - 1) * (WIDE // hd) + e
                q_buf[pl.ds(n, batch, stride=16), :] = acc[:, e * hd : (e + 1) * hd]
        if k + W_SLOTS <= blocks:
            w_copy(k + W_SLOTS).start()


def attend_kernel(
    dims,
    lens_ref,
    q_buf,
    kv_buf,
    k_ref,
    v_ref,
    part_ref,
    k_out_ref,
    v_out_ref,
    k_buf,
    v_buf,
    o_buf,
    in_sem,
    out_sem,
):
    batch, d_model, heads, pos_local = dims
    hd, seqs = LANES, ATTEND_SEQS
    steps = batch // seqs
    first_pos = lax.axis_index("sq") * pos_local
    scale = hd ** -0.5
    lowest = float(jnp.finfo(jnp.float32).min)

    def rows_of(c):
        return pl.ds(pl.multiple_of(c * seqs, seqs), seqs)

    def read(c):
        return (
            pltpu.make_async_copy(k_ref.at[rows_of(c)], k_buf.at[rows_of(c)], in_sem.at[0, c]),
            pltpu.make_async_copy(v_ref.at[rows_of(c)], v_buf.at[rows_of(c)], in_sem.at[1, c]),
        )

    def write(c):
        return (
            pltpu.make_async_copy(k_buf.at[rows_of(c)], k_out_ref.at[rows_of(c)], out_sem.at[0, c]),
            pltpu.make_async_copy(v_buf.at[rows_of(c)], v_out_ref.at[rows_of(c)], out_sem.at[1, c]),
        )

    for c in range(steps):
        for copy in read(c):
            copy.start()

    def attend(c, _):
        for copy in read(c):
            copy.wait()
        sub = lax.broadcasted_iota(jnp.int32, (16, hd), 0)
        for i in range(seqs):
            b = c * seqs + i
            pos = lens_ref[b] - first_pos
            base = pl.multiple_of(lax.div(jnp.clip(pos, 0, pos_local - 1), 16) * 16, 16)
            here = sub + base == pos
            for which, buf in enumerate((k_buf, v_buf)):
                old = buf[b, pl.ds(base, 16), :].astype(jnp.float32)
                new = kv_buf[which, pl.ds(b, 1), :]
                buf[b, pl.ds(base, 16), :] = jnp.where(here, new, old).astype(jnp.bfloat16)
        for copy in write(c):
            copy.start()
        zero = jnp.zeros((16, hd), jnp.bfloat16)
        at_pos = lax.broadcasted_iota(jnp.int32, (16, pos_local), 1) + first_pos
        row = lax.broadcasted_iota(jnp.int32, (16, hd), 0)
        lane = lax.broadcasted_iota(jnp.int32, (16, hd), 1)
        pick_m = (lane == row) & (row < heads)
        pick_l = (lane == row + 64) & (row < heads)
        for i in range(0, seqs, 2):
            b = c * seqs + i
            q0 = q_buf[pl.ds(pl.multiple_of(b * 16, 16), 16), :].astype(jnp.bfloat16)
            q1 = q_buf[pl.ds(pl.multiple_of(b * 16 + 16, 16), 16), :].astype(jnp.bfloat16)
            q2 = jnp.concatenate([jnp.concatenate([q0, zero], axis=1), jnp.concatenate([zero, q1], axis=1)], axis=0)
            k2 = jnp.concatenate([k_buf[b], k_buf[b + 1]], axis=1)
            v2 = jnp.concatenate([v_buf[b], v_buf[b + 1]], axis=1)
            s2 = lax.dot_general(q2, k2, (((1,), (1,)), ((), ())), preferred_element_type=jnp.float32) * scale
            valid = jnp.concatenate([at_pos <= lens_ref[b], at_pos <= lens_ref[b + 1]], axis=0)
            s2 = jnp.where(valid, s2, lowest)
            top = jnp.max(s2, axis=-1, keepdims=True)
            p2 = jnp.where(valid, jnp.exp(s2 - top), 0.0)
            total = jnp.sum(p2, axis=-1, keepdims=True)
            o2 = jnp.dot(p2.astype(jnp.bfloat16), v2, preferred_element_type=jnp.float32)
            for e in range(2):
                half = slice(e * 16, e * 16 + 16)
                stat = jnp.where(pick_m, top[half], 0.0) + jnp.where(pick_l, total[half], 0.0)
                stat = jnp.sum(stat, axis=0, keepdims=True)
                o_buf[(i + e) * 16 : (i + e) * 16 + 16, :] = jnp.where(row == heads, stat, o2[half, e * hd : (e + 1) * hd])
        for n in range(heads + 1):
            part_ref[rows_of(c), n * hd : (n + 1) * hd] = o_buf[pl.ds(n, seqs, stride=16), :]
        return 0

    lax.fori_loop(0, steps, attend, 0)

    def drain(c, _):
        for copy in write(c):
            copy.wait()
        return 0

    lax.fori_loop(0, steps, drain, 0)


def attend(hidden, cache_lens, k_cache, v_cache, ln_gain, ln_bias, w_query, b_query, w_kv, b_kv):
    batch, pos_local, hd = k_cache.shape
    d_model, q_width = w_query.shape
    heads = q_width // hd
    blocks, steps = q_width // WIDE, batch // ATTEND_SEQS
    f32, bf16, dma = jnp.float32, jnp.bfloat16, pltpu.SemaphoreType.DMA
    vmem, hbm = pl.BlockSpec(memory_space=pltpu.VMEM), pl.BlockSpec(memory_space=pl.ANY)
    query, key_val = pl.pallas_call(
        functools.partial(project_kernel, (batch, d_model, heads)),
        out_shape=[pltpu.VMEM((batch * 16, hd), f32), pltpu.VMEM((2, batch, hd), f32)],
        in_specs=[hbm, vmem, vmem, vmem, vmem, hbm, hbm],
        out_specs=[vmem, vmem],
        scratch_shapes=[
            pltpu.VMEM((batch, d_model), bf16),
            pltpu.VMEM((W_SLOTS, d_model, WIDE), bf16),
            dma,
            dma((blocks + 1,)),
        ],
        compiler_params=pltpu.CompilerParams(vmem_limit_bytes=24 * 1024 * 1024),
        name="project",
    )(
        hidden,
        ln_gain.reshape(1, d_model),
        ln_bias.reshape(1, d_model),
        b_query.reshape(1, q_width),
        b_kv.reshape(1, 2 * hd),
        w_query,
        w_kv,
    )
    return pl.pallas_call(
        functools.partial(attend_kernel, (batch, d_model, heads, pos_local)),
        out_shape=[
            pltpu.VMEM((batch, (heads + 1) * hd), f32),
            jax.ShapeDtypeStruct(k_cache.shape, bf16),
            jax.ShapeDtypeStruct(v_cache.shape, bf16),
        ],
        in_specs=[pl.BlockSpec(memory_space=pltpu.SMEM), vmem, vmem, hbm, hbm],
        out_specs=[vmem, hbm, hbm],
        scratch_shapes=[
            pltpu.VMEM(k_cache.shape, bf16),
            pltpu.VMEM(v_cache.shape, bf16),
            pltpu.VMEM((ATTEND_SEQS * 16, hd), f32),
            dma((2, steps)),
            dma((2, steps)),
        ],
        compiler_params=pltpu.CompilerParams(vmem_limit_bytes=40 * 1024 * 1024),
        name="attend",
    )(cache_lens, query, key_val, k_cache, v_cache)


def solution(mesh):
    nx, ny = mesh.shape["sq"] // 2, mesh.shape["tp"]

    def local_step(hidden, cache_lens, k_cache, v_cache, ln_gain, ln_bias, w_query, b_query, w_kv, b_kv, w_out, b_out):
        parts, key_new, val_new = attend(hidden, cache_lens, k_cache, v_cache, ln_gain, ln_bias, w_query, b_query, w_kv, b_kv)
        out_hidden = finish(parts, hidden, w_out, b_out, nx, ny)
        return out_hidden, key_new, val_new

    cache_spec = P("dp", "sq", None)
    row_spec = P("dp", None)
    in_specs = (row_spec, P("dp"), cache_spec, cache_spec, P(None), P(None), P(None, "tp"), P("tp"), P(None, None), P(None), P("tp", None), P(None))
    out_specs = (row_spec, cache_spec, cache_spec)
    return jax.shard_map(local_step, mesh=mesh, in_specs=in_specs, out_specs=out_specs, check_vma=False)
```

```python
import functools

import jax
import jax.numpy as jnp
from jax import lax
from jax.experimental import pallas as pl
from jax.experimental.pallas import tpu as pltpu
from jax.sharding import PartitionSpec as P

MESH = pl.DeviceIdType.MESH
LANES = 128


def merge_into(dst, part_a, part_b, heads):
    width = heads * LANES
    stat_a, stat_b = part_a[:, width:], part_b[:, width:]
    top = jnp.maximum(stat_a, stat_b)
    exp_a, exp_b = jnp.exp(stat_a - top), jnp.exp(stat_b - top)
    sums = stat_a * pltpu.roll(exp_a, 64, 1) + stat_b * pltpu.roll(exp_b, 64, 1)
    lane = lax.broadcasted_iota(jnp.int32, top.shape, 1)
    dst[:, width:] = jnp.where(lane < 64, top, sums)
    for n in range(heads):
        cols = slice(n * LANES, (n + 1) * LANES)
        dst[:, cols] = part_a[:, cols] * exp_a[:, n : n + 1] + part_b[:, cols] * exp_b[:, n : n + 1]


def finish_kernel(
    dims,
    part_ref,
    b_out_ref,
    hidden_ref,
    w_out_ref,
    out_ref,
    w_buf,
    pair_buf,
    merge_buf,
    x_buf,
    att_buf,
    proj_buf,
    y_buf,
    hid_buf,
    gather_buf,
    w_sem,
    hid_sem,
    pair_send,
    pair_recv,
    x_send,
    x_recv,
    y_send,
    y_recv,
    g_send,
    g_recv,
    d_send,
    d_recv,
):
    nx, ny, heads, rows, cols = dims
    half = cols // 2
    width = heads * LANES
    sq = lax.axis_index("sq")
    y = lax.axis_index("tp")
    x = sq // 2
    core = sq % 2
    step = 1 - 2 * core

    def wrap(value, size):
        return lax.rem(value + 2 * size, size)

    x_fwd, x_bwd, x_opp = wrap(x + step, nx), wrap(x - step, nx), wrap(x + 2, nx)
    y_fwd, y_bwd, y_opp = wrap(y + step, ny), wrap(y - step, ny), wrap(y + 2, ny)
    to_pair = {"sq": x * 2 + 1 - core}
    to_x_fwd, to_x_bwd = {"sq": x_fwd * 2 + core}, {"sq": x_bwd * 2 + core}
    to_y_fwd, to_y_bwd = {"tp": y_fwd}, {"tp": y_bwd}

    barrier = pltpu.get_barrier_semaphore()
    for peer in (to_pair, to_x_fwd, to_x_bwd, to_y_fwd, to_y_bwd):
        pl.semaphore_signal(barrier, inc=1, device_id=peer, device_id_type=MESH)

    y_order = (y_opp, y_bwd, y_fwd, y)
    w_copies = []
    for k, target in enumerate(y_order):
        src = w_out_ref.at[:, pl.ds(pl.multiple_of(target * cols, cols), cols)]
        w_copies.append(pltpu.make_async_copy(src, w_buf.at[k], w_sem.at[k]))
    my_row = pl.multiple_of(sq * rows, rows)
    my_col = pl.multiple_of(y * cols, cols)
    hid_copy = pltpu.make_async_copy(hidden_ref.at[pl.ds(my_row, rows), pl.ds(my_col, cols)], hid_buf, hid_sem)
    pl.semaphore_wait(barrier, 5)

    sends = []

    def send(src, dst, ssem, rsem, peer):
        copy = pltpu.make_async_remote_copy(
            src_ref=src, dst_ref=dst, send_sem=ssem, recv_sem=rsem, device_id=peer, device_id_type=MESH
        )
        copy.start()
        sends.append(copy)
        return copy

    def part_rows(xt, ct):
        return pl.ds(pl.multiple_of((xt * 2 + ct) * rows, rows), rows)

    pair = []
    for k, xt in enumerate((x_opp, x_fwd, x_bwd, x)):
        pair.append(send(part_ref.at[part_rows(xt, 1 - core), :], pair_buf.at[k], pair_send.at[k], pair_recv.at[k], to_pair))
    for copy in w_copies:
        copy.start()
    hid_copy.start()

    pair[0].wait_recv()
    merge_into(merge_buf.at[0], part_ref[part_rows(x_opp, core), :], pair_buf[0], heads)
    x_o = send(merge_buf.at[0], x_buf.at[0], x_send.at[0], x_recv.at[0], to_x_fwd)
    pair[1].wait_recv()
    merge_into(merge_buf.at[1], part_ref[part_rows(x_bwd, core), :], pair_buf[1], heads)
    x_b = send(merge_buf.at[1], x_buf.at[1], x_send.at[1], x_recv.at[1], to_x_bwd)
    pair[2].wait_recv()
    merge_into(merge_buf.at[2], part_ref[part_rows(x_fwd, core), :], pair_buf[2], heads)
    x_o.wait_recv()
    merge_into(merge_buf.at[3], merge_buf[2], x_buf[0], heads)
    x_a = send(merge_buf.at[3], x_buf.at[2], x_send.at[2], x_recv.at[2], to_x_fwd)
    pair[3].wait_recv()
    merge_into(merge_buf.at[4], part_ref[part_rows(x, core), :], pair_buf[3], heads)
    x_b.wait_recv()
    merge_into(merge_buf.at[5], merge_buf[4], x_buf[1], heads)
    x_a.wait_recv()
    merge_into(merge_buf.at[6], merge_buf[5], x_buf[2], heads)
    stat = merge_buf[6, :, width:]
    for n in range(heads):
        block = slice(n * LANES, (n + 1) * LANES)
        att_buf[:, block] = (merge_buf[6, :, block] / stat[:, 64 + n : 65 + n]).astype(jnp.bfloat16)

    for copy in w_copies:
        copy.wait()
    hid_copy.wait()

    def project(k, h):
        return jnp.dot(att_buf[...], w_buf[k, :, h * half : (h + 1) * half], preferred_element_type=jnp.float32)

    y_o, y_b, y_a = [None, None], [None, None], [None, None]
    for h in range(2):
        proj_buf[0, h] = project(0, h)
        y_o[h] = send(proj_buf.at[0, h], y_buf.at[0, h], y_send.at[0, h], y_recv.at[0, h], to_y_fwd)
    for h in range(2):
        proj_buf[1, h] = project(1, h)
        y_b[h] = send(proj_buf.at[1, h], y_buf.at[1, h], y_send.at[1, h], y_recv.at[1, h], to_y_bwd)
        fwd_part = project(2, h)
        y_o[h].wait_recv()
        proj_buf[2, h] = fwd_part + y_buf[0, h]
        y_a[h] = send(proj_buf.at[2, h], y_buf.at[2, h], y_send.at[2, h], y_recv.at[2, h], to_y_fwd)
        own_cols = pl.ds(pl.multiple_of(y * cols + h * half, half), half)
        own = project(3, h) + hid_buf[:, h * half : (h + 1) * half].astype(jnp.float32) + b_out_ref[:, own_cols]
        proj_buf[3, h] = own

    def place(xt, yt, ct, h):
        row = pl.multiple_of((xt * 2 + ct) * rows, rows)
        col = pl.multiple_of(yt * cols + h * half, half)
        return pl.ds(row, rows), pl.ds(col, half)

    xs = (x, x_bwd, x_fwd, x_opp)
    ys = (y, y_bwd, y_fwd, y_opp)
    x_peers, y_peers = (to_x_fwd, to_x_bwd), (to_y_fwd, to_y_bwd)
    gathers = {}
    pairs = {}

    def spot(h, first, second, ct=None):
        ct = core if ct is None else ct
        if h == 0:
            return place(xs[first], ys[second], ct, h)
        return place(xs[second], ys[first], ct, h)

    def piece(h, first, second):
        return gather_buf.at[spot(h, first, second)]

    def ring_send(h, first, second, slot, phase):
        peers = (x_peers, y_peers) if h == 0 else (y_peers, x_peers)
        peer = peers[phase][1 if slot == 2 else 0]
        index = slot - 1 if phase == 0 else 3 + first * 3 + slot - 1
        key = (h, phase, first if phase else 0, slot)
        ref = piece(h, first, second)
        gathers[key] = send(ref, ref, g_send.at[h, index], g_recv.at[h, index], peer)

    def pair_forward(h, first, second):
        ref = piece(h, first, second)
        index = first * 4 + second
        pairs[(h, first, second)] = send(ref, ref, d_send.at[h, index], d_recv.at[h, index], to_pair)

    def convert(where):
        out_ref[where] = gather_buf[where].astype(jnp.bfloat16)

    def mirrored(slot):
        return (0, 2, 1, 3)[slot]

    todo = []

    def drain(limit):
        while len(todo) > limit:
            h, first, second = todo.pop(0)
            pairs[(h, first, second)].wait_recv()
            convert(spot(h, mirrored(first), mirrored(second), 1 - core))

    def have(h, first, second):
        pair_forward(h, first, second)
        convert(spot(h, first, second))
        todo.append((h, first, second))
        drain(2)

    for h in range(2):
        y_b[h].wait_recv()
        part = proj_buf[3, h] + y_buf[1, h]
        y_a[h].wait_recv()
        gather_buf[spot(h, 0, 0)] = part + y_buf[2, h]
        ring_send(h, 0, 0, 1, 0)
        ring_send(h, 0, 0, 2, 0)
        pair_forward(h, 0, 0)
    for h in range(2):
        ring_send(h, 0, 0, 1, 1)
        ring_send(h, 0, 0, 2, 1)
        convert(spot(h, 0, 0))
        todo.append((h, 0, 0))

    def arrived(h, first, second):
        if second == 0:
            gathers[(h, 0, 0, first)].wait_recv()
            if first == 1:
                ring_send(h, 1, 0, 3, 0)
            ring_send(h, first, 0, 1, 1)
            ring_send(h, first, 0, 2, 1)
        else:
            gathers[(h, 1, first, second)].wait_recv()
            if second == 1:
                ring_send(h, first, 1, 3, 1)
        have(h, first, second)

    order = [(1, 0), (2, 0), (0, 1), (0, 2), (3, 0), (1, 1), (0, 3), (2, 1), (1, 2), (1, 3), (2, 2), (3, 1), (2, 3), (3, 2), (3, 3)]
    for first, second in order:
        for h in range(2):
            arrived(h, first, second)
    drain(0)
    for copy in sends:
        copy.wait_send()


def finish(parts, hidden, w_out, b_out, nx, ny):
    batch, width = parts.shape
    heads = width // LANES - 1
    depth, d_model = w_out.shape
    rows, cols = batch // (2 * nx), d_model // ny
    half = cols // 2
    f32, dma = jnp.float32, pltpu.SemaphoreType.DMA
    return pl.pallas_call(
        functools.partial(finish_kernel, (nx, ny, heads, rows, cols)),
        out_shape=jax.ShapeDtypeStruct((batch, d_model), jnp.bfloat16),
        in_specs=[
            pl.BlockSpec(memory_space=pltpu.VMEM),
            pl.BlockSpec(memory_space=pltpu.VMEM),
            pl.BlockSpec(memory_space=pl.ANY),
            pl.BlockSpec(memory_space=pl.ANY),
        ],
        out_specs=pl.BlockSpec(memory_space=pltpu.VMEM),
        scratch_shapes=[
            pltpu.VMEM((4, depth, cols), jnp.bfloat16),
            pltpu.VMEM((4, rows, width), f32),
            pltpu.VMEM((7, rows, width), f32),
            pltpu.VMEM((3, rows, width), f32),
            pltpu.VMEM((rows, heads * LANES), jnp.bfloat16),
            pltpu.VMEM((4, 2, rows, half), f32),
            pltpu.VMEM((3, 2, rows, half), f32),
            pltpu.VMEM((rows, cols), jnp.bfloat16),
            pltpu.VMEM((batch, d_model), f32),
            dma((4,)),
            dma,
            dma((4,)),
            dma((4,)),
            dma((3,)),
            dma((3,)),
            dma((3, 2)),
            dma((3, 2)),
            dma((2, 15)),
            dma((2, 15)),
            dma((2, 16)),
            dma((2, 16)),
        ],
        compiler_params=pltpu.CompilerParams(collective_id=0, has_side_effects=True, vmem_limit_bytes=48 * 1024 * 1024),
        name="finish",
    )(parts, b_out.reshape(1, d_model), hidden, w_out)


ATTEND_SEQS = 16
WIDE = 256
W_SLOTS = 5


def attend_kernel(
    dims,
    lens_ref,
    hidden_ref,
    gain_ref,
    bias_ref,
    b_query_ref,
    b_kv_ref,
    w_query_ref,
    w_kv_ref,
    k_ref,
    v_ref,
    part_ref,
    k_out_ref,
    v_out_ref,
    h_buf,
    w_buf,
    q_buf,
    kv_buf,
    k_buf,
    v_buf,
    o_buf,
    s_buf0,
    s_buf1,
    stat_buf,
    stat_buf2,
    h_sem,
    w_sem,
    in_sem,
    out_sem,
):
    batch, d_model, heads, pos_local = dims
    hd, seqs = LANES, ATTEND_SEQS
    steps = batch // seqs
    blocks = heads * hd // WIDE
    first_pos = lax.axis_index("sq") * pos_local
    scale = hd ** -0.5
    lowest = float(jnp.finfo(jnp.float32).min)

    def w_copy(k):
        src = w_kv_ref if k == 0 else w_query_ref.at[:, (k - 1) * WIDE : k * WIDE]
        return pltpu.make_async_copy(src, w_buf.at[k % W_SLOTS], w_sem.at[k])

    def rows_of(c):
        return pl.ds(pl.multiple_of(c * seqs, seqs), seqs)

    def read(c):
        return (
            pltpu.make_async_copy(k_ref.at[rows_of(c)], k_buf.at[rows_of(c)], in_sem.at[0, c]),
            pltpu.make_async_copy(v_ref.at[rows_of(c)], v_buf.at[rows_of(c)], in_sem.at[1, c]),
        )

    def write(c):
        return (
            pltpu.make_async_copy(k_buf.at[rows_of(c)], k_out_ref.at[rows_of(c)], out_sem.at[0, c]),
            pltpu.make_async_copy(v_buf.at[rows_of(c)], v_out_ref.at[rows_of(c)], out_sem.at[1, c]),
        )

    h_copy = pltpu.make_async_copy(hidden_ref, h_buf, h_sem)
    h_copy.start()
    for k in range(W_SLOTS):
        w_copy(k).start()
    q_buf[...] = jnp.zeros_like(q_buf)
    h_copy.wait()

    tiles = d_model // hd

    def lane_tiles(at):
        return [h_buf[at, t * hd : (t + 1) * hd].astype(jnp.float32) for t in range(tiles)]

    def add_up(values):
        while len(values) > 1:
            values = [sum(values[i : i + 2]) for i in range(0, len(values), 2)]
        return values[0]

    def rows16(r):
        return pl.ds(pl.multiple_of(r * 16, 16), 16)

    def sum_rows(r, _):
        stat_buf[rows16(r), :] = add_up(lane_tiles(rows16(r)))
        return 0

    def spread_rows(r, _):
        mean_val = stat_buf[rows16(r), :]
        stat_buf2[rows16(r), :] = add_up([(v - mean_val) * (v - mean_val) for v in lane_tiles(rows16(r))])
        return 0

    def norm_rows(r, _):
        at = rows16(r)
        mean_val, inv = stat_buf[at, :], stat_buf2[at, :]
        for t in range(tiles):
            cols = slice(t * hd, (t + 1) * hd)
            normed = (h_buf[at, cols].astype(jnp.float32) - mean_val) * inv
            h_buf[at, cols] = (normed * gain_ref[:, cols] + bias_ref[:, cols]).astype(jnp.bfloat16)
        return 0

    def row_means(buf):
        return jnp.broadcast_to(jnp.sum(buf[...], axis=-1, keepdims=True) * (1.0 / d_model), buf.shape)

    lax.fori_loop(0, batch // 16, sum_rows, 0)
    stat_buf[...] = row_means(stat_buf)
    lax.fori_loop(0, batch // 16, spread_rows, 0)
    stat_buf2[...] = lax.rsqrt(row_means(stat_buf2) + 1e-5)
    lax.fori_loop(0, batch // 16, norm_rows, 0)

    for k in range(blocks + 1):
        w_copy(k).wait()
        acc = jnp.dot(h_buf[...], w_buf[k % W_SLOTS], preferred_element_type=jnp.float32)
        if k == 0:
            acc = (acc + b_kv_ref[...]).astype(jnp.bfloat16).astype(jnp.float32)
            kv_buf[0] = acc[:, :hd]
            kv_buf[1] = acc[:, hd:]
        else:
            acc = (acc + b_query_ref[:, (k - 1) * WIDE : k * WIDE]).astype(jnp.bfloat16).astype(jnp.float32)
            for e in range(WIDE // hd):
                n = (k - 1) * (WIDE // hd) + e
                q_buf[pl.ds(n, batch, stride=16), :] = acc[:, e * hd : (e + 1) * hd]
        if k + W_SLOTS <= blocks:
            w_copy(k + W_SLOTS).start()
        if k + W_SLOTS == blocks:
            for c in range(steps):
                for copy in read(c):
                    copy.start()

    zero = jnp.zeros((16, hd), jnp.bfloat16)
    at_pos = lax.broadcasted_iota(jnp.int32, (16, pos_local), 1) + first_pos
    row = lax.broadcasted_iota(jnp.int32, (16, hd), 0)
    lane = lax.broadcasted_iota(jnp.int32, (16, hd), 1)
    pick_m = (lane == row) & (row < heads)
    pick_l = (lane == row + 64) & (row < heads)

    def take(c):
        for copy in read(c):
            copy.wait()
        for i in range(seqs):
            b = c * seqs + i
            pos = lens_ref[b] - first_pos
            base = pl.multiple_of(lax.div(jnp.clip(pos, 0, pos_local - 1), 16) * 16, 16)
            here = row + base == pos
            for which, buf in enumerate((k_buf, v_buf)):
                old = buf[b, pl.ds(base, 16), :].astype(jnp.float32)
                new = kv_buf[which, pl.ds(b, 1), :]
                buf[b, pl.ds(base, 16), :] = jnp.where(here, new, old).astype(jnp.bfloat16)
        for copy in write(c):
            copy.start()

    def score(c, s_buf):
        for i in range(0, seqs, 2):
            b = c * seqs + i
            q0 = q_buf[pl.ds(pl.multiple_of(b * 16, 16), 16), :].astype(jnp.bfloat16)
            q1 = q_buf[pl.ds(pl.multiple_of(b * 16 + 16, 16), 16), :].astype(jnp.bfloat16)
            q2 = jnp.concatenate([jnp.concatenate([q0, zero], axis=1), jnp.concatenate([zero, q1], axis=1)], axis=0)
            k2 = jnp.concatenate([k_buf[b], k_buf[b + 1]], axis=1)
            s2 = lax.dot_general(q2, k2, (((1,), (1,)), ((), ())), preferred_element_type=jnp.float32)
            s_buf[i * 16 : i * 16 + 32, :] = s2 * scale

    def combine(c, s_buf):
        for i in range(0, seqs, 2):
            b = c * seqs + i
            v2 = jnp.concatenate([v_buf[b], v_buf[b + 1]], axis=1)
            valid = jnp.concatenate([at_pos <= lens_ref[b], at_pos <= lens_ref[b + 1]], axis=0)
            s2 = jnp.where(valid, s_buf[i * 16 : i * 16 + 32, :], lowest)
            top = jnp.max(s2, axis=-1, keepdims=True)
            p2 = jnp.where(valid, jnp.exp(s2 - top), 0.0)
            total = jnp.sum(p2, axis=-1, keepdims=True)
            o2 = jnp.dot(p2.astype(jnp.bfloat16), v2, preferred_element_type=jnp.float32)
            for e in range(2):
                half = slice(e * 16, e * 16 + 16)
                stat = jnp.where(pick_m, top[half], 0.0) + jnp.where(pick_l, total[half], 0.0)
                stat = jnp.sum(stat, axis=0, keepdims=True)
                o_buf[(i + e) * 16 : (i + e) * 16 + 16, :] = jnp.where(row == heads, stat, o2[half, e * hd : (e + 1) * hd])
        for n in range(heads + 1):
            part_ref[rows_of(c), n * hd : (n + 1) * hd] = o_buf[pl.ds(n, seqs, stride=16), :]

    take(0)
    score(0, s_buf0)

    def two_steps(t, _):
        c = t * 2
        take(c + 1)
        score(c + 1, s_buf1)
        combine(c, s_buf0)
        take(c + 2)
        score(c + 2, s_buf0)
        combine(c + 1, s_buf1)
        return 0

    lax.fori_loop(0, steps // 2 - 1, two_steps, 0)
    take(steps - 1)
    score(steps - 1, s_buf1)
    combine(steps - 2, s_buf0)
    combine(steps - 1, s_buf1)

    def drain(c, _):
        for copy in write(c):
            copy.wait()
        return 0

    lax.fori_loop(0, steps, drain, 0)


def attend(hidden, cache_lens, k_cache, v_cache, ln_gain, ln_bias, w_query, b_query, w_kv, b_kv):
    batch, pos_local, hd = k_cache.shape
    d_model, q_width = w_query.shape
    heads = q_width // hd
    blocks, steps = q_width // WIDE, batch // ATTEND_SEQS
    f32, bf16, dma = jnp.float32, jnp.bfloat16, pltpu.SemaphoreType.DMA
    vmem, hbm = pl.BlockSpec(memory_space=pltpu.VMEM), pl.BlockSpec(memory_space=pl.ANY)
    return pl.pallas_call(
        functools.partial(attend_kernel, (batch, d_model, heads, pos_local)),
        out_shape=[
            pltpu.VMEM((batch, (heads + 1) * hd), f32),
            jax.ShapeDtypeStruct(k_cache.shape, bf16),
            jax.ShapeDtypeStruct(v_cache.shape, bf16),
        ],
        in_specs=[pl.BlockSpec(memory_space=pltpu.SMEM), hbm, vmem, vmem, vmem, vmem, hbm, hbm, hbm, hbm],
        out_specs=[vmem, hbm, hbm],
        scratch_shapes=[
            pltpu.VMEM((batch, d_model), bf16),
            pltpu.VMEM((W_SLOTS, d_model, WIDE), bf16),
            pltpu.VMEM((batch * 16, hd), f32),
            pltpu.VMEM((2, batch, hd), f32),
            pltpu.VMEM(k_cache.shape, bf16),
            pltpu.VMEM(v_cache.shape, bf16),
            pltpu.VMEM((ATTEND_SEQS * 16, hd), f32),
            pltpu.VMEM((ATTEND_SEQS * 16, pos_local), f32),
            pltpu.VMEM((ATTEND_SEQS * 16, pos_local), f32),
            pltpu.VMEM((batch, hd), f32),
            pltpu.VMEM((batch, hd), f32),
            dma,
            dma((blocks + 1,)),
            dma((2, steps)),
            dma((2, steps)),
        ],
        compiler_params=pltpu.CompilerParams(vmem_limit_bytes=60 * 1024 * 1024),
        name="attend",
    )(
        cache_lens,
        hidden,
        ln_gain.reshape(1, d_model),
        ln_bias.reshape(1, d_model),
        b_query.reshape(1, q_width),
        b_kv.reshape(1, 2 * hd),
        w_query,
        w_kv,
        k_cache,
        v_cache,
    )


def solution(mesh):
    nx, ny = mesh.shape["sq"] // 2, mesh.shape["tp"]

    def local_step(hidden, cache_lens, k_cache, v_cache, ln_gain, ln_bias, w_query, b_query, w_kv, b_kv, w_out, b_out):
        parts, key_new, val_new = attend(hidden, cache_lens, k_cache, v_cache, ln_gain, ln_bias, w_query, b_query, w_kv, b_kv)
        out_hidden = finish(parts, hidden, w_out, b_out, nx, ny)
        return out_hidden, key_new, val_new

    cache_spec = P("dp", "sq", None)
    row_spec = P("dp", None)
    in_specs = (row_spec, P("dp"), cache_spec, cache_spec, P(None), P(None), P(None, "tp"), P("tp"), P(None, None), P(None), P("tp", None), P(None))
    out_specs = (row_spec, cache_spec, cache_spec)
    return jax.shard_map(local_step, mesh=mesh, in_specs=in_specs, out_specs=out_specs, check_vma=False)
```

```python
import functools

import jax
import jax.numpy as jnp
from jax import lax
from jax.experimental import pallas as pl
from jax.experimental.pallas import tpu as pltpu
from jax.sharding import PartitionSpec as P

MESH = pl.DeviceIdType.MESH
LANES = 128
SEQS = 16
WIDE = 256
W_SLOTS = 3


def merge_into(dst, part_a, part_b, heads):
    stat_a, stat_b = part_a(heads), part_b(heads)
    top = jnp.maximum(stat_a, stat_b)
    exp_a, exp_b = jnp.exp(stat_a - top), jnp.exp(stat_b - top)
    sums = stat_a * pltpu.roll(exp_a, 64, 1) + stat_b * pltpu.roll(exp_b, 64, 1)
    lane = lax.broadcasted_iota(jnp.int32, top.shape, 1)
    stat = jnp.where(lane < 64, top, sums)
    for n in range(heads):
        dst[:, n * LANES : (n + 1) * LANES] = part_a(n) * exp_a[:, n : n + 1] + part_b(n) * exp_b[:, n : n + 1]
    dst[:, heads * LANES :] = stat


def decode_kernel(
    dims,
    lens_ref,
    gain_ref,
    bias_ref,
    b_query_ref,
    b_kv_ref,
    b_out_ref,
    hidden_ref,
    w_query_ref,
    w_kv_ref,
    w_out_ref,
    k_ref,
    v_ref,
    out_ref,
    kv_buf,
    cache_buf,
    w_buf,
    q_buf,
    part_buf,
    o_buf,
    s_buf0,
    s_buf1,
    stat_buf,
    stat_buf2,
    pair_buf,
    x_buf,
    att_buf,
    proj_buf,
    y_buf,
    hid_buf,
    gather_buf,
    h_sem,
    w_sem,
    in_sem,
    wo_sem,
    hid_sem,
    pair_send,
    pair_recv,
    x_send,
    x_recv,
    y_send,
    y_recv,
    g_send,
    g_recv,
    d_send,
    d_recv,
):
    nx, ny, heads, rows, cols, pos_local = dims
    k_buf, v_buf = cache_buf.at[0], cache_buf.at[1]
    batch, d_model = out_ref.shape
    hd, seqs = LANES, SEQS
    half = cols // 2
    depth = heads * hd
    steps = batch // seqs
    blocks = depth // WIDE
    sq = lax.axis_index("sq")
    y = lax.axis_index("tp")
    x = sq // 2
    core = sq % 2
    step = 1 - 2 * core
    first_pos = sq * pos_local
    scale = hd ** -0.5
    lowest = float(jnp.finfo(jnp.float32).min)

    def wrap(value, size):
        return lax.rem(value + 2 * size, size)

    x_fwd, x_bwd, x_opp = wrap(x + step, nx), wrap(x - step, nx), wrap(x + 2, nx)
    y_fwd, y_bwd, y_opp = wrap(y + step, ny), wrap(y - step, ny), wrap(y + 2, ny)
    to_pair = {"sq": x * 2 + 1 - core}
    to_x_fwd, to_x_bwd = {"sq": x_fwd * 2 + core}, {"sq": x_bwd * 2 + core}
    to_y_fwd, to_y_bwd = {"tp": y_fwd}, {"tp": y_bwd}

    barrier = pltpu.get_barrier_semaphore()
    for peer in (to_pair, to_x_fwd, to_x_bwd, to_y_fwd, to_y_bwd):
        pl.semaphore_signal(barrier, inc=1, device_id=peer, device_id_type=MESH)

    h_buf = out_ref

    def w_copy(k):
        src = w_kv_ref if k == 0 else w_query_ref.at[:, (k - 1) * WIDE : k * WIDE]
        return pltpu.make_async_copy(src, w_buf.at[k % W_SLOTS], w_sem.at[k])

    def block_row(i):
        slot, mine = i // 2, i % 2
        sign = step * (1 - 2 * mine)
        shift = 2 * ((3 - slot) // 3) + sign * (slot * (3 - slot) * (3 - 2 * slot) // 2)
        owner = wrap(x + shift, nx) * 2 + (1 - core) * (1 - mine) + core * mine
        return owner * rows

    def step_rows(c):
        per = rows // seqs
        return pl.multiple_of(block_row(c // per) + (c % per) * seqs, seqs)

    def read(c):
        at = pl.ds(step_rows(c), seqs)
        return (
            pltpu.make_async_copy(k_ref.at[at], k_buf.at[at], in_sem.at[0, c]),
            pltpu.make_async_copy(v_ref.at[at], v_buf.at[at], in_sem.at[1, c]),
        )

    h_copy = pltpu.make_async_copy(hidden_ref, h_buf, h_sem)
    h_copy.start()
    for k in range(W_SLOTS):
        w_copy(k).start()
    q_buf[...] = jnp.zeros_like(q_buf)
    h_copy.wait()

    tiles = d_model // hd

    def lane_tiles(at):
        return [h_buf[at, t * hd : (t + 1) * hd].astype(jnp.float32) for t in range(tiles)]

    def add_up(values):
        while len(values) > 1:
            values = [sum(values[i : i + 2]) for i in range(0, len(values), 2)]
        return values[0]

    def rows16(r):
        return pl.ds(pl.multiple_of(r * 16, 16), 16)

    def sum_rows(r, _):
        stat_buf[rows16(r), :] = add_up(lane_tiles(rows16(r)))
        return 0

    def spread_rows(r, _):
        mean_val = stat_buf[rows16(r), :]
        stat_buf2[rows16(r), :] = add_up([(v - mean_val) * (v - mean_val) for v in lane_tiles(rows16(r))])
        return 0

    def norm_rows(r, _):
        at = rows16(r)
        mean_val, inv = stat_buf[at, :], stat_buf2[at, :]
        for t in range(tiles):
            cols = slice(t * hd, (t + 1) * hd)
            normed = (h_buf[at, cols].astype(jnp.float32) - mean_val) * inv
            h_buf[at, cols] = (normed * gain_ref[:, cols] + bias_ref[:, cols]).astype(jnp.bfloat16)
        return 0

    def row_means(buf):
        return jnp.broadcast_to(jnp.sum(buf[...], axis=-1, keepdims=True) * (1.0 / d_model), buf.shape)

    lax.fori_loop(0, batch // 16, sum_rows, 0)
    stat_buf[...] = row_means(stat_buf)
    lax.fori_loop(0, batch // 16, spread_rows, 0)
    stat_buf2[...] = lax.rsqrt(row_means(stat_buf2) + 1e-5)
    lax.fori_loop(0, batch // 16, norm_rows, 0)

    units = ((0, 0), (0, 1), (1, 0), (2, 0), (3, 0), (1, 1), (2, 1), (3, 1))
    y_order = (y_opp, y_bwd, y_fwd, y)
    per_unit, per_slot = half // WIDE, d_model // depth

    def wo_place(u, j):
        at = (u % 4) * per_unit + j
        return at // per_slot, slice((at % per_slot) * depth, (at % per_slot + 1) * depth)

    def wo_copies(u):
        target, h = units[u]
        copies = []
        for j in range(per_unit):
            col = pl.multiple_of(y_order[target] * cols + h * half + j * WIDE, WIDE)
            slot, at = wo_place(u, j)
            copies.append(
                pltpu.make_async_copy(w_out_ref.at[:, pl.ds(col, WIDE)], w_buf.at[slot, at, :], wo_sem.at[u, j])
            )
        return copies

    for k in range(blocks + 1):
        w_copy(k).wait()
        acc = jnp.dot(h_buf[...], w_buf[k % W_SLOTS], preferred_element_type=jnp.float32)
        if k == 0:
            acc = (acc + b_kv_ref[...]).astype(jnp.bfloat16).astype(jnp.float32)
            kv_buf[0] = acc[:, :hd]
            kv_buf[1] = acc[:, hd:]
        else:
            bias = b_query_ref[(k - 1) * WIDE : k * WIDE].reshape(1, WIDE)
            acc = (acc + bias).astype(jnp.bfloat16).astype(jnp.float32)
            for e in range(WIDE // hd):
                n = (k - 1) * (WIDE // hd) + e
                q_buf[pl.ds(n, batch, stride=16), :] = acc[:, e * hd : (e + 1) * hd]
        if k + W_SLOTS <= blocks:
            w_copy(k + W_SLOTS).start()
        if k + W_SLOTS == blocks:
            for c in range(steps):
                for copy in read(c):
                    copy.start()
    hid_copy = pltpu.make_async_copy(
        hidden_ref.at[pl.ds(pl.multiple_of(sq * rows, rows), rows), pl.ds(pl.multiple_of(y * cols, cols), cols)], hid_buf, hid_sem
    )
    hid_copy.start()
    for u in range(4):
        for copy in wo_copies(u):
            copy.start()

    zero = jnp.zeros((16, hd), jnp.bfloat16)
    at_pos = lax.broadcasted_iota(jnp.int32, (16, pos_local), 1) + first_pos
    row = lax.broadcasted_iota(jnp.int32, (16, hd), 0)
    lane = lax.broadcasted_iota(jnp.int32, (16, hd), 1)
    pick_m = (lane == row) & (row < heads)
    pick_l = (lane == row + 64) & (row < heads)

    def score(c, s_buf):
        for copy in read(c):
            copy.wait()
        b0 = step_rows(c)
        for i in range(0, seqs, 2):
            q0 = q_buf[pl.ds(pl.multiple_of(b0 * 16 + i * 16, 16), 16), :].astype(jnp.bfloat16)
            q1 = q_buf[pl.ds(pl.multiple_of(b0 * 16 + i * 16 + 16, 16), 16), :].astype(jnp.bfloat16)
            q2 = jnp.concatenate([jnp.concatenate([q0, zero], axis=1), jnp.concatenate([zero, q1], axis=1)], axis=0)
            k2 = jnp.concatenate([k_buf[b0 + i], k_buf[b0 + i + 1]], axis=1)
            s2 = lax.dot_general(q2, k2, (((1,), (1,)), ((), ())), preferred_element_type=jnp.float32)
            s_buf[i * 16 : i * 16 + 32, :] = s2 * scale

    def combine(c, s_buf):
        b0 = step_rows(c)
        for i in range(0, seqs, 2):
            v2 = jnp.concatenate([v_buf[b0 + i], v_buf[b0 + i + 1]], axis=1)
            valid = jnp.concatenate([at_pos < lens_ref[b0 + i], at_pos < lens_ref[b0 + i + 1]], axis=0)
            s2 = jnp.where(valid, s_buf[i * 16 : i * 16 + 32, :], lowest)
            top = jnp.max(s2, axis=-1, keepdims=True)
            p2 = jnp.where(valid, jnp.exp(s2 - top), 0.0)
            total = jnp.sum(p2, axis=-1, keepdims=True)
            o2 = jnp.dot(p2.astype(jnp.bfloat16), v2, preferred_element_type=jnp.float32)
            for e in range(2):
                part = slice(e * 16, e * 16 + 16)
                stat = jnp.where(pick_m, top[part], 0.0) + jnp.where(pick_l, total[part], 0.0)
                stat = jnp.sum(stat, axis=0, keepdims=True)
                o_buf[(i + e) * 16 : (i + e) * 16 + 16, :] = jnp.where(row == heads, stat, o2[part, e * hd : (e + 1) * hd])
        for n in range(heads + 1):
            part_buf[pl.ds(b0, seqs), n * hd : (n + 1) * hd] = o_buf[pl.ds(n, seqs, stride=16), :]

    sends = []

    def remote(src, dst, ssem, rsem, peer):
        return pltpu.make_async_remote_copy(
            src_ref=src, dst_ref=dst, send_sem=ssem, recv_sem=rsem, device_id=peer, device_id_type=MESH
        )

    def send(*args):
        copy = remote(*args)
        copy.start()
        sends.append(copy)
        return copy

    def part_at(i):
        return pl.ds(pl.multiple_of(block_row(i), rows), rows)

    def of_part(i):
        return lambda n: part_buf[part_at(i), n * hd : (n + 1) * hd]

    def of(ref):
        return lambda n: ref[:, n * hd : (n + 1) * hd]

    pair = [remote(part_buf.at[part_at(2 * k), :], pair_buf.at[k], pair_send.at[k], pair_recv.at[k], to_pair) for k in range(4)]
    x_o = remote(pair_buf.at[0], x_buf.at[0], x_send.at[0], x_recv.at[0], to_x_fwd)
    x_b = remote(pair_buf.at[1], x_buf.at[1], x_send.at[1], x_recv.at[1], to_x_bwd)
    x_a = remote(pair_buf.at[2], x_buf.at[2], x_send.at[2], x_recv.at[2], to_x_fwd)
    sends.extend(pair + [x_o, x_b, x_a])

    def after_block(i):
        slot = i // 2
        if i % 2 == 0:
            pair[slot].start()
            return
        pair[slot].wait_recv()
        merge_into(pair_buf.at[slot], of_part(i), of(pair_buf.at[slot]), heads)
        if slot == 0:
            x_o.start()
        elif slot == 1:
            x_b.start()
        elif slot == 2:
            x_o.wait_recv()
            merge_into(pair_buf.at[2], of(pair_buf.at[2]), of(x_buf.at[0]), heads)
            x_a.start()

    pl.semaphore_wait(barrier, 5)
    score(0, s_buf0)

    def one_block(i, _):
        c = i * 2
        score(c + 1, s_buf1)
        combine(c, s_buf0)
        score(c + 2, s_buf0)
        combine(c + 1, s_buf1)
        for j in range(7):
            pl.when(i == j)(functools.partial(after_block, j))
        return 0

    lax.fori_loop(0, steps // 2 - 1, one_block, 0)
    score(steps - 1, s_buf1)
    combine(steps - 2, s_buf0)
    combine(steps - 1, s_buf1)

    own = pl.multiple_of(sq * rows, rows)
    k_new, v_new = kv_buf[0, pl.ds(own, rows), :], kv_buf[1, pl.ds(own, rows), :]
    new_lane = lax.broadcasted_iota(jnp.int32, (rows, hd), 1)
    new_stat = jnp.where((new_lane >= 64) & (new_lane < 64 + heads), 1.0, 0.0)
    for n in range(heads):
        s_new = jnp.sum(q_buf[pl.ds(own * 16 + n, rows, stride=16), :] * k_new, axis=-1, keepdims=True) * scale
        new_stat = jnp.where(new_lane == n, s_new, new_stat)

    after_block(7)
    total = pair_buf.at[3]
    merge_into(total, of(total), lambda n: new_stat if n == heads else v_new, heads)
    x_b.wait_recv()
    merge_into(total, of(total), of(x_buf.at[1]), heads)
    x_a.wait_recv()
    merge_into(total, of(total), of(x_buf.at[2]), heads)
    stat = total[:, depth:]
    for n in range(heads):
        block = slice(n * hd, (n + 1) * hd)
        att_buf[:, block] = (total[:, block] / stat[:, 64 + n : 65 + n]).astype(jnp.bfloat16)

    def project(u):
        for copy in wo_copies(u):
            copy.wait()
        parts = []
        for j in range(per_unit):
            slot, at = wo_place(u, j)
            parts.append(jnp.dot(att_buf[...], w_buf[slot, at, :], preferred_element_type=jnp.float32))
        return jnp.concatenate(parts, axis=1)

    def refill(u):
        if u + 4 < len(units):
            for copy in wo_copies(u + 4):
                copy.start()

    y_o, y_b, y_a = [None, None], [None, None], [None, None]
    for u, (target, h) in enumerate(units):
        if target < 2:
            proj_buf[target, h] = project(u)
            refill(u)
            peer = (to_y_fwd, to_y_bwd)[target]
            copy = send(proj_buf.at[target, h], y_buf.at[target, h], y_send.at[target, h], y_recv.at[target, h], peer)
            (y_o, y_b)[target][h] = copy
        elif target == 2:
            fwd_part = project(u)
            refill(u)
            y_o[h].wait_recv()
            proj_buf[2, h] = fwd_part + y_buf[0, h]
            y_a[h] = send(proj_buf.at[2, h], y_buf.at[2, h], y_send.at[2, h], y_recv.at[2, h], to_y_fwd)
        else:
            if h == 0:
                hid_copy.wait()
            own_cols = pl.ds(pl.multiple_of(y * cols + h * half, half), half)
            proj_buf[3, h] = project(u) + hid_buf[:, h * half : (h + 1) * half].astype(jnp.float32) + b_out_ref[:, own_cols]
            refill(u)

    def place(xt, yt, ct, h):
        row = pl.multiple_of((xt * 2 + ct) * rows, rows)
        col = pl.multiple_of(yt * cols + h * half, half)
        return pl.ds(row, rows), pl.ds(col, half)

    xs = (x, x_bwd, x_fwd, x_opp)
    ys = (y, y_bwd, y_fwd, y_opp)
    x_peers, y_peers = (to_x_fwd, to_x_bwd), (to_y_fwd, to_y_bwd)
    gathers = {}
    pairs = {}

    def spot(h, first, second, ct=None):
        ct = core if ct is None else ct
        if h == 0:
            return place(xs[first], ys[second], ct, h)
        return place(xs[second], ys[first], ct, h)

    def piece(h, first, second):
        return gather_buf.at[spot(h, first, second)]

    def ring_send(h, first, second, slot, phase):
        peers = (x_peers, y_peers) if h == 0 else (y_peers, x_peers)
        peer = peers[phase][1 if slot == 2 else 0]
        index = slot - 1 if phase == 0 else 3 + first * 3 + slot - 1
        key = (h, phase, first if phase else 0, slot)
        ref = piece(h, first, second)
        gathers[key] = send(ref, ref, g_send.at[h, index], g_recv.at[h, index], peer)

    def pair_forward(h, first, second):
        ref = piece(h, first, second)
        index = first * 4 + second
        pairs[(h, first, second)] = send(ref, ref, d_send.at[h, index], d_recv.at[h, index], to_pair)

    def convert(where):
        out_ref[where] = gather_buf[where].astype(jnp.bfloat16)

    def mirrored(slot):
        return (0, 2, 1, 3)[slot]

    todo = []

    def drain(limit):
        while len(todo) > limit:
            h, first, second = todo.pop(0)
            pairs[(h, first, second)].wait_recv()
            convert(spot(h, mirrored(first), mirrored(second), 1 - core))

    def have(h, first, second):
        pair_forward(h, first, second)
        convert(spot(h, first, second))
        todo.append((h, first, second))
        drain(2)

    for h in range(2):
        y_b[h].wait_recv()
        part = proj_buf[3, h] + y_buf[1, h]
        y_a[h].wait_recv()
        gather_buf[spot(h, 0, 0)] = part + y_buf[2, h]
        ring_send(h, 0, 0, 1, 0)
        ring_send(h, 0, 0, 2, 0)
        pair_forward(h, 0, 0)
    for h in range(2):
        ring_send(h, 0, 0, 1, 1)
        ring_send(h, 0, 0, 2, 1)
        convert(spot(h, 0, 0))
        todo.append((h, 0, 0))

    def arrived(h, first, second):
        if second == 0:
            gathers[(h, 0, 0, first)].wait_recv()
            if first == 1:
                ring_send(h, 1, 0, 3, 0)
            ring_send(h, first, 0, 1, 1)
            ring_send(h, first, 0, 2, 1)
        else:
            gathers[(h, 1, first, second)].wait_recv()
            if second == 1:
                ring_send(h, first, 1, 3, 1)
        have(h, first, second)

    order = [(1, 0), (2, 0), (0, 1), (0, 2), (3, 0), (1, 1), (0, 3), (2, 1), (1, 2), (1, 3), (2, 2), (3, 1), (2, 3), (3, 2), (3, 3)]
    for first, second in order:
        for h in range(2):
            arrived(h, first, second)
    drain(0)
    for copy in sends:
        copy.wait_send()


def store_kernel(lens_ref, y_ref, kv_ref, cache_ref, y_out_ref, cache_buf, k_out_ref, v_out_ref, y_sem, out_sem):
    k_buf, v_buf = cache_buf.at[0], cache_buf.at[1]
    batch, pos_local, hd = k_buf.shape
    first_pos = lax.axis_index("sq") * pos_local
    row = lax.broadcasted_iota(jnp.int32, (16, hd), 0)
    pairs = ((k_buf, k_out_ref), (v_buf, v_out_ref))

    def write(c):
        at = pl.ds(pl.multiple_of(c * SEQS, SEQS), SEQS)
        return [pltpu.make_async_copy(buf.at[at], out.at[at], out_sem.at[w, c]) for w, (buf, out) in enumerate(pairs)]

    def replace(c, _):
        for i in range(SEQS):
            b = c * SEQS + i
            pos = lens_ref[b] - first_pos
            base = pl.multiple_of(lax.div(jnp.clip(pos, 0, pos_local - 1), 16) * 16, 16)
            here = row + base == pos
            for which, (buf, _) in enumerate(pairs):
                old = buf[b, pl.ds(base, 16), :].astype(jnp.float32)
                new = kv_ref[which, pl.ds(b, 1), :]
                buf[b, pl.ds(base, 16), :] = jnp.where(here, new, old).astype(jnp.bfloat16)
        for copy in write(c):
            copy.start()
        return 0

    def drain(c, _):
        for copy in write(c):
            copy.wait()
        return 0

    y_copy = pltpu.make_async_copy(y_ref, y_out_ref, y_sem)
    y_copy.start()
    lax.fori_loop(0, batch // SEQS, replace, 0)
    lax.fori_loop(0, batch // SEQS, drain, 0)
    y_copy.wait()


def solution(mesh):
    nx, ny = mesh.shape["sq"] // 2, mesh.shape["tp"]

    def local_step(hidden, cache_lens, k_cache, v_cache, ln_gain, ln_bias, w_query, b_query, w_kv, b_kv, w_out, b_out):
        batch, pos_local, hd = k_cache.shape
        d_model, depth = w_query.shape
        heads = depth // hd
        rows, cols = batch // (2 * nx), d_model // ny
        width = depth + hd
        half = cols // 2
        f32, bf16, dma, vmem_buf = jnp.float32, jnp.bfloat16, pltpu.SemaphoreType.DMA, pltpu.VMEM
        smem, vmem, hbm = (pl.BlockSpec(memory_space=m) for m in (pltpu.SMEM, pltpu.VMEM, pl.ANY))
        out_hidden, key_val, caches = pl.pallas_call(
            functools.partial(decode_kernel, (nx, ny, heads, rows, cols, pos_local)),
            out_shape=[
                vmem_buf((batch, d_model), bf16),
                vmem_buf((2, batch, hd), f32),
                vmem_buf((2,) + k_cache.shape, bf16),
            ],
            in_specs=[smem] + [vmem] * 5 + [hbm] * 6,
            out_specs=[vmem] * 3,
            scratch_shapes=[
                vmem_buf((W_SLOTS, d_model, WIDE), bf16),
                vmem_buf((batch * 16, hd), f32),
                vmem_buf((batch, width), f32),
                vmem_buf((SEQS * 16, hd), f32),
                vmem_buf((SEQS * 16, pos_local), f32),
                vmem_buf((SEQS * 16, pos_local), f32),
                vmem_buf((batch, hd), f32),
                vmem_buf((batch, hd), f32),
                vmem_buf((4, rows, width), f32),
                vmem_buf((3, rows, width), f32),
                vmem_buf((rows, depth), bf16),
                vmem_buf((4, 2, rows, half), f32),
                vmem_buf((3, 2, rows, half), f32),
                vmem_buf((rows, cols), bf16),
                vmem_buf((batch, d_model), f32),
                dma,
                dma((depth // WIDE + 1,)),
                dma((2, batch // SEQS)),
                dma((8, half // WIDE)),
                dma,
                dma((4,)),
                dma((4,)),
                dma((3,)),
                dma((3,)),
                dma((3, 2)),
                dma((3, 2)),
                dma((2, 15)),
                dma((2, 15)),
                dma((2, 16)),
                dma((2, 16)),
            ],
            compiler_params=pltpu.CompilerParams(collective_id=0, has_side_effects=True, vmem_limit_bytes=24 * 1024 * 1024),
            name="decode",
        )(
            cache_lens,
            ln_gain.reshape(1, d_model),
            ln_bias.reshape(1, d_model),
            b_query,
            b_kv.reshape(1, 2 * hd),
            b_out.reshape(1, d_model),
            hidden,
            w_query,
            w_kv,
            w_out,
            k_cache,
            v_cache,
        )
        out_hidden, _, key_new, val_new = pl.pallas_call(
            store_kernel,
            out_shape=[
                jax.ShapeDtypeStruct((batch, d_model), bf16),
                vmem_buf((2,) + k_cache.shape, bf16),
                jax.ShapeDtypeStruct(k_cache.shape, bf16),
                jax.ShapeDtypeStruct(v_cache.shape, bf16),
            ],
            in_specs=[smem] + [vmem] * 3,
            out_specs=[hbm, vmem, hbm, hbm],
            input_output_aliases={3: 1},
            scratch_shapes=[dma, dma((2, batch // SEQS))],
            compiler_params=pltpu.CompilerParams(vmem_limit_bytes=1 * 1024 * 1024),
            name="store",
        )(cache_lens, out_hidden, key_val, caches)
        return out_hidden, key_new, val_new

    cache_spec = P("dp", "sq", None)
    row_spec = P("dp", None)
    in_specs = (row_spec, P("dp"), cache_spec, cache_spec, P(None), P(None), P(None, "tp"), P("tp"), P(None, None), P(None), P("tp", None), P(None))
    out_specs = (row_spec, cache_spec, cache_spec)
    return jax.shard_map(local_step, mesh=mesh, in_specs=in_specs, out_specs=out_specs, check_vma=False)
```

```python
import functools

import jax
import jax.numpy as jnp
from jax import lax
from jax.experimental import pallas as pl
from jax.experimental.pallas import tpu as pltpu
from jax.sharding import PartitionSpec as P

MESH = pl.DeviceIdType.MESH
LANES = 128
SEQS = 16
TALL = 1024
WIDE = 512
EARLY = 6
W_SLOTS = 3


def merge_into(dst, part_a, part_b, heads):
    stat_a, stat_b = part_a(heads), part_b(heads)
    top = jnp.maximum(stat_a, stat_b)
    exp_a, exp_b = jnp.exp(stat_a - top), jnp.exp(stat_b - top)
    sums = stat_a * pltpu.roll(exp_a, 64, 1) + stat_b * pltpu.roll(exp_b, 64, 1)
    lane = lax.broadcasted_iota(jnp.int32, top.shape, 1)
    stat = jnp.where(lane < 64, top, sums)
    for n in range(heads):
        dst[:, n * LANES : (n + 1) * LANES] = part_a(n) * exp_a[:, n : n + 1] + part_b(n) * exp_b[:, n : n + 1]
    dst[:, heads * LANES :] = stat


def decode_kernel(
    dims,
    lens_ref,
    gain_ref,
    bias_ref,
    b_query_ref,
    b_kv_ref,
    b_out_ref,
    hidden_ref,
    w_query_ref,
    w_kv_ref,
    w_out_ref,
    k_ref,
    v_ref,
    out_ref,
    kv_buf,
    cache_buf,
    w_buf,
    wkv_buf,
    q_buf,
    part_buf,
    o_buf,
    s_buf0,
    s_buf1,
    stat_buf,
    stat_buf2,
    pair_buf,
    x_buf,
    att_buf,
    proj_buf,
    y_buf,
    hid_buf,
    gather_buf,
    h_sem,
    w_sem,
    in_sem,
    wo_sem,
    hid_sem,
    pair_send,
    pair_recv,
    x_send,
    x_recv,
    y_send,
    y_recv,
    g_send,
    g_recv,
    d_send,
    d_recv,
):
    nx, ny, heads, rows, cols, pos_local = dims
    k_buf, v_buf = cache_buf.at[0], cache_buf.at[1]
    batch, d_model = out_ref.shape
    hd, seqs = LANES, SEQS
    half = cols // 2
    depth = heads * hd
    steps = batch // seqs
    blocks = d_model // TALL
    sq = lax.axis_index("sq")
    y = lax.axis_index("tp")
    x = sq // 2
    core = sq % 2
    step = 1 - 2 * core
    first_pos = sq * pos_local
    scale = hd ** -0.5
    lowest = float(jnp.finfo(jnp.float32).min)

    def wrap(value, size):
        return lax.rem(value + 2 * size, size)

    x_fwd, x_bwd, x_opp = wrap(x + step, nx), wrap(x - step, nx), wrap(x + 2, nx)
    y_fwd, y_bwd, y_opp = wrap(y + step, ny), wrap(y - step, ny), wrap(y + 2, ny)
    to_pair = {"sq": x * 2 + 1 - core}
    to_x_fwd, to_x_bwd = {"sq": x_fwd * 2 + core}, {"sq": x_bwd * 2 + core}
    to_y_fwd, to_y_bwd = {"tp": y_fwd}, {"tp": y_bwd}

    barrier = pltpu.get_barrier_semaphore()
    for peer in (to_pair, to_x_fwd, to_x_bwd, to_y_fwd, to_y_bwd):
        pl.semaphore_signal(barrier, inc=1, device_id=peer, device_id_type=MESH)

    h_buf = out_ref

    def w_copies(k):
        slot, at = k % W_SLOTS, pl.ds(k * TALL, TALL)
        return (
            pltpu.make_async_copy(w_query_ref.at[at, :], w_buf.at[pl.ds(slot * TALL, TALL), :], w_sem.at[0, k]),
            pltpu.make_async_copy(w_kv_ref.at[at, :], wkv_buf.at[slot], w_sem.at[1, k]),
        )

    def block_row(i):
        slot, mine = i // 2, i % 2
        sign = step * (1 - 2 * mine)
        shift = 2 * ((3 - slot) // 3) + sign * (slot * (3 - slot) * (3 - 2 * slot) // 2)
        owner = wrap(x + shift, nx) * 2 + (1 - core) * (1 - mine) + core * mine
        return owner * rows

    def step_rows(c):
        per = rows // seqs
        return pl.multiple_of(block_row(c // per) + (c % per) * seqs, seqs)

    def read(c):
        at = pl.ds(step_rows(c), seqs)
        return (
            pltpu.make_async_copy(k_ref.at[at], k_buf.at[at], in_sem.at[0, c]),
            pltpu.make_async_copy(v_ref.at[at], v_buf.at[at], in_sem.at[1, c]),
        )

    h_copy = pltpu.make_async_copy(hidden_ref, h_buf, h_sem)
    h_copy.start()
    for k in range(W_SLOTS):
        for copy in w_copies(k):
            copy.start()
    for c in range(EARLY):
        for copy in read(c):
            copy.start()
    q_buf[...] = jnp.zeros_like(q_buf)
    h_copy.wait()

    tiles = d_model // hd

    def lane_tiles(at):
        return [h_buf[at, t * hd : (t + 1) * hd].astype(jnp.float32) for t in range(tiles)]

    def add_up(values):
        while len(values) > 1:
            values = [sum(values[i : i + 2]) for i in range(0, len(values), 2)]
        return values[0]

    def rows16(r):
        return pl.ds(pl.multiple_of(r * 16, 16), 16)

    def sum_rows(r, _):
        stat_buf[rows16(r), :] = add_up(lane_tiles(rows16(r)))
        return 0

    def spread_rows(r, _):
        mean_val = stat_buf[rows16(r), :]
        stat_buf2[rows16(r), :] = add_up([(v - mean_val) * (v - mean_val) for v in lane_tiles(rows16(r))])
        return 0

    def norm_rows(r, _):
        at = rows16(r)
        mean_val, inv = stat_buf[at, :], stat_buf2[at, :]
        for t in range(tiles):
            cols = slice(t * hd, (t + 1) * hd)
            normed = (h_buf[at, cols].astype(jnp.float32) - mean_val) * inv
            h_buf[at, cols] = (normed * gain_ref[:, cols] + bias_ref[:, cols]).astype(jnp.bfloat16)
        return 0

    def row_means(buf):
        return jnp.broadcast_to(jnp.sum(buf[...], axis=-1, keepdims=True) * (1.0 / d_model), buf.shape)

    lax.fori_loop(0, batch // 16, sum_rows, 0)
    stat_buf[...] = row_means(stat_buf)
    lax.fori_loop(0, batch // 16, spread_rows, 0)
    stat_buf2[...] = lax.rsqrt(row_means(stat_buf2) + 1e-5)
    lax.fori_loop(0, batch // 16, norm_rows, 0)

    y_order = (y_opp, y_bwd, y_fwd, y)

    def wo_copy(k):
        src = w_out_ref.at[:, pl.ds(pl.multiple_of(y_order[k] * cols, cols), cols)]
        return pltpu.make_async_copy(src, w_buf.at[pl.ds((k % 2) * depth, depth), :], wo_sem.at[k])

    for k in range(blocks):
        for copy in w_copies(k):
            copy.wait()
        h_cols, slot = h_buf[:, k * TALL : (k + 1) * TALL], k % W_SLOTS
        kv = jnp.dot(h_cols, wkv_buf[slot], preferred_element_type=jnp.float32)
        for e in range(2):
            part = kv[:, e * hd : (e + 1) * hd]
            kv_buf[e] = part if k == 0 else kv_buf[e] + part
        for n in range(0, depth, WIDE):
            w_block = w_buf[slot * TALL : (slot + 1) * TALL, n : n + WIDE]
            part = jnp.dot(h_cols, w_block, preferred_element_type=jnp.float32)
            part_buf[:, n : n + WIDE] = part if k == 0 else part_buf[:, n : n + WIDE] + part
        if k + W_SLOTS < blocks:
            for copy in w_copies(k + W_SLOTS):
                copy.start()
        if k + W_SLOTS == blocks - 1:
            for c in range(EARLY, steps):
                for copy in read(c):
                    copy.start()
    for e in range(2):
        new = kv_buf[e] + b_kv_ref[:, e * hd : (e + 1) * hd]
        kv_buf[e] = new.astype(jnp.bfloat16).astype(jnp.float32)
    for n in range(heads):
        new = part_buf[:, n * hd : (n + 1) * hd] + b_query_ref[n * hd : (n + 1) * hd].reshape(1, hd)
        q_buf[pl.ds(n, batch, stride=16), :] = new.astype(jnp.bfloat16).astype(jnp.float32)
    hid_copy = pltpu.make_async_copy(
        hidden_ref.at[pl.ds(pl.multiple_of(sq * rows, rows), rows), pl.ds(pl.multiple_of(y * cols, cols), cols)], hid_buf, hid_sem
    )
    hid_copy.start()
    for k in range(2):
        wo_copy(k).start()

    zero = jnp.zeros((16, hd), jnp.bfloat16)
    at_pos = lax.broadcasted_iota(jnp.int32, (16, pos_local), 1) + first_pos
    row = lax.broadcasted_iota(jnp.int32, (16, hd), 0)
    lane = lax.broadcasted_iota(jnp.int32, (16, hd), 1)
    pick_m = (lane == row) & (row < heads)
    pick_l = (lane == row + 64) & (row < heads)

    def score(c, s_buf):
        for copy in read(c):
            copy.wait()
        b0 = step_rows(c)
        for i in range(0, seqs, 2):
            q0 = q_buf[pl.ds(pl.multiple_of(b0 * 16 + i * 16, 16), 16), :].astype(jnp.bfloat16)
            q1 = q_buf[pl.ds(pl.multiple_of(b0 * 16 + i * 16 + 16, 16), 16), :].astype(jnp.bfloat16)
            q2 = jnp.concatenate([jnp.concatenate([q0, zero], axis=1), jnp.concatenate([zero, q1], axis=1)], axis=0)
            k2 = jnp.concatenate([k_buf[b0 + i], k_buf[b0 + i + 1]], axis=1)
            s2 = lax.dot_general(q2, k2, (((1,), (1,)), ((), ())), preferred_element_type=jnp.float32)
            s_buf[i * 16 : i * 16 + 32, :] = s2 * scale

    def combine(c, s_buf):
        b0 = step_rows(c)
        for i in range(0, seqs, 2):
            v2 = jnp.concatenate([v_buf[b0 + i], v_buf[b0 + i + 1]], axis=1)
            valid = jnp.concatenate([at_pos < lens_ref[b0 + i], at_pos < lens_ref[b0 + i + 1]], axis=0)
            s2 = jnp.where(valid, s_buf[i * 16 : i * 16 + 32, :], lowest)
            top = jnp.max(s2, axis=-1, keepdims=True)
            p2 = jnp.where(valid, jnp.exp(s2 - top), 0.0)
            total = jnp.sum(p2, axis=-1, keepdims=True)
            o2 = jnp.dot(p2.astype(jnp.bfloat16), v2, preferred_element_type=jnp.float32)
            for e in range(2):
                part = slice(e * 16, e * 16 + 16)
                stat = jnp.where(pick_m, top[part], 0.0) + jnp.where(pick_l, total[part], 0.0)
                stat = jnp.sum(stat, axis=0, keepdims=True)
                o_buf[(i + e) * 16 : (i + e) * 16 + 16, :] = jnp.where(row == heads, stat, o2[part, e * hd : (e + 1) * hd])
        for n in range(heads + 1):
            part_buf[pl.ds(b0, seqs), n * hd : (n + 1) * hd] = o_buf[pl.ds(n, seqs, stride=16), :]

    sends = []

    def remote(src, dst, ssem, rsem, peer):
        return pltpu.make_async_remote_copy(
            src_ref=src, dst_ref=dst, send_sem=ssem, recv_sem=rsem, device_id=peer, device_id_type=MESH
        )

    def send(*args):
        copy = remote(*args)
        copy.start()
        sends.append(copy)
        return copy

    def part_at(i):
        return pl.ds(pl.multiple_of(block_row(i), rows), rows)

    def of_part(i):
        return lambda n: part_buf[part_at(i), n * hd : (n + 1) * hd]

    def of(ref):
        return lambda n: ref[:, n * hd : (n + 1) * hd]

    pair = [remote(part_buf.at[part_at(2 * k), :], pair_buf.at[k], pair_send.at[k], pair_recv.at[k], to_pair) for k in range(4)]
    x_o = remote(pair_buf.at[0], x_buf.at[0], x_send.at[0], x_recv.at[0], to_x_fwd)
    x_b = remote(pair_buf.at[1], x_buf.at[1], x_send.at[1], x_recv.at[1], to_x_bwd)
    x_a = remote(pair_buf.at[2], x_buf.at[2], x_send.at[2], x_recv.at[2], to_x_fwd)
    sends.extend(pair + [x_o, x_b, x_a])

    def after_block(i):
        slot = i // 2
        if i % 2 == 0:
            pair[slot].start()
            return
        pair[slot].wait_recv()
        merge_into(pair_buf.at[slot], of_part(i), of(pair_buf.at[slot]), heads)
        if slot == 0:
            x_o.start()
        elif slot == 1:
            x_b.start()
        elif slot == 2:
            x_o.wait_recv()
            merge_into(pair_buf.at[2], of(pair_buf.at[2]), of(x_buf.at[0]), heads)
            x_a.start()

    pl.semaphore_wait(barrier, 5)
    score(0, s_buf0)

    def one_block(i, _):
        c = i * 2
        score(c + 1, s_buf1)
        combine(c, s_buf0)
        score(c + 2, s_buf0)
        combine(c + 1, s_buf1)
        for j in range(7):
            pl.when(i == j)(functools.partial(after_block, j))
        return 0

    lax.fori_loop(0, steps // 2 - 1, one_block, 0)
    score(steps - 1, s_buf1)
    combine(steps - 2, s_buf0)
    combine(steps - 1, s_buf1)

    own = pl.multiple_of(sq * rows, rows)
    k_new, v_new = kv_buf[0, pl.ds(own, rows), :], kv_buf[1, pl.ds(own, rows), :]
    new_lane = lax.broadcasted_iota(jnp.int32, (rows, hd), 1)
    new_stat = jnp.where((new_lane >= 64) & (new_lane < 64 + heads), 1.0, 0.0)
    for n in range(heads):
        s_new = jnp.sum(q_buf[pl.ds(own * 16 + n, rows, stride=16), :] * k_new, axis=-1, keepdims=True) * scale
        new_stat = jnp.where(new_lane == n, s_new, new_stat)

    after_block(7)
    total = pair_buf.at[3]
    merge_into(total, of(total), lambda n: new_stat if n == heads else v_new, heads)
    x_b.wait_recv()
    merge_into(total, of(total), of(x_buf.at[1]), heads)
    x_a.wait_recv()
    merge_into(total, of(total), of(x_buf.at[2]), heads)
    stat = total[:, depth:]
    for n in range(heads):
        block = slice(n * hd, (n + 1) * hd)
        att_buf[:, block] = (total[:, block] / stat[:, 64 + n : 65 + n]).astype(jnp.bfloat16)

    def project(k, h):
        w_block = w_buf[(k % 2) * depth : (k % 2 + 1) * depth, h * half : (h + 1) * half]
        return jnp.dot(att_buf[...], w_block, preferred_element_type=jnp.float32)

    y_o, y_b, y_a = [None, None], [None, None], [None, None]
    for k in range(4):
        wo_copy(k).wait()
        for h in range(2):
            part = project(k, h)
            if k < 2:
                proj_buf[k, h] = part
                copy = send(proj_buf.at[k, h], y_buf.at[k, h], y_send.at[k, h], y_recv.at[k, h], (to_y_fwd, to_y_bwd)[k])
                (y_o, y_b)[k][h] = copy
            elif k == 2:
                y_o[h].wait_recv()
                proj_buf[2, h] = part + y_buf[0, h]
                y_a[h] = send(proj_buf.at[2, h], y_buf.at[2, h], y_send.at[2, h], y_recv.at[2, h], to_y_fwd)
            else:
                if h == 0:
                    hid_copy.wait()
                own_cols = pl.ds(pl.multiple_of(y * cols + h * half, half), half)
                proj_buf[3, h] = part + hid_buf[:, h * half : (h + 1) * half].astype(jnp.float32) + b_out_ref[:, own_cols]
        if k < 2:
            wo_copy(k + 2).start()

    def place(xt, yt, ct, h):
        row = pl.multiple_of((xt * 2 + ct) * rows, rows)
        col = pl.multiple_of(yt * cols + h * half, half)
        return pl.ds(row, rows), pl.ds(col, half)

    xs = (x, x_bwd, x_fwd, x_opp)
    ys = (y, y_bwd, y_fwd, y_opp)
    x_peers, y_peers = (to_x_fwd, to_x_bwd), (to_y_fwd, to_y_bwd)
    gathers = {}
    pairs = {}

    def spot(h, first, second, ct=None):
        ct = core if ct is None else ct
        if h == 0:
            return place(xs[first], ys[second], ct, h)
        return place(xs[second], ys[first], ct, h)

    def piece(h, first, second):
        return gather_buf.at[spot(h, first, second)]

    def ring_send(h, first, second, slot, phase):
        peers = (x_peers, y_peers) if h == 0 else (y_peers, x_peers)
        peer = peers[phase][1 if slot == 2 else 0]
        index = slot - 1 if phase == 0 else 3 + first * 3 + slot - 1
        key = (h, phase, first if phase else 0, slot)
        ref = piece(h, first, second)
        gathers[key] = send(ref, ref, g_send.at[h, index], g_recv.at[h, index], peer)

    def pair_forward(h, first, second):
        ref = piece(h, first, second)
        index = first * 4 + second
        pairs[(h, first, second)] = send(ref, ref, d_send.at[h, index], d_recv.at[h, index], to_pair)

    def convert(where):
        out_ref[where] = gather_buf[where].astype(jnp.bfloat16)

    def mirrored(slot):
        return (0, 2, 1, 3)[slot]

    todo = []

    def drain(limit):
        while len(todo) > limit:
            h, first, second = todo.pop(0)
            pairs[(h, first, second)].wait_recv()
            convert(spot(h, mirrored(first), mirrored(second), 1 - core))

    def have(h, first, second):
        pair_forward(h, first, second)
        convert(spot(h, first, second))
        todo.append((h, first, second))
        drain(2)

    for h in range(2):
        y_b[h].wait_recv()
        part = proj_buf[3, h] + y_buf[1, h]
        y_a[h].wait_recv()
        gather_buf[spot(h, 0, 0)] = part + y_buf[2, h]
        ring_send(h, 0, 0, 1, 0)
        ring_send(h, 0, 0, 2, 0)
        pair_forward(h, 0, 0)
    for h in range(2):
        ring_send(h, 0, 0, 1, 1)
        ring_send(h, 0, 0, 2, 1)
        convert(spot(h, 0, 0))
        todo.append((h, 0, 0))

    def arrived(h, first, second):
        if second == 0:
            gathers[(h, 0, 0, first)].wait_recv()
            if first == 1:
                ring_send(h, 1, 0, 3, 0)
            ring_send(h, first, 0, 1, 1)
            ring_send(h, first, 0, 2, 1)
        else:
            gathers[(h, 1, first, second)].wait_recv()
            if second == 1:
                ring_send(h, first, 1, 3, 1)
        have(h, first, second)

    order = [(1, 0), (2, 0), (0, 1), (0, 2), (3, 0), (1, 1), (0, 3), (2, 1), (1, 2), (1, 3), (2, 2), (3, 1), (2, 3), (3, 2), (3, 3)]
    for first, second in order:
        for h in range(2):
            arrived(h, first, second)
    drain(0)
    for copy in sends:
        copy.wait_send()


def store_kernel(lens_ref, y_ref, kv_ref, cache_ref, y_out_ref, cache_buf, k_out_ref, v_out_ref, y_sem, out_sem):
    k_buf, v_buf = cache_buf.at[0], cache_buf.at[1]
    batch, pos_local, hd = k_buf.shape
    first_pos = lax.axis_index("sq") * pos_local
    row = lax.broadcasted_iota(jnp.int32, (16, hd), 0)
    pairs = ((k_buf, k_out_ref), (v_buf, v_out_ref))

    def write(c):
        at = pl.ds(pl.multiple_of(c * SEQS, SEQS), SEQS)
        return [pltpu.make_async_copy(buf.at[at], out.at[at], out_sem.at[w, c]) for w, (buf, out) in enumerate(pairs)]

    def replace(c, _):
        for i in range(SEQS):
            b = c * SEQS + i
            pos = lens_ref[b] - first_pos
            base = pl.multiple_of(lax.div(jnp.clip(pos, 0, pos_local - 1), 16) * 16, 16)
            here = row + base == pos
            for which, (buf, _) in enumerate(pairs):
                old = buf[b, pl.ds(base, 16), :].astype(jnp.float32)
                new = kv_ref[which, pl.ds(b, 1), :]
                buf[b, pl.ds(base, 16), :] = jnp.where(here, new, old).astype(jnp.bfloat16)
        for copy in write(c):
            copy.start()
        return 0

    def drain(c, _):
        for copy in write(c):
            copy.wait()
        return 0

    y_copy = pltpu.make_async_copy(y_ref, y_out_ref, y_sem)
    y_copy.start()
    lax.fori_loop(0, batch // SEQS, replace, 0)
    lax.fori_loop(0, batch // SEQS, drain, 0)
    y_copy.wait()


def solution(mesh):
    nx, ny = mesh.shape["sq"] // 2, mesh.shape["tp"]

    def local_step(hidden, cache_lens, k_cache, v_cache, ln_gain, ln_bias, w_query, b_query, w_kv, b_kv, w_out, b_out):
        batch, pos_local, hd = k_cache.shape
        d_model, depth = w_query.shape
        heads = depth // hd
        rows, cols = batch // (2 * nx), d_model // ny
        width = depth + hd
        half = cols // 2
        f32, bf16, dma, vmem_buf = jnp.float32, jnp.bfloat16, pltpu.SemaphoreType.DMA, pltpu.VMEM
        smem, vmem, hbm = (pl.BlockSpec(memory_space=m) for m in (pltpu.SMEM, pltpu.VMEM, pl.ANY))
        out_hidden, key_val, caches = pl.pallas_call(
            functools.partial(decode_kernel, (nx, ny, heads, rows, cols, pos_local)),
            out_shape=[
                vmem_buf((batch, d_model), bf16),
                vmem_buf((2, batch, hd), f32),
                vmem_buf((2,) + k_cache.shape, bf16),
            ],
            in_specs=[smem] + [vmem] * 5 + [hbm] * 6,
            out_specs=[vmem] * 3,
            scratch_shapes=[
                vmem_buf((W_SLOTS * TALL, depth), bf16),
                vmem_buf((W_SLOTS, TALL, 2 * hd), bf16),
                vmem_buf((batch * 16, hd), f32),
                vmem_buf((batch, width), f32),
                vmem_buf((SEQS * 16, hd), f32),
                vmem_buf((SEQS * 16, pos_local), f32),
                vmem_buf((SEQS * 16, pos_local), f32),
                vmem_buf((batch, hd), f32),
                vmem_buf((batch, hd), f32),
                vmem_buf((4, rows, width), f32),
                vmem_buf((3, rows, width), f32),
                vmem_buf((rows, depth), bf16),
                vmem_buf((4, 2, rows, half), f32),
                vmem_buf((3, 2, rows, half), f32),
                vmem_buf((rows, cols), bf16),
                vmem_buf((batch, d_model), f32),
                dma,
                dma((2, d_model // TALL)),
                dma((2, batch // SEQS)),
                dma((4,)),
                dma,
                dma((4,)),
                dma((4,)),
                dma((3,)),
                dma((3,)),
                dma((3, 2)),
                dma((3, 2)),
                dma((2, 15)),
                dma((2, 15)),
                dma((2, 16)),
                dma((2, 16)),
            ],
            compiler_params=pltpu.CompilerParams(collective_id=0, has_side_effects=True, vmem_limit_bytes=27 * 1024 * 1024),
            name="decode",
        )(
            cache_lens,
            ln_gain.reshape(1, d_model),
            ln_bias.reshape(1, d_model),
            b_query,
            b_kv.reshape(1, 2 * hd),
            b_out.reshape(1, d_model),
            hidden,
            w_query,
            w_kv,
            w_out,
            k_cache,
            v_cache,
        )
        out_hidden, _, key_new, val_new = pl.pallas_call(
            store_kernel,
            out_shape=[
                jax.ShapeDtypeStruct((batch, d_model), bf16),
                vmem_buf((2,) + k_cache.shape, bf16),
                jax.ShapeDtypeStruct(k_cache.shape, bf16),
                jax.ShapeDtypeStruct(v_cache.shape, bf16),
            ],
            in_specs=[smem] + [vmem] * 3,
            out_specs=[hbm, vmem, hbm, hbm],
            input_output_aliases={3: 1},
            scratch_shapes=[dma, dma((2, batch // SEQS))],
            compiler_params=pltpu.CompilerParams(vmem_limit_bytes=1 * 1024 * 1024),
            name="store",
        )(cache_lens, out_hidden, key_val, caches)
        return out_hidden, key_new, val_new

    cache_spec = P("dp", "sq", None)
    row_spec = P("dp", None)
    in_specs = (row_spec, P("dp"), cache_spec, cache_spec, P(None), P(None), P(None, "tp"), P("tp"), P(None, None), P(None), P("tp", None), P(None))
    out_specs = (row_spec, cache_spec, cache_spec)
    return jax.shard_map(local_step, mesh=mesh, in_specs=in_specs, out_specs=out_specs, check_vma=False)
```

```python
import functools

import jax
import jax.numpy as jnp
from jax import lax
from jax.experimental import pallas as pl
from jax.experimental.pallas import tpu as pltpu
from jax.sharding import PartitionSpec as P

MESH = pl.DeviceIdType.MESH
LANES = 128
SEQS = 16
TALL = 1024
WIDE = 512
EARLY = 6
W_SLOTS = 3


def merge_into(dst, part_a, part_b, heads):
    stat_a, stat_b = part_a(heads), part_b(heads)
    top = jnp.maximum(stat_a, stat_b)
    exp_a, exp_b = jnp.exp(stat_a - top), jnp.exp(stat_b - top)
    sums = stat_a * pltpu.roll(exp_a, 64, 1) + stat_b * pltpu.roll(exp_b, 64, 1)
    lane = lax.broadcasted_iota(jnp.int32, top.shape, 1)
    stat = jnp.where(lane < 64, top, sums)
    for n in range(heads):
        dst[:, n * LANES : (n + 1) * LANES] = part_a(n) * exp_a[:, n : n + 1] + part_b(n) * exp_b[:, n : n + 1]
    dst[:, heads * LANES :] = stat


def decode_kernel(
    dims,
    lens_ref,
    gain_ref,
    bias_ref,
    b_query_ref,
    b_kv_ref,
    b_out_ref,
    hidden_ref,
    w_query_ref,
    w_kv_ref,
    w_out_ref,
    k_ref,
    v_ref,
    out_ref,
    kv_buf,
    cache_buf,
    w_buf,
    wkv_buf,
    q_buf,
    part_buf,
    o_buf,
    s_buf0,
    s_buf1,
    stat_buf,
    stat_buf2,
    pair_buf,
    x_buf,
    att_buf,
    proj_buf,
    y_buf,
    hid_buf,
    gather_buf,
    h_sem,
    w_sem,
    in_sem,
    wo_sem,
    hid_sem,
    pair_send,
    pair_recv,
    x_send,
    x_recv,
    y_send,
    y_recv,
    g_send,
    g_recv,
    d_send,
    d_recv,
):
    nx, ny, heads, rows, cols, pos_local = dims
    k_buf, v_buf = cache_buf.at[0], cache_buf.at[1]
    batch, d_model = out_ref.shape
    hd, seqs = LANES, SEQS
    half = cols // 2
    depth = heads * hd
    steps = batch // seqs
    blocks = d_model // TALL
    sq = lax.axis_index("sq")
    y = lax.axis_index("tp")
    x = sq // 2
    core = sq % 2
    step = 1 - 2 * core
    first_pos = sq * pos_local
    scale = hd ** -0.5
    lowest = float(jnp.finfo(jnp.float32).min)

    def wrap(value, size):
        return lax.rem(value + 2 * size, size)

    x_fwd, x_bwd, x_opp = wrap(x + step, nx), wrap(x - step, nx), wrap(x + 2, nx)
    y_fwd, y_bwd, y_opp = wrap(y + step, ny), wrap(y - step, ny), wrap(y + 2, ny)
    to_pair = {"sq": x * 2 + 1 - core}
    to_x_fwd, to_x_bwd = {"sq": x_fwd * 2 + core}, {"sq": x_bwd * 2 + core}
    to_y_fwd, to_y_bwd = {"tp": y_fwd}, {"tp": y_bwd}

    barrier = pltpu.get_barrier_semaphore()
    for peer in (to_pair, to_x_fwd, to_x_bwd, to_y_fwd, to_y_bwd):
        pl.semaphore_signal(barrier, inc=1, device_id=peer, device_id_type=MESH)

    h_buf = out_ref

    def w_copies(k):
        slot, at = k % W_SLOTS, pl.ds(k * TALL, TALL)
        return (
            pltpu.make_async_copy(w_query_ref.at[at, :], w_buf.at[pl.ds(slot * TALL, TALL), :], w_sem.at[0, k]),
            pltpu.make_async_copy(w_kv_ref.at[at, :], wkv_buf.at[slot], w_sem.at[1, k]),
        )

    def block_row(i):
        slot, mine = i // 2, i % 2
        sign = step * (1 - 2 * mine)
        shift = 2 * ((3 - slot) // 3) + sign * (slot * (3 - slot) * (3 - 2 * slot) // 2)
        owner = wrap(x + shift, nx) * 2 + (1 - core) * (1 - mine) + core * mine
        return owner * rows

    def step_rows(c):
        per = rows // seqs
        return pl.multiple_of(block_row(c // per) + (c % per) * seqs, seqs)

    def read(c):
        at = pl.ds(step_rows(c), seqs)
        return (
            pltpu.make_async_copy(k_ref.at[at], k_buf.at[at], in_sem.at[0, c]),
            pltpu.make_async_copy(v_ref.at[at], v_buf.at[at], in_sem.at[1, c]),
        )

    h_copy = pltpu.make_async_copy(hidden_ref, h_buf, h_sem)
    h_copy.start()

    def start_weights(k, _):
        for copy in w_copies(k):
            copy.start()
        return 0

    def start_caches(c, _):
        for copy in read(c):
            copy.start()
        return 0

    lax.fori_loop(0, W_SLOTS, start_weights, 0)
    lax.fori_loop(0, EARLY, start_caches, 0)
    q_buf[...] = jnp.zeros_like(q_buf)
    h_copy.wait()

    tiles = d_model // hd

    def lane_tiles(at):
        return [h_buf[at, t * hd : (t + 1) * hd].astype(jnp.float32) for t in range(tiles)]

    def add_up(values):
        while len(values) > 1:
            values = [sum(values[i : i + 2]) for i in range(0, len(values), 2)]
        return values[0]

    def rows16(r):
        return pl.ds(pl.multiple_of(r * 16, 16), 16)

    def sum_rows(r, _):
        stat_buf[rows16(r), :] = add_up(lane_tiles(rows16(r)))
        return 0

    def spread_rows(r, _):
        mean_val = stat_buf[rows16(r), :]
        stat_buf2[rows16(r), :] = add_up([(v - mean_val) * (v - mean_val) for v in lane_tiles(rows16(r))])
        return 0

    def norm_rows(r, _):
        at = rows16(r)
        mean_val, inv = stat_buf[at, :], stat_buf2[at, :]
        for t in range(tiles):
            cols = slice(t * hd, (t + 1) * hd)
            normed = (h_buf[at, cols].astype(jnp.float32) - mean_val) * inv
            h_buf[at, cols] = (normed * gain_ref[:, cols] + bias_ref[:, cols]).astype(jnp.bfloat16)
        return 0

    def row_means(buf):
        return jnp.broadcast_to(jnp.sum(buf[...], axis=-1, keepdims=True) * (1.0 / d_model), buf.shape)

    lax.fori_loop(0, batch // 16, sum_rows, 0)
    stat_buf[...] = row_means(stat_buf)
    lax.fori_loop(0, batch // 16, spread_rows, 0)
    stat_buf2[...] = lax.rsqrt(row_means(stat_buf2) + 1e-5)
    lax.fori_loop(0, batch // 16, norm_rows, 0)

    y_order = (y_opp, y_bwd, y_fwd, y)

    def wo_copy(k):
        src = w_out_ref.at[:, pl.ds(pl.multiple_of(y_order[k] * cols, cols), cols)]
        return pltpu.make_async_copy(src, w_buf.at[pl.ds((k % 2) * depth, depth), :], wo_sem.at[k])

    for k in range(blocks):
        for copy in w_copies(k):
            copy.wait()
        h_cols, slot = h_buf[:, k * TALL : (k + 1) * TALL], k % W_SLOTS
        kv = jnp.dot(h_cols, wkv_buf[slot], preferred_element_type=jnp.float32)
        for e in range(2):
            part = kv[:, e * hd : (e + 1) * hd]
            kv_buf[e] = part if k == 0 else kv_buf[e] + part
        for n in range(0, depth, WIDE):
            w_block = w_buf[slot * TALL : (slot + 1) * TALL, n : n + WIDE]
            part = jnp.dot(h_cols, w_block, preferred_element_type=jnp.float32)
            part_buf[:, n : n + WIDE] = part if k == 0 else part_buf[:, n : n + WIDE] + part
        if k + W_SLOTS < blocks:
            for copy in w_copies(k + W_SLOTS):
                copy.start()
        if k + W_SLOTS == blocks - 1:
            lax.fori_loop(EARLY, steps, start_caches, 0)
    for e in range(2):
        new = kv_buf[e] + b_kv_ref[:, e * hd : (e + 1) * hd]
        kv_buf[e] = new.astype(jnp.bfloat16).astype(jnp.float32)
    for n in range(heads):
        new = part_buf[:, n * hd : (n + 1) * hd] + b_query_ref[n * hd : (n + 1) * hd].reshape(1, hd)
        q_buf[pl.ds(n, batch, stride=16), :] = new.astype(jnp.bfloat16).astype(jnp.float32)
    hid_copy = pltpu.make_async_copy(
        hidden_ref.at[pl.ds(pl.multiple_of(sq * rows, rows), rows), pl.ds(pl.multiple_of(y * cols, cols), cols)], hid_buf, hid_sem
    )
    hid_copy.start()
    for k in range(2):
        wo_copy(k).start()

    zero = jnp.zeros((16, hd), jnp.bfloat16)
    at_pos = lax.broadcasted_iota(jnp.int32, (16, pos_local), 1) + first_pos
    row = lax.broadcasted_iota(jnp.int32, (16, hd), 0)
    lane = lax.broadcasted_iota(jnp.int32, (16, hd), 1)
    pick_m = (lane == row) & (row < heads)
    pick_l = (lane == row + 64) & (row < heads)

    def score(c, s_buf):
        for copy in read(c):
            copy.wait()
        b0 = step_rows(c)
        for i in range(0, seqs, 2):
            q0 = q_buf[pl.ds(pl.multiple_of(b0 * 16 + i * 16, 16), 16), :].astype(jnp.bfloat16)
            q1 = q_buf[pl.ds(pl.multiple_of(b0 * 16 + i * 16 + 16, 16), 16), :].astype(jnp.bfloat16)
            q2 = jnp.concatenate([jnp.concatenate([q0, zero], axis=1), jnp.concatenate([zero, q1], axis=1)], axis=0)
            k2 = jnp.concatenate([k_buf[b0 + i], k_buf[b0 + i + 1]], axis=1)
            s2 = lax.dot_general(q2, k2, (((1,), (1,)), ((), ())), preferred_element_type=jnp.float32)
            s_buf[i * 16 : i * 16 + 32, :] = s2 * scale

    def combine(c, s_buf):
        b0 = step_rows(c)
        for i in range(0, seqs, 2):
            v2 = jnp.concatenate([v_buf[b0 + i], v_buf[b0 + i + 1]], axis=1)
            valid = jnp.concatenate([at_pos < lens_ref[b0 + i], at_pos < lens_ref[b0 + i + 1]], axis=0)
            s2 = jnp.where(valid, s_buf[i * 16 : i * 16 + 32, :], lowest)
            top = jnp.max(s2, axis=-1, keepdims=True)
            p2 = jnp.where(valid, jnp.exp(s2 - top), 0.0)
            total = jnp.sum(p2, axis=-1, keepdims=True)
            o2 = jnp.dot(p2.astype(jnp.bfloat16), v2, preferred_element_type=jnp.float32)
            for e in range(2):
                part = slice(e * 16, e * 16 + 16)
                stat = jnp.where(pick_m, top[part], 0.0) + jnp.where(pick_l, total[part], 0.0)
                stat = jnp.sum(stat, axis=0, keepdims=True)
                o_buf[(i + e) * 16 : (i + e) * 16 + 16, :] = jnp.where(row == heads, stat, o2[part, e * hd : (e + 1) * hd])
        for n in range(heads + 1):
            part_buf[pl.ds(b0, seqs), n * hd : (n + 1) * hd] = o_buf[pl.ds(n, seqs, stride=16), :]

    sends = []

    def remote(src, dst, ssem, rsem, peer):
        return pltpu.make_async_remote_copy(
            src_ref=src, dst_ref=dst, send_sem=ssem, recv_sem=rsem, device_id=peer, device_id_type=MESH
        )

    def send(*args):
        copy = remote(*args)
        copy.start()
        sends.append(copy)
        return copy

    def part_at(i):
        return pl.ds(pl.multiple_of(block_row(i), rows), rows)

    def of_part(i):
        return lambda n: part_buf[part_at(i), n * hd : (n + 1) * hd]

    def of(ref):
        return lambda n: ref[:, n * hd : (n + 1) * hd]

    pair = [remote(part_buf.at[part_at(2 * k), :], pair_buf.at[k], pair_send.at[k], pair_recv.at[k], to_pair) for k in range(4)]
    x_o = remote(pair_buf.at[0], x_buf.at[0], x_send.at[0], x_recv.at[0], to_x_fwd)
    x_b = remote(pair_buf.at[1], x_buf.at[1], x_send.at[1], x_recv.at[1], to_x_bwd)
    x_a = remote(pair_buf.at[2], x_buf.at[2], x_send.at[2], x_recv.at[2], to_x_fwd)
    sends.extend(pair + [x_o, x_b, x_a])

    def after_block(i):
        slot = i // 2
        if i % 2 == 0:
            pair[slot].start()
            return
        pair[slot].wait_recv()
        merge_into(pair_buf.at[slot], of_part(i), of(pair_buf.at[slot]), heads)
        if slot == 0:
            x_o.start()
        elif slot == 1:
            x_b.start()
        elif slot == 2:
            x_o.wait_recv()
            merge_into(pair_buf.at[2], of(pair_buf.at[2]), of(x_buf.at[0]), heads)
            x_a.start()

    pl.semaphore_wait(barrier, 5)
    score(0, s_buf0)

    def one_block(i, _):
        c = i * 2
        score(c + 1, s_buf1)
        combine(c, s_buf0)
        score(c + 2, s_buf0)
        combine(c + 1, s_buf1)
        for j in range(7):
            pl.when(i == j)(functools.partial(after_block, j))
        return 0

    lax.fori_loop(0, steps // 2 - 1, one_block, 0)
    score(steps - 1, s_buf1)
    combine(steps - 2, s_buf0)
    combine(steps - 1, s_buf1)

    own = pl.multiple_of(sq * rows, rows)
    k_new, v_new = kv_buf[0, pl.ds(own, rows), :], kv_buf[1, pl.ds(own, rows), :]
    new_lane = lax.broadcasted_iota(jnp.int32, (rows, hd), 1)
    new_stat = jnp.where((new_lane >= 64) & (new_lane < 64 + heads), 1.0, 0.0)
    for n in range(heads):
        s_new = jnp.sum(q_buf[pl.ds(own * 16 + n, rows, stride=16), :] * k_new, axis=-1, keepdims=True) * scale
        new_stat = jnp.where(new_lane == n, s_new, new_stat)

    after_block(7)
    total = pair_buf.at[3]
    merge_into(total, of(total), lambda n: new_stat if n == heads else v_new, heads)
    x_b.wait_recv()
    merge_into(total, of(total), of(x_buf.at[1]), heads)
    x_a.wait_recv()
    merge_into(total, of(total), of(x_buf.at[2]), heads)
    stat = total[:, depth:]
    for n in range(heads):
        block = slice(n * hd, (n + 1) * hd)
        att_buf[:, block] = (total[:, block] / stat[:, 64 + n : 65 + n]).astype(jnp.bfloat16)

    def project(k, h):
        w_block = w_buf[(k % 2) * depth : (k % 2 + 1) * depth, h * half : (h + 1) * half]
        return jnp.dot(att_buf[...], w_block, preferred_element_type=jnp.float32)

    y_o, y_b, y_a = [None, None], [None, None], [None, None]
    for k in range(4):
        wo_copy(k).wait()
        for h in range(2):
            part = project(k, h)
            if k < 2:
                proj_buf[k, h] = part
                copy = send(proj_buf.at[k, h], y_buf.at[k, h], y_send.at[k, h], y_recv.at[k, h], (to_y_fwd, to_y_bwd)[k])
                (y_o, y_b)[k][h] = copy
            elif k == 2:
                y_o[h].wait_recv()
                proj_buf[2, h] = part + y_buf[0, h]
                y_a[h] = send(proj_buf.at[2, h], y_buf.at[2, h], y_send.at[2, h], y_recv.at[2, h], to_y_fwd)
            else:
                if h == 0:
                    hid_copy.wait()
                own_cols = pl.ds(pl.multiple_of(y * cols + h * half, half), half)
                proj_buf[3, h] = part + hid_buf[:, h * half : (h + 1) * half].astype(jnp.float32) + b_out_ref[:, own_cols]
        if k < 2:
            wo_copy(k + 2).start()

    def place(xt, yt, ct, h):
        row = pl.multiple_of((xt * 2 + ct) * rows, rows)
        col = pl.multiple_of(yt * cols + h * half, half)
        return pl.ds(row, rows), pl.ds(col, half)

    xs = (x, x_bwd, x_fwd, x_opp)
    ys = (y, y_bwd, y_fwd, y_opp)
    x_peers, y_peers = (to_x_fwd, to_x_bwd), (to_y_fwd, to_y_bwd)
    gathers = {}
    pairs = {}

    def spot(h, first, second, ct=None):
        ct = core if ct is None else ct
        if h == 0:
            return place(xs[first], ys[second], ct, h)
        return place(xs[second], ys[first], ct, h)

    def piece(h, first, second):
        return gather_buf.at[spot(h, first, second)]

    def ring_send(h, first, second, slot, phase):
        peers = (x_peers, y_peers) if h == 0 else (y_peers, x_peers)
        peer = peers[phase][1 if slot == 2 else 0]
        index = slot - 1 if phase == 0 else 3 + first * 3 + slot - 1
        key = (h, phase, first if phase else 0, slot)
        ref = piece(h, first, second)
        gathers[key] = send(ref, ref, g_send.at[h, index], g_recv.at[h, index], peer)

    def pair_forward(h, first, second):
        ref = piece(h, first, second)
        index = first * 4 + second
        pairs[(h, first, second)] = send(ref, ref, d_send.at[h, index], d_recv.at[h, index], to_pair)

    def convert(where):
        out_ref[where] = gather_buf[where].astype(jnp.bfloat16)

    def mirrored(slot):
        return (0, 2, 1, 3)[slot]

    todo = []

    def drain(limit):
        while len(todo) > limit:
            h, first, second = todo.pop(0)
            pairs[(h, first, second)].wait_recv()
            convert(spot(h, mirrored(first), mirrored(second), 1 - core))

    def have(h, first, second):
        pair_forward(h, first, second)
        convert(spot(h, first, second))
        todo.append((h, first, second))
        drain(2)

    for h in range(2):
        y_b[h].wait_recv()
        part = proj_buf[3, h] + y_buf[1, h]
        y_a[h].wait_recv()
        gather_buf[spot(h, 0, 0)] = part + y_buf[2, h]
        ring_send(h, 0, 0, 1, 0)
        ring_send(h, 0, 0, 2, 0)
        pair_forward(h, 0, 0)
    for h in range(2):
        ring_send(h, 0, 0, 1, 1)
        ring_send(h, 0, 0, 2, 1)
        convert(spot(h, 0, 0))
        todo.append((h, 0, 0))

    def arrived(h, first, second):
        if second == 0:
            gathers[(h, 0, 0, first)].wait_recv()
            if first == 1:
                ring_send(h, 1, 0, 3, 0)
            ring_send(h, first, 0, 1, 1)
            ring_send(h, first, 0, 2, 1)
        else:
            gathers[(h, 1, first, second)].wait_recv()
            if second == 1:
                ring_send(h, first, 1, 3, 1)
        have(h, first, second)

    order = [(1, 0), (2, 0), (0, 1), (0, 2), (3, 0), (1, 1), (0, 3), (2, 1), (1, 2), (1, 3), (2, 2), (3, 1), (2, 3), (3, 2), (3, 3)]
    for first, second in order:
        for h in range(2):
            arrived(h, first, second)
    drain(0)
    for copy in sends:
        copy.wait_send()


def store_kernel(lens_ref, y_ref, kv_ref, cache_ref, y_out_ref, cache_buf, k_out_ref, v_out_ref, y_sem, out_sem):
    k_buf, v_buf = cache_buf.at[0], cache_buf.at[1]
    batch, pos_local, hd = k_buf.shape
    first_pos = lax.axis_index("sq") * pos_local
    row = lax.broadcasted_iota(jnp.int32, (16, hd), 0)
    pairs = ((k_buf, k_out_ref), (v_buf, v_out_ref))

    def write(c):
        at = pl.ds(pl.multiple_of(c * SEQS, SEQS), SEQS)
        return [pltpu.make_async_copy(buf.at[at], out.at[at], out_sem.at[w, c]) for w, (buf, out) in enumerate(pairs)]

    def replace(c, _):
        for i in range(SEQS):
            b = c * SEQS + i
            pos = lens_ref[b] - first_pos
            base = pl.multiple_of(lax.div(jnp.clip(pos, 0, pos_local - 1), 16) * 16, 16)
            here = row + base == pos
            for which, (buf, _) in enumerate(pairs):
                old = buf[b, pl.ds(base, 16), :].astype(jnp.float32)
                new = kv_ref[which, pl.ds(b, 1), :]
                buf[b, pl.ds(base, 16), :] = jnp.where(here, new, old).astype(jnp.bfloat16)
        for copy in write(c):
            copy.start()
        return 0

    def drain(c, _):
        for copy in write(c):
            copy.wait()
        return 0

    y_copy = pltpu.make_async_copy(y_ref, y_out_ref, y_sem)
    y_copy.start()
    lax.fori_loop(0, batch // SEQS, replace, 0)
    lax.fori_loop(0, batch // SEQS, drain, 0)
    y_copy.wait()


def solution(mesh):
    nx, ny = mesh.shape["sq"] // 2, mesh.shape["tp"]

    def local_step(hidden, cache_lens, k_cache, v_cache, ln_gain, ln_bias, w_query, b_query, w_kv, b_kv, w_out, b_out):
        batch, pos_local, hd = k_cache.shape
        d_model, depth = w_query.shape
        heads = depth // hd
        rows, cols = batch // (2 * nx), d_model // ny
        width = depth + hd
        half = cols // 2
        f32, bf16, dma, vmem_buf = jnp.float32, jnp.bfloat16, pltpu.SemaphoreType.DMA, pltpu.VMEM
        smem, vmem, hbm = (pl.BlockSpec(memory_space=m) for m in (pltpu.SMEM, pltpu.VMEM, pl.ANY))
        out_hidden, key_val, caches = pl.pallas_call(
            functools.partial(decode_kernel, (nx, ny, heads, rows, cols, pos_local)),
            out_shape=[
                vmem_buf((batch, d_model), bf16),
                vmem_buf((2, batch, hd), f32),
                vmem_buf((2,) + k_cache.shape, bf16),
            ],
            in_specs=[smem] + [vmem] * 5 + [hbm] * 6,
            out_specs=[vmem] * 3,
            scratch_shapes=[
                vmem_buf((W_SLOTS * TALL, depth), bf16),
                vmem_buf((W_SLOTS, TALL, 2 * hd), bf16),
                vmem_buf((batch * 16, hd), f32),
                vmem_buf((batch, width), f32),
                vmem_buf((SEQS * 16, hd), f32),
                vmem_buf((SEQS * 16, pos_local), f32),
                vmem_buf((SEQS * 16, pos_local), f32),
                vmem_buf((batch, hd), f32),
                vmem_buf((batch, hd), f32),
                vmem_buf((4, rows, width), f32),
                vmem_buf((3, rows, width), f32),
                vmem_buf((rows, depth), bf16),
                vmem_buf((4, 2, rows, half), f32),
                vmem_buf((3, 2, rows, half), f32),
                vmem_buf((rows, cols), bf16),
                vmem_buf((batch, d_model), f32),
                dma,
                dma((2, d_model // TALL)),
                dma((2, batch // SEQS)),
                dma((4,)),
                dma,
                dma((4,)),
                dma((4,)),
                dma((3,)),
                dma((3,)),
                dma((3, 2)),
                dma((3, 2)),
                dma((2, 15)),
                dma((2, 15)),
                dma((2, 16)),
                dma((2, 16)),
            ],
            compiler_params=pltpu.CompilerParams(collective_id=0, has_side_effects=True, vmem_limit_bytes=27 * 1024 * 1024),
            name="decode",
        )(
            cache_lens,
            ln_gain.reshape(1, d_model),
            ln_bias.reshape(1, d_model),
            b_query,
            b_kv.reshape(1, 2 * hd),
            b_out.reshape(1, d_model),
            hidden,
            w_query,
            w_kv,
            w_out,
            k_cache,
            v_cache,
        )
        out_hidden, _, key_new, val_new = pl.pallas_call(
            store_kernel,
            out_shape=[
                jax.ShapeDtypeStruct((batch, d_model), bf16),
                vmem_buf((2,) + k_cache.shape, bf16),
                jax.ShapeDtypeStruct(k_cache.shape, bf16),
                jax.ShapeDtypeStruct(v_cache.shape, bf16),
            ],
            in_specs=[smem] + [vmem] * 3,
            out_specs=[hbm, vmem, hbm, hbm],
            input_output_aliases={3: 1},
            scratch_shapes=[dma, dma((2, batch // SEQS))],
            compiler_params=pltpu.CompilerParams(vmem_limit_bytes=1 * 1024 * 1024),
            name="store",
        )(cache_lens, out_hidden, key_val, caches)
        return out_hidden, key_new, val_new

    cache_spec = P("dp", "sq", None)
    row_spec = P("dp", None)
    in_specs = (row_spec, P("dp"), cache_spec, cache_spec, P(None), P(None), P(None, "tp"), P("tp"), P(None, None), P(None), P("tp", None), P(None))
    out_specs = (row_spec, cache_spec, cache_spec)
    return jax.shard_map(local_step, mesh=mesh, in_specs=in_specs, out_specs=out_specs, check_vma=False)
```

```python
import functools

import jax
import jax.numpy as jnp
from jax import lax
from jax.experimental import pallas as pl
from jax.experimental.pallas import tpu as pltpu
from jax.sharding import PartitionSpec as P

MESH = pl.DeviceIdType.MESH
LANES = 128
SEQS = 16
TALL = 1024
WIDE = 512
EARLY = 6
W_SLOTS = 3


def merge_into(dst, part_a, part_b, heads):
    stat_a, stat_b = part_a(heads), part_b(heads)
    top = jnp.maximum(stat_a, stat_b)
    exp_a, exp_b = jnp.exp(stat_a - top), jnp.exp(stat_b - top)
    sums = stat_a * pltpu.roll(exp_a, 64, 1) + stat_b * pltpu.roll(exp_b, 64, 1)
    lane = lax.broadcasted_iota(jnp.int32, top.shape, 1)
    stat = jnp.where(lane < 64, top, sums)
    for n in range(heads):
        dst[:, n * LANES : (n + 1) * LANES] = part_a(n) * exp_a[:, n : n + 1] + part_b(n) * exp_b[:, n : n + 1]
    dst[:, heads * LANES :] = stat


def decode_kernel(
    dims,
    lens_ref,
    gain_ref,
    bias_ref,
    b_query_ref,
    b_kv_ref,
    b_out_ref,
    hidden_ref,
    w_query_ref,
    w_kv_ref,
    w_out_ref,
    k_ref,
    v_ref,
    out_ref,
    kv_buf,
    cache_buf,
    w_buf,
    wkv_buf,
    q_buf,
    part_buf,
    o_buf,
    s_buf0,
    s_buf1,
    stat_buf,
    stat_buf2,
    pair_buf,
    x_buf,
    att_buf,
    proj_buf,
    y_buf,
    hid_buf,
    gather_buf,
    h_sem,
    w_sem,
    in_sem,
    wo_sem,
    hid_sem,
    pair_send,
    pair_recv,
    x_send,
    x_recv,
    y_send,
    y_recv,
    g_send,
    g_recv,
    d_send,
    d_recv,
):
    nx, ny, heads, rows, cols, pos_local = dims
    k_buf, v_buf = cache_buf.at[0], cache_buf.at[1]
    batch, d_model = out_ref.shape
    hd, seqs = LANES, SEQS
    half = cols // 2
    depth = heads * hd
    steps = batch // seqs
    blocks = d_model // TALL
    sq = lax.axis_index("sq")
    y = lax.axis_index("tp")
    x = sq // 2
    core = sq % 2
    step = 1 - 2 * core
    first_pos = sq * pos_local
    scale = hd ** -0.5
    lowest = float(jnp.finfo(jnp.float32).min)

    def wrap(value, size):
        return lax.rem(value + 2 * size, size)

    x_fwd, x_bwd, x_opp = wrap(x + step, nx), wrap(x - step, nx), wrap(x + 2, nx)
    y_fwd, y_bwd, y_opp = wrap(y + step, ny), wrap(y - step, ny), wrap(y + 2, ny)
    to_pair = {"sq": x * 2 + 1 - core}
    to_x_fwd, to_x_bwd = {"sq": x_fwd * 2 + core}, {"sq": x_bwd * 2 + core}
    to_y_fwd, to_y_bwd = {"tp": y_fwd}, {"tp": y_bwd}

    barrier = pltpu.get_barrier_semaphore()
    for peer in (to_pair, to_x_fwd, to_x_bwd, to_y_fwd, to_y_bwd):
        pl.semaphore_signal(barrier, inc=1, device_id=peer, device_id_type=MESH)

    h_buf = out_ref

    def w_copies(k):
        slot, at = k % W_SLOTS, pl.ds(k * TALL, TALL)
        return (
            pltpu.make_async_copy(w_query_ref.at[at, :], w_buf.at[pl.ds(slot * TALL, TALL), :], w_sem.at[0, k]),
            pltpu.make_async_copy(w_kv_ref.at[at, :], wkv_buf.at[slot], w_sem.at[1, k]),
        )

    def block_row(i):
        slot, mine = i // 2, i % 2
        sign = step * (1 - 2 * mine)
        shift = 2 * ((3 - slot) // 3) + sign * (slot * (3 - slot) * (3 - 2 * slot) // 2)
        owner = wrap(x + shift, nx) * 2 + (1 - core) * (1 - mine) + core * mine
        return owner * rows

    def step_rows(c):
        per = rows // seqs
        return pl.multiple_of(block_row(c // per) + (c % per) * seqs, seqs)

    def read(c):
        at = pl.ds(step_rows(c), seqs)
        return (
            pltpu.make_async_copy(k_ref.at[at], k_buf.at[at], in_sem.at[0, c]),
            pltpu.make_async_copy(v_ref.at[at], v_buf.at[at], in_sem.at[1, c]),
        )

    h_parts = 4
    h_rows = batch // h_parts
    h_copies = [
        pltpu.make_async_copy(hidden_ref.at[pl.ds(j * h_rows, h_rows), :], h_buf.at[pl.ds(j * h_rows, h_rows), :], h_sem.at[j])
        for j in range(h_parts)
    ]
    for copy in h_copies:
        copy.start()

    def start_weights(k, _):
        for copy in w_copies(k):
            copy.start()
        return 0

    def start_caches(c, _):
        for copy in read(c):
            copy.start()
        return 0

    lax.fori_loop(0, W_SLOTS, start_weights, 0)
    lax.fori_loop(0, EARLY, start_caches, 0)
    q_buf[...] = jnp.zeros_like(q_buf)

    tiles = d_model // hd

    def lane_tiles(at):
        return [h_buf[at, t * hd : (t + 1) * hd].astype(jnp.float32) for t in range(tiles)]

    def add_up(values):
        while len(values) > 1:
            values = [sum(values[i : i + 2]) for i in range(0, len(values), 2)]
        return values[0]

    def rows16(r):
        return pl.ds(pl.multiple_of(r * 16, 16), 16)

    def sum_rows(r, _):
        stat_buf[rows16(r), :] = add_up(lane_tiles(rows16(r)))
        return 0

    def spread_rows(r, _):
        mean_val = stat_buf[rows16(r), :]
        stat_buf2[rows16(r), :] = add_up([(v - mean_val) * (v - mean_val) for v in lane_tiles(rows16(r))])
        return 0

    def norm_rows(r, _):
        at = rows16(r)
        mean_val, inv = stat_buf[at, :], stat_buf2[at, :]
        for t in range(tiles):
            cols = slice(t * hd, (t + 1) * hd)
            normed = (h_buf[at, cols].astype(jnp.float32) - mean_val) * inv
            h_buf[at, cols] = (normed * gain_ref[:, cols] + bias_ref[:, cols]).astype(jnp.bfloat16)
        return 0

    def row_means(buf):
        return jnp.broadcast_to(jnp.sum(buf[...], axis=-1, keepdims=True) * (1.0 / d_model), buf.shape)

    for j, copy in enumerate(h_copies):
        copy.wait()
        lax.fori_loop(j * h_rows // 16, (j + 1) * h_rows // 16, sum_rows, 0, unroll=2)
    stat_buf[...] = row_means(stat_buf)
    lax.fori_loop(0, batch // 16, spread_rows, 0, unroll=2)
    stat_buf2[...] = lax.rsqrt(row_means(stat_buf2) + 1e-5)
    lax.fori_loop(0, batch // 16, norm_rows, 0, unroll=2)

    y_order = (y_opp, y_bwd, y_fwd, y)

    def wo_copy(k):
        src = w_out_ref.at[:, pl.ds(pl.multiple_of(y_order[k] * cols, cols), cols)]
        return pltpu.make_async_copy(src, w_buf.at[pl.ds((k % 2) * depth, depth), :], wo_sem.at[k])

    for k in range(blocks):
        for copy in w_copies(k):
            copy.wait()
        h_cols, slot = h_buf[:, k * TALL : (k + 1) * TALL], k % W_SLOTS
        kv = jnp.dot(h_cols, wkv_buf[slot], preferred_element_type=jnp.float32)
        for e in range(2):
            part = kv[:, e * hd : (e + 1) * hd]
            kv_buf[e] = part if k == 0 else kv_buf[e] + part
        for n in range(0, depth, WIDE):
            w_block = w_buf[slot * TALL : (slot + 1) * TALL, n : n + WIDE]
            part = jnp.dot(h_cols, w_block, preferred_element_type=jnp.float32)
            part_buf[:, n : n + WIDE] = part if k == 0 else part_buf[:, n : n + WIDE] + part
        if k + W_SLOTS < blocks:
            for copy in w_copies(k + W_SLOTS):
                copy.start()
        if k + W_SLOTS == blocks - 1:
            lax.fori_loop(EARLY, steps, start_caches, 0)
    for e in range(2):
        new = kv_buf[e] + b_kv_ref[:, e * hd : (e + 1) * hd]
        kv_buf[e] = new.astype(jnp.bfloat16).astype(jnp.float32)
    for n in range(heads):
        new = part_buf[:, n * hd : (n + 1) * hd] + b_query_ref[n * hd : (n + 1) * hd].reshape(1, hd)
        q_buf[pl.ds(n, batch, stride=16), :] = new.astype(jnp.bfloat16).astype(jnp.float32)
    hid_copy = pltpu.make_async_copy(
        hidden_ref.at[pl.ds(pl.multiple_of(sq * rows, rows), rows), pl.ds(pl.multiple_of(y * cols, cols), cols)], hid_buf, hid_sem
    )
    hid_copy.start()
    for k in range(2):
        wo_copy(k).start()

    zero = jnp.zeros((16, hd), jnp.bfloat16)
    at_pos = lax.broadcasted_iota(jnp.int32, (16, pos_local), 1) + first_pos
    row = lax.broadcasted_iota(jnp.int32, (16, hd), 0)
    lane = lax.broadcasted_iota(jnp.int32, (16, hd), 1)
    pick_m = (lane == row) & (row < heads)
    pick_l = (lane == row + 64) & (row < heads)

    def score(c, s_buf):
        for copy in read(c):
            copy.wait()
        b0 = step_rows(c)
        for i in range(0, seqs, 2):
            q0 = q_buf[pl.ds(pl.multiple_of(b0 * 16 + i * 16, 16), 16), :].astype(jnp.bfloat16)
            q1 = q_buf[pl.ds(pl.multiple_of(b0 * 16 + i * 16 + 16, 16), 16), :].astype(jnp.bfloat16)
            q2 = jnp.concatenate([jnp.concatenate([q0, zero], axis=1), jnp.concatenate([zero, q1], axis=1)], axis=0)
            k2 = jnp.concatenate([k_buf[b0 + i], k_buf[b0 + i + 1]], axis=1)
            s2 = lax.dot_general(q2, k2, (((1,), (1,)), ((), ())), preferred_element_type=jnp.float32)
            s_buf[i * 16 : i * 16 + 32, :] = s2 * scale

    def combine(c, s_buf):
        b0 = step_rows(c)
        for i in range(0, seqs, 2):
            v2 = jnp.concatenate([v_buf[b0 + i], v_buf[b0 + i + 1]], axis=1)
            valid = jnp.concatenate([at_pos < lens_ref[b0 + i], at_pos < lens_ref[b0 + i + 1]], axis=0)
            s2 = jnp.where(valid, s_buf[i * 16 : i * 16 + 32, :], lowest)
            top = jnp.max(s2, axis=-1, keepdims=True)
            p2 = jnp.where(valid, jnp.exp(s2 - top), 0.0)
            total = jnp.sum(p2, axis=-1, keepdims=True)
            o2 = jnp.dot(p2.astype(jnp.bfloat16), v2, preferred_element_type=jnp.float32)
            for e in range(2):
                part = slice(e * 16, e * 16 + 16)
                stat = jnp.where(pick_m, top[part], 0.0) + jnp.where(pick_l, total[part], 0.0)
                stat = jnp.sum(stat, axis=0, keepdims=True)
                o_buf[(i + e) * 16 : (i + e) * 16 + 16, :] = jnp.where(row == heads, stat, o2[part, e * hd : (e + 1) * hd])
        for n in range(heads + 1):
            part_buf[pl.ds(b0, seqs), n * hd : (n + 1) * hd] = o_buf[pl.ds(n, seqs, stride=16), :]

    sends = []

    def remote(src, dst, ssem, rsem, peer):
        return pltpu.make_async_remote_copy(
            src_ref=src, dst_ref=dst, send_sem=ssem, recv_sem=rsem, device_id=peer, device_id_type=MESH
        )

    def send(*args):
        copy = remote(*args)
        copy.start()
        sends.append(copy)
        return copy

    def part_at(i):
        return pl.ds(pl.multiple_of(block_row(i), rows), rows)

    def of_part(i):
        return lambda n: part_buf[part_at(i), n * hd : (n + 1) * hd]

    def of(ref):
        return lambda n: ref[:, n * hd : (n + 1) * hd]

    pair = [remote(part_buf.at[part_at(2 * k), :], pair_buf.at[k], pair_send.at[k], pair_recv.at[k], to_pair) for k in range(4)]
    x_o = remote(pair_buf.at[0], x_buf.at[0], x_send.at[0], x_recv.at[0], to_x_fwd)
    x_b = remote(pair_buf.at[1], x_buf.at[1], x_send.at[1], x_recv.at[1], to_x_bwd)
    x_a = remote(pair_buf.at[2], x_buf.at[2], x_send.at[2], x_recv.at[2], to_x_fwd)
    sends.extend(pair + [x_o, x_b, x_a])

    def after_block(i):
        slot = i // 2
        if i % 2 == 0:
            pair[slot].start()
            return
        pair[slot].wait_recv()
        merge_into(pair_buf.at[slot], of_part(i), of(pair_buf.at[slot]), heads)
        if slot == 0:
            x_o.start()
        elif slot == 1:
            x_b.start()
        elif slot == 2:
            x_o.wait_recv()
            merge_into(pair_buf.at[2], of(pair_buf.at[2]), of(x_buf.at[0]), heads)
            x_a.start()

    pl.semaphore_wait(barrier, 5)
    score(0, s_buf0)

    def one_block(i, _):
        c = i * 2
        score(c + 1, s_buf1)
        combine(c, s_buf0)
        score(c + 2, s_buf0)
        combine(c + 1, s_buf1)
        for j in range(7):
            pl.when(i == j)(functools.partial(after_block, j))
        return 0

    lax.fori_loop(0, steps // 2 - 1, one_block, 0)
    score(steps - 1, s_buf1)
    combine(steps - 2, s_buf0)
    combine(steps - 1, s_buf1)

    own = pl.multiple_of(sq * rows, rows)
    k_new, v_new = kv_buf[0, pl.ds(own, rows), :], kv_buf[1, pl.ds(own, rows), :]
    new_lane = lax.broadcasted_iota(jnp.int32, (rows, hd), 1)
    new_stat = jnp.where((new_lane >= 64) & (new_lane < 64 + heads), 1.0, 0.0)
    for n in range(heads):
        s_new = jnp.sum(q_buf[pl.ds(own * 16 + n, rows, stride=16), :] * k_new, axis=-1, keepdims=True) * scale
        new_stat = jnp.where(new_lane == n, s_new, new_stat)

    after_block(7)
    total = pair_buf.at[3]
    merge_into(total, of(total), lambda n: new_stat if n == heads else v_new, heads)
    x_b.wait_recv()
    merge_into(total, of(total), of(x_buf.at[1]), heads)
    x_a.wait_recv()
    merge_into(total, of(total), of(x_buf.at[2]), heads)
    stat = total[:, depth:]
    for n in range(heads):
        block = slice(n * hd, (n + 1) * hd)
        att_buf[:, block] = (total[:, block] / stat[:, 64 + n : 65 + n]).astype(jnp.bfloat16)

    def project(k, h):
        w_block = w_buf[(k % 2) * depth : (k % 2 + 1) * depth, h * half : (h + 1) * half]
        return jnp.dot(att_buf[...], w_block, preferred_element_type=jnp.float32)

    y_o, y_b, y_a = [None, None], [None, None], [None, None]
    for k in range(4):
        wo_copy(k).wait()
        for h in range(2):
            part = project(k, h)
            if k < 2:
                proj_buf[k, h] = part
                copy = send(proj_buf.at[k, h], y_buf.at[k, h], y_send.at[k, h], y_recv.at[k, h], (to_y_fwd, to_y_bwd)[k])
                (y_o, y_b)[k][h] = copy
            elif k == 2:
                proj_buf[2, h] = part
            else:
                if h == 0:
                    hid_copy.wait()
                own_cols = pl.ds(pl.multiple_of(y * cols + h * half, half), half)
                proj_buf[3, h] = part + hid_buf[:, h * half : (h + 1) * half].astype(jnp.float32) + b_out_ref[:, own_cols]
        if k < 2:
            wo_copy(k + 2).start()
        if k == 2:
            for h in range(2):
                y_o[h].wait_recv()
                proj_buf[2, h] = proj_buf[2, h] + y_buf[0, h]
                y_a[h] = send(proj_buf.at[2, h], y_buf.at[2, h], y_send.at[2, h], y_recv.at[2, h], to_y_fwd)

    def place(xt, yt, ct, h):
        row = pl.multiple_of((xt * 2 + ct) * rows, rows)
        col = pl.multiple_of(yt * cols + h * half, half)
        return pl.ds(row, rows), pl.ds(col, half)

    xs = (x, x_bwd, x_fwd, x_opp)
    ys = (y, y_bwd, y_fwd, y_opp)
    x_peers, y_peers = (to_x_fwd, to_x_bwd), (to_y_fwd, to_y_bwd)
    gathers = {}
    pairs = {}

    def spot(h, first, second, ct=None):
        ct = core if ct is None else ct
        if h == 0:
            return place(xs[first], ys[second], ct, h)
        return place(xs[second], ys[first], ct, h)

    def piece(h, first, second):
        return gather_buf.at[spot(h, first, second)]

    def ring_send(h, first, second, slot, phase):
        peers = (x_peers, y_peers) if h == 0 else (y_peers, x_peers)
        peer = peers[phase][1 if slot == 2 else 0]
        index = slot - 1 if phase == 0 else 3 + first * 3 + slot - 1
        key = (h, phase, first if phase else 0, slot)
        ref = piece(h, first, second)
        gathers[key] = send(ref, ref, g_send.at[h, index], g_recv.at[h, index], peer)

    def pair_forward(h, first, second):
        ref = piece(h, first, second)
        index = first * 4 + second
        pairs[(h, first, second)] = send(ref, ref, d_send.at[h, index], d_recv.at[h, index], to_pair)

    def convert(where):
        out_ref[where] = gather_buf[where].astype(jnp.bfloat16)

    def mirrored(slot):
        return (0, 2, 1, 3)[slot]

    todo = []

    def drain(limit):
        while len(todo) > limit:
            h, first, second = todo.pop(0)
            pairs[(h, first, second)].wait_recv()
            convert(spot(h, mirrored(first), mirrored(second), 1 - core))

    def have(h, first, second):
        pair_forward(h, first, second)
        convert(spot(h, first, second))
        todo.append((h, first, second))
        drain(4)

    for h in range(2):
        y_b[h].wait_recv()
        part = proj_buf[3, h] + y_buf[1, h]
        y_a[h].wait_recv()
        gather_buf[spot(h, 0, 0)] = part + y_buf[2, h]
        ring_send(h, 0, 0, 1, 0)
        ring_send(h, 0, 0, 2, 0)
        pair_forward(h, 0, 0)
    for h in range(2):
        ring_send(h, 0, 0, 1, 1)
        ring_send(h, 0, 0, 2, 1)
        convert(spot(h, 0, 0))
        todo.append((h, 0, 0))

    def arrived(h, first, second):
        if second == 0:
            gathers[(h, 0, 0, first)].wait_recv()
            if first == 1:
                ring_send(h, 1, 0, 3, 0)
            ring_send(h, first, 0, 1, 1)
            ring_send(h, first, 0, 2, 1)
        else:
            gathers[(h, 1, first, second)].wait_recv()
            if second == 1:
                ring_send(h, first, 1, 3, 1)
        have(h, first, second)

    order = [(1, 0), (2, 0), (0, 1), (0, 2), (3, 0), (1, 1), (0, 3), (2, 1), (1, 2), (1, 3), (2, 2), (3, 1), (2, 3), (3, 2), (3, 3)]
    for first, second in order:
        for h in range(2):
            arrived(h, first, second)
    drain(0)
    for copy in sends:
        copy.wait_send()


def store_kernel(lens_ref, y_ref, kv_ref, cache_ref, y_out_ref, cache_buf, k_out_ref, v_out_ref, y_sem, out_sem):
    k_buf, v_buf = cache_buf.at[0], cache_buf.at[1]
    batch, pos_local, hd = k_buf.shape
    first_pos = lax.axis_index("sq") * pos_local
    row = lax.broadcasted_iota(jnp.int32, (16, hd), 0)
    pairs = ((k_buf, k_out_ref), (v_buf, v_out_ref))

    def write(c):
        at = pl.ds(pl.multiple_of(c * SEQS, SEQS), SEQS)
        return [pltpu.make_async_copy(buf.at[at], out.at[at], out_sem.at[w, c]) for w, (buf, out) in enumerate(pairs)]

    def replace(c, _):
        for i in range(SEQS):
            b = c * SEQS + i
            pos = lens_ref[b] - first_pos
            base = pl.multiple_of(lax.div(jnp.clip(pos, 0, pos_local - 1), 16) * 16, 16)
            here = row + base == pos
            for which, (buf, _) in enumerate(pairs):
                old = buf[b, pl.ds(base, 16), :].astype(jnp.float32)
                new = kv_ref[which, pl.ds(b, 1), :]
                buf[b, pl.ds(base, 16), :] = jnp.where(here, new, old).astype(jnp.bfloat16)
        for copy in write(c):
            copy.start()
        return 0

    def drain(c, _):
        for copy in write(c):
            copy.wait()
        return 0

    y_copy = pltpu.make_async_copy(y_ref, y_out_ref, y_sem)
    y_copy.start()
    lax.fori_loop(0, batch // SEQS, replace, 0)
    lax.fori_loop(0, batch // SEQS, drain, 0)
    y_copy.wait()


def solution(mesh):
    nx, ny = mesh.shape["sq"] // 2, mesh.shape["tp"]

    def local_step(hidden, cache_lens, k_cache, v_cache, ln_gain, ln_bias, w_query, b_query, w_kv, b_kv, w_out, b_out):
        batch, pos_local, hd = k_cache.shape
        d_model, depth = w_query.shape
        heads = depth // hd
        rows, cols = batch // (2 * nx), d_model // ny
        width = depth + hd
        half = cols // 2
        f32, bf16, dma, vmem_buf = jnp.float32, jnp.bfloat16, pltpu.SemaphoreType.DMA, pltpu.VMEM
        smem, vmem, hbm = (pl.BlockSpec(memory_space=m) for m in (pltpu.SMEM, pltpu.VMEM, pl.ANY))
        out_hidden, key_val, caches = pl.pallas_call(
            functools.partial(decode_kernel, (nx, ny, heads, rows, cols, pos_local)),
            out_shape=[
                vmem_buf((batch, d_model), bf16),
                vmem_buf((2, batch, hd), f32),
                vmem_buf((2,) + k_cache.shape, bf16),
            ],
            in_specs=[smem] + [vmem] * 5 + [hbm] * 6,
            out_specs=[vmem] * 3,
            scratch_shapes=[
                vmem_buf((W_SLOTS * TALL, depth), bf16),
                vmem_buf((W_SLOTS, TALL, 2 * hd), bf16),
                vmem_buf((batch * 16, hd), f32),
                vmem_buf((batch, width), f32),
                vmem_buf((SEQS * 16, hd), f32),
                vmem_buf((SEQS * 16, pos_local), f32),
                vmem_buf((SEQS * 16, pos_local), f32),
                vmem_buf((batch, hd), f32),
                vmem_buf((batch, hd), f32),
                vmem_buf((4, rows, width), f32),
                vmem_buf((3, rows, width), f32),
                vmem_buf((rows, depth), bf16),
                vmem_buf((4, 2, rows, half), f32),
                vmem_buf((3, 2, rows, half), f32),
                vmem_buf((rows, cols), bf16),
                vmem_buf((batch, d_model), f32),
                dma((4,)),
                dma((2, d_model // TALL)),
                dma((2, batch // SEQS)),
                dma((4,)),
                dma,
                dma((4,)),
                dma((4,)),
                dma((3,)),
                dma((3,)),
                dma((3, 2)),
                dma((3, 2)),
                dma((2, 15)),
                dma((2, 15)),
                dma((2, 16)),
                dma((2, 16)),
            ],
            compiler_params=pltpu.CompilerParams(collective_id=0, has_side_effects=True, vmem_limit_bytes=27 * 1024 * 1024),
            name="decode",
        )(
            cache_lens,
            ln_gain.reshape(1, d_model),
            ln_bias.reshape(1, d_model),
            b_query,
            b_kv.reshape(1, 2 * hd),
            b_out.reshape(1, d_model),
            hidden,
            w_query,
            w_kv,
            w_out,
            k_cache,
            v_cache,
        )
        out_hidden, _, key_new, val_new = pl.pallas_call(
            store_kernel,
            out_shape=[
                jax.ShapeDtypeStruct((batch, d_model), bf16),
                vmem_buf((2,) + k_cache.shape, bf16),
                jax.ShapeDtypeStruct(k_cache.shape, bf16),
                jax.ShapeDtypeStruct(v_cache.shape, bf16),
            ],
            in_specs=[smem] + [vmem] * 3,
            out_specs=[hbm, vmem, hbm, hbm],
            input_output_aliases={3: 1},
            scratch_shapes=[dma, dma((2, batch // SEQS))],
            compiler_params=pltpu.CompilerParams(vmem_limit_bytes=1 * 1024 * 1024),
            name="store",
        )(cache_lens, out_hidden, key_val, caches)
        return out_hidden, key_new, val_new

    cache_spec = P("dp", "sq", None)
    row_spec = P("dp", None)
    in_specs = (row_spec, P("dp"), cache_spec, cache_spec, P(None), P(None), P(None, "tp"), P("tp"), P(None, None), P(None), P("tp", None), P(None))
    out_specs = (row_spec, cache_spec, cache_spec)
    return jax.shard_map(local_step, mesh=mesh, in_specs=in_specs, out_specs=out_specs, check_vma=False)
```

```python
import functools

import jax
import jax.numpy as jnp
from jax import lax
from jax.experimental import pallas as pl
from jax.experimental.pallas import tpu as pltpu
from jax.sharding import PartitionSpec as P

MESH = pl.DeviceIdType.MESH
LANES = 128
SEQS = 32
TALL = 1024
WIDE = 512
STORE_SEQS = 16
EARLY = 3
W_SLOTS = 3


def merge_into(dst, part_a, part_b, heads):
    stat_a, stat_b = part_a(heads), part_b(heads)
    top = jnp.maximum(stat_a, stat_b)
    exp_a, exp_b = jnp.exp(stat_a - top), jnp.exp(stat_b - top)
    sums = stat_a * pltpu.roll(exp_a, 64, 1) + stat_b * pltpu.roll(exp_b, 64, 1)
    lane = lax.broadcasted_iota(jnp.int32, top.shape, 1)
    stat = jnp.where(lane < 64, top, sums)
    for n in range(heads):
        dst[:, n * LANES : (n + 1) * LANES] = part_a(n) * exp_a[:, n : n + 1] + part_b(n) * exp_b[:, n : n + 1]
    dst[:, heads * LANES :] = stat


def decode_kernel(
    dims,
    lens_ref,
    gain_ref,
    bias_ref,
    b_query_ref,
    b_kv_ref,
    b_out_ref,
    hidden_ref,
    w_query_ref,
    w_kv_ref,
    w_out_ref,
    k_ref,
    v_ref,
    out_ref,
    kv_buf,
    cache_buf,
    w_buf,
    wkv_buf,
    q_buf,
    part_buf,
    o_buf,
    s_buf0,
    s_buf1,
    stat_buf,
    stat_buf2,
    pair_buf,
    x_buf,
    att_buf,
    proj_buf,
    y_buf,
    hid_buf,
    gather_buf,
    h_sem,
    w_sem,
    in_sem,
    wo_sem,
    hid_sem,
    pair_send,
    pair_recv,
    x_send,
    x_recv,
    y_send,
    y_recv,
    g_send,
    g_recv,
    d_send,
    d_recv,
):
    nx, ny, heads, rows, cols, pos_local = dims
    k_buf, v_buf = cache_buf.at[0], cache_buf.at[1]
    batch, d_model = out_ref.shape
    hd, seqs = LANES, SEQS
    half = cols // 2
    depth = heads * hd
    steps = batch // seqs
    blocks = d_model // TALL
    sq = lax.axis_index("sq")
    y = lax.axis_index("tp")
    x = sq // 2
    core = sq % 2
    step = 1 - 2 * core
    first_pos = sq * pos_local
    scale = hd ** -0.5
    lowest = float(jnp.finfo(jnp.float32).min)

    def wrap(value, size):
        return lax.rem(value + 2 * size, size)

    x_fwd, x_bwd, x_opp = wrap(x + step, nx), wrap(x - step, nx), wrap(x + 2, nx)
    y_fwd, y_bwd, y_opp = wrap(y + step, ny), wrap(y - step, ny), wrap(y + 2, ny)
    to_pair = {"sq": x * 2 + 1 - core}
    to_x_fwd, to_x_bwd = {"sq": x_fwd * 2 + core}, {"sq": x_bwd * 2 + core}
    to_y_fwd, to_y_bwd = {"tp": y_fwd}, {"tp": y_bwd}

    barrier = pltpu.get_barrier_semaphore()
    for peer in (to_pair, to_x_fwd, to_x_bwd, to_y_fwd, to_y_bwd):
        pl.semaphore_signal(barrier, inc=1, device_id=peer, device_id_type=MESH)

    h_buf = out_ref

    def w_copies(k):
        slot, at = k % W_SLOTS, pl.ds(k * TALL, TALL)
        return (
            pltpu.make_async_copy(w_query_ref.at[at, :], w_buf.at[pl.ds(slot * TALL, TALL), :], w_sem.at[0, k]),
            pltpu.make_async_copy(w_kv_ref.at[at, :], wkv_buf.at[slot], w_sem.at[1, k]),
        )

    def block_row(i):
        slot, mine = i // 2, i % 2
        sign = step * (1 - 2 * mine)
        shift = 2 * ((3 - slot) // 3) + sign * (slot * (3 - slot) * (3 - 2 * slot) // 2)
        owner = wrap(x + shift, nx) * 2 + (1 - core) * (1 - mine) + core * mine
        return owner * rows

    def step_rows(c):
        per = rows // seqs
        return pl.multiple_of(block_row(c // per) + (c % per) * seqs, seqs)

    def read(c):
        at = pl.ds(step_rows(c), seqs)
        return (
            pltpu.make_async_copy(k_ref.at[at], k_buf.at[at], in_sem.at[0, c]),
            pltpu.make_async_copy(v_ref.at[at], v_buf.at[at], in_sem.at[1, c]),
        )

    h_parts = 4
    h_rows = batch // h_parts
    h_copies = [
        pltpu.make_async_copy(hidden_ref.at[pl.ds(j * h_rows, h_rows), :], h_buf.at[pl.ds(j * h_rows, h_rows), :], h_sem.at[j])
        for j in range(h_parts)
    ]
    for copy in h_copies:
        copy.start()

    def start_weights(k, _):
        for copy in w_copies(k):
            copy.start()
        return 0

    def start_caches(c, _):
        for copy in read(c):
            copy.start()
        return 0

    lax.fori_loop(0, W_SLOTS, start_weights, 0)
    lax.fori_loop(0, EARLY, start_caches, 0)
    q_buf[...] = jnp.zeros_like(q_buf)

    tiles = d_model // hd

    def lane_tiles(at):
        return [h_buf[at, t * hd : (t + 1) * hd].astype(jnp.float32) for t in range(tiles)]

    def add_up(values):
        while len(values) > 1:
            values = [sum(values[i : i + 2]) for i in range(0, len(values), 2)]
        return values[0]

    def rows16(r):
        return pl.ds(pl.multiple_of(r * 16, 16), 16)

    def sum_rows(r, _):
        stat_buf[rows16(r), :] = add_up(lane_tiles(rows16(r)))
        return 0

    def spread_rows(r, _):
        mean_val = stat_buf[rows16(r), :]
        stat_buf2[rows16(r), :] = add_up([(v - mean_val) * (v - mean_val) for v in lane_tiles(rows16(r))])
        return 0

    def norm_rows(r, _):
        at = rows16(r)
        mean_val, inv = stat_buf[at, :], stat_buf2[at, :]
        for t in range(tiles):
            cols = slice(t * hd, (t + 1) * hd)
            normed = (h_buf[at, cols].astype(jnp.float32) - mean_val) * inv
            h_buf[at, cols] = (normed * gain_ref[:, cols] + bias_ref[:, cols]).astype(jnp.bfloat16)
        return 0

    def row_means(buf):
        return jnp.broadcast_to(jnp.sum(buf[...], axis=-1, keepdims=True) * (1.0 / d_model), buf.shape)

    for j, copy in enumerate(h_copies):
        copy.wait()
        lax.fori_loop(j * h_rows // 16, (j + 1) * h_rows // 16, sum_rows, 0, unroll=2)
    stat_buf[...] = row_means(stat_buf)
    lax.fori_loop(0, batch // 16, spread_rows, 0, unroll=2)
    stat_buf2[...] = lax.rsqrt(row_means(stat_buf2) + 1e-5)
    lax.fori_loop(0, batch // 16, norm_rows, 0, unroll=2)

    y_order = (y_opp, y_bwd, y_fwd, y)

    def wo_copy(k):
        src = w_out_ref.at[:, pl.ds(pl.multiple_of(y_order[k] * cols, cols), cols)]
        return pltpu.make_async_copy(src, w_buf.at[pl.ds((k % 2) * depth, depth), :], wo_sem.at[k])

    for k in range(blocks):
        for copy in w_copies(k):
            copy.wait()
        h_cols, slot = h_buf[:, k * TALL : (k + 1) * TALL], k % W_SLOTS
        kv = jnp.dot(h_cols, wkv_buf[slot], preferred_element_type=jnp.float32)
        for e in range(2):
            part = kv[:, e * hd : (e + 1) * hd]
            kv_buf[e] = part if k == 0 else kv_buf[e] + part
        for n in range(0, depth, WIDE):
            w_block = w_buf[slot * TALL : (slot + 1) * TALL, n : n + WIDE]
            part = jnp.dot(h_cols, w_block, preferred_element_type=jnp.float32)
            part_buf[:, n : n + WIDE] = part if k == 0 else part_buf[:, n : n + WIDE] + part
        if k + W_SLOTS < blocks:
            for copy in w_copies(k + W_SLOTS):
                copy.start()
        if k + W_SLOTS == blocks - 1:
            lax.fori_loop(EARLY, steps, start_caches, 0)
    for e in range(2):
        new = kv_buf[e] + b_kv_ref[:, e * hd : (e + 1) * hd]
        kv_buf[e] = new.astype(jnp.bfloat16).astype(jnp.float32)
    for n in range(heads):
        new = part_buf[:, n * hd : (n + 1) * hd] + b_query_ref[n * hd : (n + 1) * hd].reshape(1, hd)
        q_buf[pl.ds(n, batch, stride=16), :] = new.astype(jnp.bfloat16).astype(jnp.float32)
    hid_copy = pltpu.make_async_copy(
        hidden_ref.at[pl.ds(pl.multiple_of(sq * rows, rows), rows), pl.ds(pl.multiple_of(y * cols, cols), cols)], hid_buf, hid_sem
    )
    hid_copy.start()
    for k in range(2):
        wo_copy(k).start()

    zero = jnp.zeros((16, hd), jnp.bfloat16)
    at_pos = lax.broadcasted_iota(jnp.int32, (16, pos_local), 1) + first_pos
    row = lax.broadcasted_iota(jnp.int32, (16, hd), 0)
    lane = lax.broadcasted_iota(jnp.int32, (16, hd), 1)
    pick_m = (lane == row) & (row < heads)
    pick_l = (lane == row + 64) & (row < heads)

    def score(c, s_buf):
        for copy in read(c):
            copy.wait()
        b0 = step_rows(c)
        for i in range(0, seqs, 2):
            q0 = q_buf[pl.ds(pl.multiple_of(b0 * 16 + i * 16, 16), 16), :].astype(jnp.bfloat16)
            q1 = q_buf[pl.ds(pl.multiple_of(b0 * 16 + i * 16 + 16, 16), 16), :].astype(jnp.bfloat16)
            q2 = jnp.concatenate([jnp.concatenate([q0, zero], axis=1), jnp.concatenate([zero, q1], axis=1)], axis=0)
            k2 = jnp.concatenate([k_buf[b0 + i], k_buf[b0 + i + 1]], axis=1)
            s2 = lax.dot_general(q2, k2, (((1,), (1,)), ((), ())), preferred_element_type=jnp.float32)
            s_buf[i * 16 : i * 16 + 32, :] = s2 * scale

    def combine(c, s_buf):
        b0 = step_rows(c)
        for i in range(0, seqs, 2):
            v2 = jnp.concatenate([v_buf[b0 + i], v_buf[b0 + i + 1]], axis=1)
            valid = jnp.concatenate([at_pos < lens_ref[b0 + i], at_pos < lens_ref[b0 + i + 1]], axis=0)
            s2 = jnp.where(valid, s_buf[i * 16 : i * 16 + 32, :], lowest)
            top = jnp.max(s2, axis=-1, keepdims=True)
            p2 = jnp.where(valid, jnp.exp(s2 - top), 0.0)
            total = jnp.sum(p2, axis=-1, keepdims=True)
            o2 = jnp.dot(p2.astype(jnp.bfloat16), v2, preferred_element_type=jnp.float32)
            for e in range(2):
                part = slice(e * 16, e * 16 + 16)
                stat = jnp.where(pick_m, top[part], 0.0) + jnp.where(pick_l, total[part], 0.0)
                stat = jnp.sum(stat, axis=0, keepdims=True)
                o_buf[(i + e) * 16 : (i + e) * 16 + 16, :] = jnp.where(row == heads, stat, o2[part, e * hd : (e + 1) * hd])
        for n in range(heads + 1):
            part_buf[pl.ds(b0, seqs), n * hd : (n + 1) * hd] = o_buf[pl.ds(n, seqs, stride=16), :]

    sends = []

    def remote(src, dst, ssem, rsem, peer):
        return pltpu.make_async_remote_copy(
            src_ref=src, dst_ref=dst, send_sem=ssem, recv_sem=rsem, device_id=peer, device_id_type=MESH
        )

    def send(*args):
        copy = remote(*args)
        copy.start()
        sends.append(copy)
        return copy

    def part_at(i):
        return pl.ds(pl.multiple_of(block_row(i), rows), rows)

    def of_part(i):
        return lambda n: part_buf[part_at(i), n * hd : (n + 1) * hd]

    def of(ref):
        return lambda n: ref[:, n * hd : (n + 1) * hd]

    pair = [remote(part_buf.at[part_at(2 * k), :], pair_buf.at[k], pair_send.at[k], pair_recv.at[k], to_pair) for k in range(4)]
    x_o = remote(pair_buf.at[0], x_buf.at[0], x_send.at[0], x_recv.at[0], to_x_fwd)
    x_b = remote(pair_buf.at[1], x_buf.at[1], x_send.at[1], x_recv.at[1], to_x_bwd)
    x_a = remote(pair_buf.at[2], x_buf.at[2], x_send.at[2], x_recv.at[2], to_x_fwd)
    sends.extend(pair + [x_o, x_b, x_a])

    def after_block(i):
        slot = i // 2
        if i % 2 == 0:
            pair[slot].start()
            return
        pair[slot].wait_recv()
        merge_into(pair_buf.at[slot], of_part(i), of(pair_buf.at[slot]), heads)
        if slot == 0:
            x_o.start()
        elif slot == 1:
            x_b.start()
        elif slot == 2:
            x_o.wait_recv()
            merge_into(pair_buf.at[2], of(pair_buf.at[2]), of(x_buf.at[0]), heads)
            x_a.start()

    pl.semaphore_wait(barrier, 5)
    score(0, s_buf0)

    def two_blocks(t, _):
        c = t * 2
        score(c + 1, s_buf1)
        combine(c, s_buf0)
        for j in range(3):
            pl.when(t == j)(functools.partial(after_block, 2 * j))
        score(c + 2, s_buf0)
        combine(c + 1, s_buf1)
        for j in range(3):
            pl.when(t == j)(functools.partial(after_block, 2 * j + 1))
        return 0

    lax.fori_loop(0, steps // 2 - 1, two_blocks, 0)
    score(steps - 1, s_buf1)
    combine(steps - 2, s_buf0)
    after_block(6)
    combine(steps - 1, s_buf1)

    own = pl.multiple_of(sq * rows, rows)
    k_new, v_new = kv_buf[0, pl.ds(own, rows), :], kv_buf[1, pl.ds(own, rows), :]
    new_lane = lax.broadcasted_iota(jnp.int32, (rows, hd), 1)
    new_stat = jnp.where((new_lane >= 64) & (new_lane < 64 + heads), 1.0, 0.0)
    for n in range(heads):
        s_new = jnp.sum(q_buf[pl.ds(own * 16 + n, rows, stride=16), :] * k_new, axis=-1, keepdims=True) * scale
        new_stat = jnp.where(new_lane == n, s_new, new_stat)

    after_block(7)
    total = pair_buf.at[3]
    merge_into(total, of(total), lambda n: new_stat if n == heads else v_new, heads)
    x_b.wait_recv()
    merge_into(total, of(total), of(x_buf.at[1]), heads)
    x_a.wait_recv()
    merge_into(total, of(total), of(x_buf.at[2]), heads)
    stat = total[:, depth:]
    for n in range(heads):
        block = slice(n * hd, (n + 1) * hd)
        att_buf[:, block] = (total[:, block] / stat[:, 64 + n : 65 + n]).astype(jnp.bfloat16)

    def project(k, h):
        w_block = w_buf[(k % 2) * depth : (k % 2 + 1) * depth, h * half : (h + 1) * half]
        return jnp.dot(att_buf[...], w_block, preferred_element_type=jnp.float32)

    y_o, y_b, y_a = [None, None], [None, None], [None, None]
    for k in range(4):
        wo_copy(k).wait()
        for h in range(2):
            part = project(k, h)
            if k < 2:
                proj_buf[k, h] = part
                copy = send(proj_buf.at[k, h], y_buf.at[k, h], y_send.at[k, h], y_recv.at[k, h], (to_y_fwd, to_y_bwd)[k])
                (y_o, y_b)[k][h] = copy
            elif k == 2:
                proj_buf[2, h] = part
            else:
                if h == 0:
                    hid_copy.wait()
                own_cols = pl.ds(pl.multiple_of(y * cols + h * half, half), half)
                proj_buf[3, h] = part + hid_buf[:, h * half : (h + 1) * half].astype(jnp.float32) + b_out_ref[:, own_cols]
        if k < 2:
            wo_copy(k + 2).start()
        if k == 2:
            for h in range(2):
                y_o[h].wait_recv()
                proj_buf[2, h] = proj_buf[2, h] + y_buf[0, h]
                y_a[h] = send(proj_buf.at[2, h], y_buf.at[2, h], y_send.at[2, h], y_recv.at[2, h], to_y_fwd)

    def place(xt, yt, ct, h):
        row = pl.multiple_of((xt * 2 + ct) * rows, rows)
        col = pl.multiple_of(yt * cols + h * half, half)
        return pl.ds(row, rows), pl.ds(col, half)

    xs = (x, x_bwd, x_fwd, x_opp)
    ys = (y, y_bwd, y_fwd, y_opp)
    x_peers, y_peers = (to_x_fwd, to_x_bwd), (to_y_fwd, to_y_bwd)
    gathers = {}
    pairs = {}

    def spot(h, first, second, ct=None):
        ct = core if ct is None else ct
        if h == 0:
            return place(xs[first], ys[second], ct, h)
        return place(xs[second], ys[first], ct, h)

    def piece(h, first, second):
        return gather_buf.at[spot(h, first, second)]

    def ring_send(h, first, second, slot, phase):
        peers = (x_peers, y_peers) if h == 0 else (y_peers, x_peers)
        peer = peers[phase][1 if slot == 2 else 0]
        index = slot - 1 if phase == 0 else 3 + first * 3 + slot - 1
        key = (h, phase, first if phase else 0, slot)
        ref = piece(h, first, second)
        gathers[key] = send(ref, ref, g_send.at[h, index], g_recv.at[h, index], peer)

    def pair_forward(h, first, second):
        ref = piece(h, first, second)
        index = first * 4 + second
        pairs[(h, first, second)] = send(ref, ref, d_send.at[h, index], d_recv.at[h, index], to_pair)

    def convert(where):
        out_ref[where] = gather_buf[where].astype(jnp.bfloat16)

    def mirrored(slot):
        return (0, 2, 1, 3)[slot]

    todo = []

    def drain(limit):
        while len(todo) > limit:
            h, first, second = todo.pop(0)
            pairs[(h, first, second)].wait_recv()
            convert(spot(h, mirrored(first), mirrored(second), 1 - core))

    def have(h, first, second):
        pair_forward(h, first, second)
        convert(spot(h, first, second))
        todo.append((h, first, second))
        drain(4)

    for h in range(2):
        y_b[h].wait_recv()
        part = proj_buf[3, h] + y_buf[1, h]
        y_a[h].wait_recv()
        gather_buf[spot(h, 0, 0)] = part + y_buf[2, h]
        ring_send(h, 0, 0, 1, 0)
        ring_send(h, 0, 0, 2, 0)
        pair_forward(h, 0, 0)
    for h in range(2):
        ring_send(h, 0, 0, 1, 1)
        ring_send(h, 0, 0, 2, 1)
        convert(spot(h, 0, 0))
        todo.append((h, 0, 0))

    def arrived(h, first, second):
        if second == 0:
            gathers[(h, 0, 0, first)].wait_recv()
            if first == 1:
                ring_send(h, 1, 0, 3, 0)
            ring_send(h, first, 0, 1, 1)
            ring_send(h, first, 0, 2, 1)
        else:
            gathers[(h, 1, first, second)].wait_recv()
            if second == 1:
                ring_send(h, first, 1, 3, 1)
        have(h, first, second)

    order = [(1, 0), (2, 0), (0, 1), (0, 2), (3, 0), (1, 1), (0, 3), (2, 1), (1, 2), (1, 3), (2, 2), (3, 1), (2, 3), (3, 2), (3, 3)]
    for first, second in order:
        for h in range(2):
            arrived(h, first, second)
    drain(0)
    for copy in sends:
        copy.wait_send()


def store_kernel(lens_ref, y_ref, kv_ref, cache_ref, y_out_ref, cache_buf, k_out_ref, v_out_ref, y_sem, out_sem):
    k_buf, v_buf = cache_buf.at[0], cache_buf.at[1]
    batch, pos_local, hd = k_buf.shape
    first_pos = lax.axis_index("sq") * pos_local
    row = lax.broadcasted_iota(jnp.int32, (16, hd), 0)
    pairs = ((k_buf, k_out_ref), (v_buf, v_out_ref))

    def write(c):
        at = pl.ds(pl.multiple_of(c * STORE_SEQS, STORE_SEQS), STORE_SEQS)
        return [pltpu.make_async_copy(buf.at[at], out.at[at], out_sem.at[w, c]) for w, (buf, out) in enumerate(pairs)]

    def replace(c, _):
        for i in range(STORE_SEQS):
            b = c * STORE_SEQS + i
            pos = lens_ref[b] - first_pos
            base = pl.multiple_of(lax.div(jnp.clip(pos, 0, pos_local - 1), 16) * 16, 16)
            here = row + base == pos
            for which, (buf, _) in enumerate(pairs):
                old = buf[b, pl.ds(base, 16), :].astype(jnp.float32)
                new = kv_ref[which, pl.ds(b, 1), :]
                buf[b, pl.ds(base, 16), :] = jnp.where(here, new, old).astype(jnp.bfloat16)
        for copy in write(c):
            copy.start()
        return 0

    def drain(c, _):
        for copy in write(c):
            copy.wait()
        return 0

    y_copy = pltpu.make_async_copy(y_ref, y_out_ref, y_sem)
    y_copy.start()
    lax.fori_loop(0, batch // STORE_SEQS, replace, 0)
    lax.fori_loop(0, batch // STORE_SEQS, drain, 0)
    y_copy.wait()


def solution(mesh):
    nx, ny = mesh.shape["sq"] // 2, mesh.shape["tp"]

    def local_step(hidden, cache_lens, k_cache, v_cache, ln_gain, ln_bias, w_query, b_query, w_kv, b_kv, w_out, b_out):
        batch, pos_local, hd = k_cache.shape
        d_model, depth = w_query.shape
        heads = depth // hd
        rows, cols = batch // (2 * nx), d_model // ny
        width = depth + hd
        half = cols // 2
        f32, bf16, dma, vmem_buf = jnp.float32, jnp.bfloat16, pltpu.SemaphoreType.DMA, pltpu.VMEM
        smem, vmem, hbm = (pl.BlockSpec(memory_space=m) for m in (pltpu.SMEM, pltpu.VMEM, pl.ANY))
        out_hidden, key_val, caches = pl.pallas_call(
            functools.partial(decode_kernel, (nx, ny, heads, rows, cols, pos_local)),
            out_shape=[
                vmem_buf((batch, d_model), bf16),
                vmem_buf((2, batch, hd), f32),
                vmem_buf((2,) + k_cache.shape, bf16),
            ],
            in_specs=[smem] + [vmem] * 5 + [hbm] * 6,
            out_specs=[vmem] * 3,
            scratch_shapes=[
                vmem_buf((W_SLOTS * TALL, depth), bf16),
                vmem_buf((W_SLOTS, TALL, 2 * hd), bf16),
                vmem_buf((batch * 16, hd), f32),
                vmem_buf((batch, width), f32),
                vmem_buf((SEQS * 16, hd), f32),
                vmem_buf((SEQS * 16, pos_local), f32),
                vmem_buf((SEQS * 16, pos_local), f32),
                vmem_buf((batch, hd), f32),
                vmem_buf((batch, hd), f32),
                vmem_buf((4, rows, width), f32),
                vmem_buf((3, rows, width), f32),
                vmem_buf((rows, depth), bf16),
                vmem_buf((4, 2, rows, half), f32),
                vmem_buf((3, 2, rows, half), f32),
                vmem_buf((rows, cols), bf16),
                vmem_buf((batch, d_model), f32),
                dma((4,)),
                dma((2, d_model // TALL)),
                dma((2, batch // SEQS)),
                dma((4,)),
                dma,
                dma((4,)),
                dma((4,)),
                dma((3,)),
                dma((3,)),
                dma((3, 2)),
                dma((3, 2)),
                dma((2, 15)),
                dma((2, 15)),
                dma((2, 16)),
                dma((2, 16)),
            ],
            compiler_params=pltpu.CompilerParams(collective_id=0, has_side_effects=True, vmem_limit_bytes=28 * 1024 * 1024),
            name="decode",
        )(
            cache_lens,
            ln_gain.reshape(1, d_model),
            ln_bias.reshape(1, d_model),
            b_query,
            b_kv.reshape(1, 2 * hd),
            b_out.reshape(1, d_model),
            hidden,
            w_query,
            w_kv,
            w_out,
            k_cache,
            v_cache,
        )
        out_hidden, _, key_new, val_new = pl.pallas_call(
            store_kernel,
            out_shape=[
                jax.ShapeDtypeStruct((batch, d_model), bf16),
                vmem_buf((2,) + k_cache.shape, bf16),
                jax.ShapeDtypeStruct(k_cache.shape, bf16),
                jax.ShapeDtypeStruct(v_cache.shape, bf16),
            ],
            in_specs=[smem] + [vmem] * 3,
            out_specs=[hbm, vmem, hbm, hbm],
            input_output_aliases={3: 1},
            scratch_shapes=[dma, dma((2, batch // STORE_SEQS))],
            compiler_params=pltpu.CompilerParams(vmem_limit_bytes=1 * 1024 * 1024),
            name="store",
        )(cache_lens, out_hidden, key_val, caches)
        return out_hidden, key_new, val_new

    cache_spec = P("dp", "sq", None)
    row_spec = P("dp", None)
    in_specs = (row_spec, P("dp"), cache_spec, cache_spec, P(None), P(None), P(None, "tp"), P("tp"), P(None, None), P(None), P("tp", None), P(None))
    out_specs = (row_spec, cache_spec, cache_spec)
    return jax.shard_map(local_step, mesh=mesh, in_specs=in_specs, out_specs=out_specs, check_vma=False)
```

```python
import functools

import jax
import jax.numpy as jnp
from jax import lax
from jax.experimental import pallas as pl
from jax.experimental.pallas import tpu as pltpu
from jax.sharding import PartitionSpec as P

MESH = pl.DeviceIdType.MESH
LANES = 128
SEQS = 32
TALL = 768
WIDE = 512
STORE_SEQS = 16
EARLY = 3
W_SLOTS = 4


def merge_into(dst, part_a, part_b, heads):
    stat_a, stat_b = part_a(heads), part_b(heads)
    top = jnp.maximum(stat_a, stat_b)
    exp_a, exp_b = jnp.exp(stat_a - top), jnp.exp(stat_b - top)
    sums = stat_a * pltpu.roll(exp_a, 64, 1) + stat_b * pltpu.roll(exp_b, 64, 1)
    lane = lax.broadcasted_iota(jnp.int32, top.shape, 1)
    stat = jnp.where(lane < 64, top, sums)
    for n in range(heads):
        dst[:, n * LANES : (n + 1) * LANES] = part_a(n) * exp_a[:, n : n + 1] + part_b(n) * exp_b[:, n : n + 1]
    dst[:, heads * LANES :] = stat


def decode_kernel(
    dims,
    lens_ref,
    gain_ref,
    bias_ref,
    b_query_ref,
    b_kv_ref,
    b_out_ref,
    hidden_ref,
    w_query_ref,
    w_kv_ref,
    w_out_ref,
    k_ref,
    v_ref,
    out_ref,
    kv_buf,
    cache_buf,
    w_buf,
    wkv_buf,
    q_buf,
    part_buf,
    o_buf,
    s_buf0,
    s_buf1,
    stat_buf,
    stat_buf2,
    pair_buf,
    x_buf,
    att_buf,
    proj_buf,
    y_buf,
    hid_buf,
    gather_buf,
    h_sem,
    w_sem,
    in_sem,
    wo_sem,
    hid_sem,
    pair_send,
    pair_recv,
    x_send,
    x_recv,
    y_send,
    y_recv,
    g_send,
    g_recv,
    d_send,
    d_recv,
):
    nx, ny, heads, rows, cols, pos_local = dims
    k_buf, v_buf = cache_buf.at[0], cache_buf.at[1]
    batch, d_model = out_ref.shape
    hd, seqs = LANES, SEQS
    half = cols // 2
    depth = heads * hd
    steps = batch // seqs
    blocks = d_model // TALL
    sq = lax.axis_index("sq")
    y = lax.axis_index("tp")
    x = sq // 2
    core = sq % 2
    step = 1 - 2 * core
    first_pos = sq * pos_local
    scale = hd ** -0.5
    lowest = float(jnp.finfo(jnp.float32).min)

    def wrap(value, size):
        return lax.rem(value + 2 * size, size)

    x_fwd, x_bwd, x_opp = wrap(x + step, nx), wrap(x - step, nx), wrap(x + 2, nx)
    y_fwd, y_bwd, y_opp = wrap(y + step, ny), wrap(y - step, ny), wrap(y + 2, ny)
    to_pair = {"sq": x * 2 + 1 - core}
    to_x_fwd, to_x_bwd = {"sq": x_fwd * 2 + core}, {"sq": x_bwd * 2 + core}
    to_y_fwd, to_y_bwd = {"tp": y_fwd}, {"tp": y_bwd}

    barrier = pltpu.get_barrier_semaphore()
    for peer in (to_pair, to_x_fwd, to_x_bwd, to_y_fwd, to_y_bwd):
        pl.semaphore_signal(barrier, inc=1, device_id=peer, device_id_type=MESH)

    h_buf = out_ref

    def w_copies(k):
        slot, at = k % W_SLOTS, pl.ds(k * TALL, TALL)
        return (
            pltpu.make_async_copy(w_query_ref.at[at, :], w_buf.at[pl.ds(slot * TALL, TALL), :], w_sem.at[0, k]),
            pltpu.make_async_copy(w_kv_ref.at[at, :], wkv_buf.at[slot], w_sem.at[1, k]),
        )

    def block_row(i):
        slot, mine = i // 2, i % 2
        sign = step * (1 - 2 * mine)
        shift = 2 * ((3 - slot) // 3) + sign * (slot * (3 - slot) * (3 - 2 * slot) // 2)
        owner = wrap(x + shift, nx) * 2 + (1 - core) * (1 - mine) + core * mine
        return owner * rows

    def step_rows(c):
        per = rows // seqs
        return pl.multiple_of(block_row(c // per) + (c % per) * seqs, seqs)

    def read(c):
        at = pl.ds(step_rows(c), seqs)
        return (
            pltpu.make_async_copy(k_ref.at[at], k_buf.at[at], in_sem.at[0, c]),
            pltpu.make_async_copy(v_ref.at[at], v_buf.at[at], in_sem.at[1, c]),
        )

    h_parts = 4
    h_rows = batch // h_parts
    h_copies = [
        pltpu.make_async_copy(hidden_ref.at[pl.ds(j * h_rows, h_rows), :], h_buf.at[pl.ds(j * h_rows, h_rows), :], h_sem.at[j])
        for j in range(h_parts)
    ]
    for copy in h_copies:
        copy.start()

    def start_weights(k, _):
        for copy in w_copies(k):
            copy.start()
        return 0

    def start_caches(c, _):
        for copy in read(c):
            copy.start()
        return 0

    lax.fori_loop(0, W_SLOTS, start_weights, 0)
    lax.fori_loop(0, EARLY, start_caches, 0)
    q_buf[...] = jnp.zeros_like(q_buf)

    tiles = d_model // hd

    def lane_tiles(at):
        return [h_buf[at, t * hd : (t + 1) * hd].astype(jnp.float32) for t in range(tiles)]

    def add_up(values):
        while len(values) > 1:
            values = [sum(values[i : i + 2]) for i in range(0, len(values), 2)]
        return values[0]

    def rows16(r):
        return pl.ds(pl.multiple_of(r * 16, 16), 16)

    def sum_rows(r, _):
        stat_buf[rows16(r), :] = add_up(lane_tiles(rows16(r)))
        return 0

    def spread_rows(r, _):
        mean_val = stat_buf[rows16(r), :]
        stat_buf2[rows16(r), :] = add_up([(v - mean_val) * (v - mean_val) for v in lane_tiles(rows16(r))])
        return 0

    def norm_rows(r, _):
        at = rows16(r)
        mean_val, inv = stat_buf[at, :], stat_buf2[at, :]
        for t in range(tiles):
            cols = slice(t * hd, (t + 1) * hd)
            normed = (h_buf[at, cols].astype(jnp.float32) - mean_val) * inv
            h_buf[at, cols] = (normed * gain_ref[:, cols] + bias_ref[:, cols]).astype(jnp.bfloat16)
        return 0

    def row_means(buf):
        return jnp.broadcast_to(jnp.sum(buf[...], axis=-1, keepdims=True) * (1.0 / d_model), buf.shape)

    for j, copy in enumerate(h_copies):
        copy.wait()
        lax.fori_loop(j * h_rows // 16, (j + 1) * h_rows // 16, sum_rows, 0, unroll=2)
    stat_buf[...] = row_means(stat_buf)
    lax.fori_loop(0, batch // 16, spread_rows, 0, unroll=2)
    stat_buf2[...] = lax.rsqrt(row_means(stat_buf2) + 1e-5)
    lax.fori_loop(0, batch // 16, norm_rows, 0, unroll=2)

    y_order = (y_opp, y_bwd, y_fwd, y)

    def wo_copy(k):
        src = w_out_ref.at[:, pl.ds(pl.multiple_of(y_order[k] * cols, cols), cols)]
        return pltpu.make_async_copy(src, w_buf.at[pl.ds((k % 2) * depth, depth), :], wo_sem.at[k])

    for k in range(blocks):
        for copy in w_copies(k):
            copy.wait()
        h_cols, slot = h_buf[:, k * TALL : (k + 1) * TALL], k % W_SLOTS
        kv = jnp.dot(h_cols, wkv_buf[slot], preferred_element_type=jnp.float32)
        for e in range(2):
            part = kv[:, e * hd : (e + 1) * hd]
            kv_buf[e] = part if k == 0 else kv_buf[e] + part
        for n in range(0, depth, WIDE):
            w_block = w_buf[slot * TALL : (slot + 1) * TALL, n : n + WIDE]
            part = jnp.dot(h_cols, w_block, preferred_element_type=jnp.float32)
            part_buf[:, n : n + WIDE] = part if k == 0 else part_buf[:, n : n + WIDE] + part
        if k + W_SLOTS < blocks:
            for copy in w_copies(k + W_SLOTS):
                copy.start()
        if k + W_SLOTS == blocks - 1:
            lax.fori_loop(EARLY, steps, start_caches, 0)
    for e in range(2):
        new = kv_buf[e] + b_kv_ref[:, e * hd : (e + 1) * hd]
        kv_buf[e] = new.astype(jnp.bfloat16).astype(jnp.float32)
    for n in range(heads):
        new = part_buf[:, n * hd : (n + 1) * hd] + b_query_ref[n * hd : (n + 1) * hd].reshape(1, hd)
        q_buf[pl.ds(n, batch, stride=16), :] = new.astype(jnp.bfloat16).astype(jnp.float32)
    hid_copy = pltpu.make_async_copy(
        hidden_ref.at[pl.ds(pl.multiple_of(sq * rows, rows), rows), pl.ds(pl.multiple_of(y * cols, cols), cols)], hid_buf, hid_sem
    )
    hid_copy.start()
    for k in range(2):
        wo_copy(k).start()

    zero = jnp.zeros((16, hd), jnp.bfloat16)
    at_pos = lax.broadcasted_iota(jnp.int32, (16, pos_local), 1) + first_pos
    row = lax.broadcasted_iota(jnp.int32, (16, hd), 0)
    lane = lax.broadcasted_iota(jnp.int32, (16, hd), 1)
    pick_m = (lane == row) & (row < heads)
    pick_l = (lane == row + 64) & (row < heads)

    def score(c, s_buf):
        for copy in read(c):
            copy.wait()
        b0 = step_rows(c)
        for i in range(0, seqs, 2):
            q0 = q_buf[pl.ds(pl.multiple_of(b0 * 16 + i * 16, 16), 16), :].astype(jnp.bfloat16)
            q1 = q_buf[pl.ds(pl.multiple_of(b0 * 16 + i * 16 + 16, 16), 16), :].astype(jnp.bfloat16)
            q2 = jnp.concatenate([jnp.concatenate([q0, zero], axis=1), jnp.concatenate([zero, q1], axis=1)], axis=0)
            k2 = jnp.concatenate([k_buf[b0 + i], k_buf[b0 + i + 1]], axis=1)
            s2 = lax.dot_general(q2, k2, (((1,), (1,)), ((), ())), preferred_element_type=jnp.float32)
            s_buf[i * 16 : i * 16 + 32, :] = s2 * scale

    def combine(c, s_buf):
        b0 = step_rows(c)
        for i in range(0, seqs, 2):
            v2 = jnp.concatenate([v_buf[b0 + i], v_buf[b0 + i + 1]], axis=1)
            valid = jnp.concatenate([at_pos < lens_ref[b0 + i], at_pos < lens_ref[b0 + i + 1]], axis=0)
            s2 = jnp.where(valid, s_buf[i * 16 : i * 16 + 32, :], lowest)
            top = jnp.max(s2, axis=-1, keepdims=True)
            p2 = jnp.where(valid, jnp.exp(s2 - top), 0.0)
            total = jnp.sum(p2, axis=-1, keepdims=True)
            o2 = jnp.dot(p2.astype(jnp.bfloat16), v2, preferred_element_type=jnp.float32)
            for e in range(2):
                part = slice(e * 16, e * 16 + 16)
                stat = jnp.where(pick_m, top[part], 0.0) + jnp.where(pick_l, total[part], 0.0)
                stat = jnp.sum(stat, axis=0, keepdims=True)
                o_buf[(i + e) * 16 : (i + e) * 16 + 16, :] = jnp.where(row == heads, stat, o2[part, e * hd : (e + 1) * hd])
        for n in range(heads + 1):
            part_buf[pl.ds(b0, seqs), n * hd : (n + 1) * hd] = o_buf[pl.ds(n, seqs, stride=16), :]

    sends = []

    def remote(src, dst, ssem, rsem, peer):
        return pltpu.make_async_remote_copy(
            src_ref=src, dst_ref=dst, send_sem=ssem, recv_sem=rsem, device_id=peer, device_id_type=MESH
        )

    def send(*args):
        copy = remote(*args)
        copy.start()
        sends.append(copy)
        return copy

    def part_at(i):
        return pl.ds(pl.multiple_of(block_row(i), rows), rows)

    def of_part(i):
        return lambda n: part_buf[part_at(i), n * hd : (n + 1) * hd]

    def of(ref):
        return lambda n: ref[:, n * hd : (n + 1) * hd]

    pair = [remote(part_buf.at[part_at(2 * k), :], pair_buf.at[k], pair_send.at[k], pair_recv.at[k], to_pair) for k in range(4)]
    x_o = remote(pair_buf.at[0], x_buf.at[0], x_send.at[0], x_recv.at[0], to_x_fwd)
    x_b = remote(pair_buf.at[1], x_buf.at[1], x_send.at[1], x_recv.at[1], to_x_bwd)
    x_a = remote(pair_buf.at[2], x_buf.at[2], x_send.at[2], x_recv.at[2], to_x_fwd)
    sends.extend(pair + [x_o, x_b, x_a])

    def after_block(i):
        slot = i // 2
        if i % 2 == 0:
            pair[slot].start()
            return
        pair[slot].wait_recv()
        merge_into(pair_buf.at[slot], of_part(i), of(pair_buf.at[slot]), heads)
        if slot == 0:
            x_o.start()
        elif slot == 1:
            x_b.start()
        elif slot == 2:
            x_o.wait_recv()
            merge_into(pair_buf.at[2], of(pair_buf.at[2]), of(x_buf.at[0]), heads)
            x_a.start()

    pl.semaphore_wait(barrier, 5)
    score(0, s_buf0)

    def two_blocks(t, _):
        c = t * 2
        score(c + 1, s_buf1)
        combine(c, s_buf0)
        for j in range(3):
            pl.when(t == j)(functools.partial(after_block, 2 * j))
        score(c + 2, s_buf0)
        combine(c + 1, s_buf1)
        for j in range(3):
            pl.when(t == j)(functools.partial(after_block, 2 * j + 1))
        return 0

    lax.fori_loop(0, steps // 2 - 1, two_blocks, 0)
    score(steps - 1, s_buf1)
    combine(steps - 2, s_buf0)
    after_block(6)
    combine(steps - 1, s_buf1)

    own = pl.multiple_of(sq * rows, rows)
    k_new, v_new = kv_buf[0, pl.ds(own, rows), :], kv_buf[1, pl.ds(own, rows), :]
    new_lane = lax.broadcasted_iota(jnp.int32, (rows, hd), 1)
    new_stat = jnp.where((new_lane >= 64) & (new_lane < 64 + heads), 1.0, 0.0)
    for n in range(heads):
        s_new = jnp.sum(q_buf[pl.ds(own * 16 + n, rows, stride=16), :] * k_new, axis=-1, keepdims=True) * scale
        new_stat = jnp.where(new_lane == n, s_new, new_stat)

    after_block(7)
    total = pair_buf.at[3]
    merge_into(total, of(total), lambda n: new_stat if n == heads else v_new, heads)
    x_b.wait_recv()
    merge_into(total, of(total), of(x_buf.at[1]), heads)
    x_a.wait_recv()
    merge_into(total, of(total), of(x_buf.at[2]), heads)
    stat = total[:, depth:]
    for n in range(heads):
        block = slice(n * hd, (n + 1) * hd)
        att_buf[:, block] = (total[:, block] / stat[:, 64 + n : 65 + n]).astype(jnp.bfloat16)

    def project(k, h):
        w_block = w_buf[(k % 2) * depth : (k % 2 + 1) * depth, h * half : (h + 1) * half]
        return jnp.dot(att_buf[...], w_block, preferred_element_type=jnp.float32)

    y_o, y_b, y_a = [None, None], [None, None], [None, None]
    for k in range(4):
        wo_copy(k).wait()
        for h in range(2):
            part = project(k, h)
            if k < 2:
                proj_buf[k, h] = part
                copy = send(proj_buf.at[k, h], y_buf.at[k, h], y_send.at[k, h], y_recv.at[k, h], (to_y_fwd, to_y_bwd)[k])
                (y_o, y_b)[k][h] = copy
            elif k == 2:
                proj_buf[2, h] = part
            else:
                if h == 0:
                    hid_copy.wait()
                own_cols = pl.ds(pl.multiple_of(y * cols + h * half, half), half)
                proj_buf[3, h] = part + hid_buf[:, h * half : (h + 1) * half].astype(jnp.float32) + b_out_ref[:, own_cols]
        if k < 2:
            wo_copy(k + 2).start()
        if k == 2:
            for h in range(2):
                y_o[h].wait_recv()
                proj_buf[2, h] = proj_buf[2, h] + y_buf[0, h]
                y_a[h] = send(proj_buf.at[2, h], y_buf.at[2, h], y_send.at[2, h], y_recv.at[2, h], to_y_fwd)

    def place(xt, yt, ct, h):
        row = pl.multiple_of((xt * 2 + ct) * rows, rows)
        col = pl.multiple_of(yt * cols + h * half, half)
        return pl.ds(row, rows), pl.ds(col, half)

    xs = (x, x_bwd, x_fwd, x_opp)
    ys = (y, y_bwd, y_fwd, y_opp)
    x_peers, y_peers = (to_x_fwd, to_x_bwd), (to_y_fwd, to_y_bwd)
    gathers = {}
    pairs = {}

    def spot(h, first, second, ct=None):
        ct = core if ct is None else ct
        if h == 0:
            return place(xs[first], ys[second], ct, h)
        return place(xs[second], ys[first], ct, h)

    def piece(h, first, second):
        return gather_buf.at[spot(h, first, second)]

    def ring_send(h, first, second, slot, phase):
        peers = (x_peers, y_peers) if h == 0 else (y_peers, x_peers)
        peer = peers[phase][1 if slot == 2 else 0]
        index = slot - 1 if phase == 0 else 3 + first * 3 + slot - 1
        key = (h, phase, first if phase else 0, slot)
        ref = piece(h, first, second)
        gathers[key] = send(ref, ref, g_send.at[h, index], g_recv.at[h, index], peer)

    def pair_forward(h, first, second):
        ref = piece(h, first, second)
        index = first * 4 + second
        pairs[(h, first, second)] = send(ref, ref, d_send.at[h, index], d_recv.at[h, index], to_pair)

    def convert(where):
        out_ref[where] = gather_buf[where].astype(jnp.bfloat16)

    def mirrored(slot):
        return (0, 2, 1, 3)[slot]

    todo = []

    def drain(limit):
        while len(todo) > limit:
            h, first, second = todo.pop(0)
            pairs[(h, first, second)].wait_recv()
            convert(spot(h, mirrored(first), mirrored(second), 1 - core))

    def have(h, first, second):
        pair_forward(h, first, second)
        convert(spot(h, first, second))
        todo.append((h, first, second))
        drain(4)

    for h in range(2):
        y_b[h].wait_recv()
        part = proj_buf[3, h] + y_buf[1, h]
        y_a[h].wait_recv()
        gather_buf[spot(h, 0, 0)] = part + y_buf[2, h]
        ring_send(h, 0, 0, 1, 0)
        ring_send(h, 0, 0, 2, 0)
        pair_forward(h, 0, 0)
    for h in range(2):
        ring_send(h, 0, 0, 1, 1)
        ring_send(h, 0, 0, 2, 1)
        convert(spot(h, 0, 0))
        todo.append((h, 0, 0))

    def arrived(h, first, second):
        if second == 0:
            gathers[(h, 0, 0, first)].wait_recv()
            if first == 1:
                ring_send(h, 1, 0, 3, 0)
            ring_send(h, first, 0, 1, 1)
            ring_send(h, first, 0, 2, 1)
        else:
            gathers[(h, 1, first, second)].wait_recv()
            if second == 1:
                ring_send(h, first, 1, 3, 1)
        have(h, first, second)

    order = [(1, 0), (2, 0), (0, 1), (0, 2), (1, 1), (3, 0), (1, 2), (2, 1), (0, 3), (2, 2), (3, 1), (1, 3), (3, 2), (2, 3), (3, 3)]
    for first, second in order:
        for h in range(2):
            arrived(h, first, second)
    drain(0)
    for copy in sends:
        copy.wait_send()


def store_kernel(lens_ref, y_ref, kv_ref, cache_ref, y_out_ref, cache_buf, k_out_ref, v_out_ref, y_sem, out_sem):
    k_buf, v_buf = cache_buf.at[0], cache_buf.at[1]
    batch, pos_local, hd = k_buf.shape
    first_pos = lax.axis_index("sq") * pos_local
    row = lax.broadcasted_iota(jnp.int32, (16, hd), 0)
    pairs = ((k_buf, k_out_ref), (v_buf, v_out_ref))

    def write(c):
        at = pl.ds(pl.multiple_of(c * STORE_SEQS, STORE_SEQS), STORE_SEQS)
        return [pltpu.make_async_copy(buf.at[at], out.at[at], out_sem.at[w, c]) for w, (buf, out) in enumerate(pairs)]

    def replace(c, _):
        for i in range(STORE_SEQS):
            b = c * STORE_SEQS + i
            pos = lens_ref[b] - first_pos
            base = pl.multiple_of(lax.div(jnp.clip(pos, 0, pos_local - 1), 16) * 16, 16)
            here = row + base == pos
            for which, (buf, _) in enumerate(pairs):
                old = buf[b, pl.ds(base, 16), :].astype(jnp.float32)
                new = kv_ref[which, pl.ds(b, 1), :]
                buf[b, pl.ds(base, 16), :] = jnp.where(here, new, old).astype(jnp.bfloat16)
        for copy in write(c):
            copy.start()
        return 0

    def drain(c, _):
        for copy in write(c):
            copy.wait()
        return 0

    y_copy = pltpu.make_async_copy(y_ref, y_out_ref, y_sem)
    y_copy.start()
    lax.fori_loop(0, batch // STORE_SEQS, replace, 0)
    lax.fori_loop(0, batch // STORE_SEQS, drain, 0)
    y_copy.wait()


def solution(mesh):
    nx, ny = mesh.shape["sq"] // 2, mesh.shape["tp"]

    def local_step(hidden, cache_lens, k_cache, v_cache, ln_gain, ln_bias, w_query, b_query, w_kv, b_kv, w_out, b_out):
        batch, pos_local, hd = k_cache.shape
        d_model, depth = w_query.shape
        heads = depth // hd
        rows, cols = batch // (2 * nx), d_model // ny
        width = depth + hd
        half = cols // 2
        f32, bf16, dma, vmem_buf = jnp.float32, jnp.bfloat16, pltpu.SemaphoreType.DMA, pltpu.VMEM
        smem, vmem, hbm = (pl.BlockSpec(memory_space=m) for m in (pltpu.SMEM, pltpu.VMEM, pl.ANY))
        out_hidden, key_val, caches = pl.pallas_call(
            functools.partial(decode_kernel, (nx, ny, heads, rows, cols, pos_local)),
            out_shape=[
                vmem_buf((batch, d_model), bf16),
                vmem_buf((2, batch, hd), f32),
                vmem_buf((2,) + k_cache.shape, bf16),
            ],
            in_specs=[smem] + [vmem] * 5 + [hbm] * 6,
            out_specs=[vmem] * 3,
            scratch_shapes=[
                vmem_buf((W_SLOTS * TALL, depth), bf16),
                vmem_buf((W_SLOTS, TALL, 2 * hd), bf16),
                vmem_buf((batch * 16, hd), f32),
                vmem_buf((batch, width), f32),
                vmem_buf((SEQS * 16, hd), f32),
                vmem_buf((SEQS * 16, pos_local), f32),
                vmem_buf((SEQS * 16, pos_local), f32),
                vmem_buf((batch, hd), f32),
                vmem_buf((batch, hd), f32),
                vmem_buf((4, rows, width), f32),
                vmem_buf((3, rows, width), f32),
                vmem_buf((rows, depth), bf16),
                vmem_buf((4, 2, rows, half), f32),
                vmem_buf((3, 2, rows, half), f32),
                vmem_buf((rows, cols), bf16),
                vmem_buf((batch, d_model), f32),
                dma((4,)),
                dma((2, d_model // TALL)),
                dma((2, batch // SEQS)),
                dma((4,)),
                dma,
                dma((4,)),
                dma((4,)),
                dma((3,)),
                dma((3,)),
                dma((3, 2)),
                dma((3, 2)),
                dma((2, 15)),
                dma((2, 15)),
                dma((2, 16)),
                dma((2, 16)),
            ],
            compiler_params=pltpu.CompilerParams(collective_id=0, has_side_effects=True, vmem_limit_bytes=28 * 1024 * 1024),
            name="decode",
        )(
            cache_lens,
            ln_gain.reshape(1, d_model),
            ln_bias.reshape(1, d_model),
            b_query,
            b_kv.reshape(1, 2 * hd),
            b_out.reshape(1, d_model),
            hidden,
            w_query,
            w_kv,
            w_out,
            k_cache,
            v_cache,
        )
        out_hidden, _, key_new, val_new = pl.pallas_call(
            store_kernel,
            out_shape=[
                jax.ShapeDtypeStruct((batch, d_model), bf16),
                vmem_buf((2,) + k_cache.shape, bf16),
                jax.ShapeDtypeStruct(k_cache.shape, bf16),
                jax.ShapeDtypeStruct(v_cache.shape, bf16),
            ],
            in_specs=[smem] + [vmem] * 3,
            out_specs=[hbm, vmem, hbm, hbm],
            input_output_aliases={3: 1},
            scratch_shapes=[dma, dma((2, batch // STORE_SEQS))],
            compiler_params=pltpu.CompilerParams(vmem_limit_bytes=1 * 1024 * 1024),
            name="store",
        )(cache_lens, out_hidden, key_val, caches)
        return out_hidden, key_new, val_new

    cache_spec = P("dp", "sq", None)
    row_spec = P("dp", None)
    in_specs = (row_spec, P("dp"), cache_spec, cache_spec, P(None), P(None), P(None, "tp"), P("tp"), P(None, None), P(None), P("tp", None), P(None))
    out_specs = (row_spec, cache_spec, cache_spec)
    return jax.shard_map(local_step, mesh=mesh, in_specs=in_specs, out_specs=out_specs, check_vma=False)
```

```python
import functools

import jax
import jax.numpy as jnp
from jax import lax
from jax.experimental import pallas as pl
from jax.experimental.pallas import tpu as pltpu
from jax.sharding import PartitionSpec as P

MESH = pl.DeviceIdType.MESH
LANES = 128
SEQS = 32
TALL = 768
WIDE = 512
STORE_SEQS = 16
EARLY = 3
W_SLOTS = 4


def merge_into(dst, part_a, part_b, heads):
    stat_a, stat_b = part_a(heads), part_b(heads)
    top = jnp.maximum(stat_a, stat_b)
    exp_a, exp_b = jnp.exp(stat_a - top), jnp.exp(stat_b - top)
    sums = stat_a * pltpu.roll(exp_a, 64, 1) + stat_b * pltpu.roll(exp_b, 64, 1)
    lane = lax.broadcasted_iota(jnp.int32, top.shape, 1)
    stat = jnp.where(lane < 64, top, sums)
    for n in range(heads):
        dst[:, n * LANES : (n + 1) * LANES] = part_a(n) * exp_a[:, n : n + 1] + part_b(n) * exp_b[:, n : n + 1]
    dst[:, heads * LANES :] = stat


def decode_kernel(
    dims,
    lens_ref,
    gain_ref,
    bias_ref,
    b_query_ref,
    b_kv_ref,
    b_out_ref,
    hidden_ref,
    w_query_ref,
    w_kv_ref,
    w_out_ref,
    k_ref,
    v_ref,
    out_ref,
    kv_buf,
    cache_buf,
    w_buf,
    wkv_buf,
    q_buf,
    part_buf,
    o_buf,
    s_buf0,
    s_buf1,
    stat_buf,
    stat_buf2,
    pair_buf,
    x_buf,
    att_buf,
    proj_buf,
    y_buf,
    hid_buf,
    gather_buf,
    h_sem,
    w_sem,
    in_sem,
    wo_sem,
    hid_sem,
    pair_send,
    pair_recv,
    x_send,
    x_recv,
    y_send,
    y_recv,
    g_send,
    g_recv,
    d_send,
    d_recv,
):
    nx, ny, heads, rows, cols, pos_local = dims
    k_buf, v_buf = cache_buf.at[0], cache_buf.at[1]
    batch, d_model = out_ref.shape
    hd, seqs = LANES, SEQS
    half = cols // 2
    depth = heads * hd
    steps = batch // seqs
    blocks = d_model // TALL
    sq = lax.axis_index("sq")
    y = lax.axis_index("tp")
    x = sq // 2
    core = sq % 2
    step = 1 - 2 * core
    first_pos = sq * pos_local
    scale = hd ** -0.5
    lowest = float(jnp.finfo(jnp.float32).min)

    def wrap(value, size):
        return lax.rem(value + 2 * size, size)

    x_fwd, x_bwd, x_opp = wrap(x + step, nx), wrap(x - step, nx), wrap(x + 2, nx)
    y_fwd, y_bwd, y_opp = wrap(y + step, ny), wrap(y - step, ny), wrap(y + 2, ny)
    to_pair = {"sq": x * 2 + 1 - core}
    to_x_fwd, to_x_bwd = {"sq": x_fwd * 2 + core}, {"sq": x_bwd * 2 + core}
    to_y_fwd, to_y_bwd = {"tp": y_fwd}, {"tp": y_bwd}

    barrier = pltpu.get_barrier_semaphore()
    for peer in (to_pair, to_x_fwd, to_x_bwd, to_y_fwd, to_y_bwd):
        pl.semaphore_signal(barrier, inc=1, device_id=peer, device_id_type=MESH)

    h_buf = out_ref

    def w_copies(k):
        slot, at = k % W_SLOTS, pl.ds(k * TALL, TALL)
        return (
            pltpu.make_async_copy(w_query_ref.at[at, :], w_buf.at[pl.ds(slot * TALL, TALL), :], w_sem.at[0, k]),
            pltpu.make_async_copy(w_kv_ref.at[at, :], wkv_buf.at[slot], w_sem.at[1, k]),
        )

    def block_row(i):
        slot, mine = i // 2, i % 2
        sign = step * (1 - 2 * mine)
        shift = 2 * ((3 - slot) // 3) + sign * (slot * (3 - slot) * (3 - 2 * slot) // 2)
        owner = wrap(x + shift, nx) * 2 + (1 - core) * (1 - mine) + core * mine
        return owner * rows

    def step_rows(c):
        per = rows // seqs
        return pl.multiple_of(block_row(c // per) + (c % per) * seqs, seqs)

    def read(c):
        at = pl.ds(step_rows(c), seqs)
        return (
            pltpu.make_async_copy(k_ref.at[at], k_buf.at[at], in_sem.at[0, c]),
            pltpu.make_async_copy(v_ref.at[at], v_buf.at[at], in_sem.at[1, c]),
        )

    h_parts = 4
    h_rows = batch // h_parts
    h_copies = [
        pltpu.make_async_copy(hidden_ref.at[pl.ds(j * h_rows, h_rows), :], h_buf.at[pl.ds(j * h_rows, h_rows), :], h_sem.at[j])
        for j in range(h_parts)
    ]
    for copy in h_copies:
        copy.start()

    def start_weights(k, _):
        for copy in w_copies(k):
            copy.start()
        return 0

    def start_caches(c, _):
        for copy in read(c):
            copy.start()
        return 0

    lax.fori_loop(0, W_SLOTS, start_weights, 0)
    lax.fori_loop(0, EARLY, start_caches, 0)
    q_buf[...] = jnp.zeros_like(q_buf)

    tiles = d_model // hd

    def lane_tiles(at):
        return [h_buf[at, t * hd : (t + 1) * hd].astype(jnp.float32) for t in range(tiles)]

    def add_up(values):
        while len(values) > 1:
            values = [sum(values[i : i + 2]) for i in range(0, len(values), 2)]
        return values[0]

    def rows16(r):
        return pl.ds(pl.multiple_of(r * 16, 16), 16)

    def sum_rows(r, _):
        stat_buf[rows16(r), :] = add_up(lane_tiles(rows16(r)))
        return 0

    def spread_rows(r, _):
        mean_val = stat_buf[rows16(r), :]
        stat_buf2[rows16(r), :] = add_up([(v - mean_val) * (v - mean_val) for v in lane_tiles(rows16(r))])
        return 0

    def norm_rows(r, _):
        at = rows16(r)
        mean_val, inv = stat_buf[at, :], stat_buf2[at, :]
        for t in range(tiles):
            cols = slice(t * hd, (t + 1) * hd)
            normed = (h_buf[at, cols].astype(jnp.float32) - mean_val) * inv
            h_buf[at, cols] = (normed * gain_ref[:, cols] + bias_ref[:, cols]).astype(jnp.bfloat16)
        return 0

    def row_means(buf):
        return jnp.broadcast_to(jnp.sum(buf[...], axis=-1, keepdims=True) * (1.0 / d_model), buf.shape)

    for j, copy in enumerate(h_copies):
        copy.wait()
        lax.fori_loop(j * h_rows // 16, (j + 1) * h_rows // 16, sum_rows, 0, unroll=2)
    stat_buf[...] = row_means(stat_buf)
    lax.fori_loop(0, batch // 16, spread_rows, 0, unroll=2)
    stat_buf2[...] = lax.rsqrt(row_means(stat_buf2) + 1e-5)
    lax.fori_loop(0, batch // 16, norm_rows, 0, unroll=2)

    y_order = (y_opp, y_bwd, y_fwd, y)

    def wo_copy(k):
        src = w_out_ref.at[:, pl.ds(pl.multiple_of(y_order[k] * cols, cols), cols)]
        return pltpu.make_async_copy(src, w_buf.at[pl.ds((k % 2) * depth, depth), :], wo_sem.at[k])

    for k in range(blocks):
        for copy in w_copies(k):
            copy.wait()
        h_cols, slot = h_buf[:, k * TALL : (k + 1) * TALL], k % W_SLOTS
        kv = jnp.dot(h_cols, wkv_buf[slot], preferred_element_type=jnp.float32)
        for e in range(2):
            part = kv[:, e * hd : (e + 1) * hd]
            kv_buf[e] = part if k == 0 else kv_buf[e] + part
        for n in range(0, depth, WIDE):
            w_block = w_buf[slot * TALL : (slot + 1) * TALL, n : n + WIDE]
            part = jnp.dot(h_cols, w_block, preferred_element_type=jnp.float32)
            part_buf[:, n : n + WIDE] = part if k == 0 else part_buf[:, n : n + WIDE] + part
        if k + W_SLOTS < blocks:
            for copy in w_copies(k + W_SLOTS):
                copy.start()
        if k + W_SLOTS == blocks - 1:
            lax.fori_loop(EARLY, steps, start_caches, 0)
    for e in range(2):
        new = kv_buf[e] + b_kv_ref[:, e * hd : (e + 1) * hd]
        kv_buf[e] = new.astype(jnp.bfloat16).astype(jnp.float32)
    for n in range(heads):
        new = part_buf[:, n * hd : (n + 1) * hd] + b_query_ref[n * hd : (n + 1) * hd].reshape(1, hd)
        q_buf[pl.ds(n, batch, stride=16), :] = new.astype(jnp.bfloat16).astype(jnp.float32)
    hid_copy = pltpu.make_async_copy(
        hidden_ref.at[pl.ds(pl.multiple_of(sq * rows, rows), rows), pl.ds(pl.multiple_of(y * cols, cols), cols)], hid_buf, hid_sem
    )
    hid_copy.start()
    for k in range(2):
        wo_copy(k).start()

    zero = jnp.zeros((16, hd), jnp.bfloat16)
    at_pos = lax.broadcasted_iota(jnp.int32, (16, pos_local), 1) + first_pos
    row = lax.broadcasted_iota(jnp.int32, (16, hd), 0)
    lane = lax.broadcasted_iota(jnp.int32, (16, hd), 1)
    pick_m = (lane == row) & (row < heads)
    pick_l = (lane == row + 64) & (row < heads)

    def score(c, s_buf):
        for copy in read(c):
            copy.wait()
        b0 = step_rows(c)
        for i in range(0, seqs, 2):
            q0 = q_buf[pl.ds(pl.multiple_of(b0 * 16 + i * 16, 16), 16), :].astype(jnp.bfloat16)
            q1 = q_buf[pl.ds(pl.multiple_of(b0 * 16 + i * 16 + 16, 16), 16), :].astype(jnp.bfloat16)
            q2 = jnp.concatenate([jnp.concatenate([q0, zero], axis=1), jnp.concatenate([zero, q1], axis=1)], axis=0)
            k2 = jnp.concatenate([k_buf[b0 + i], k_buf[b0 + i + 1]], axis=1)
            s2 = lax.dot_general(q2, k2, (((1,), (1,)), ((), ())), preferred_element_type=jnp.float32)
            s_buf[i * 16 : i * 16 + 32, :] = s2 * scale

    def combine(c, s_buf):
        b0 = step_rows(c)
        for i in range(0, seqs, 2):
            v2 = jnp.concatenate([v_buf[b0 + i], v_buf[b0 + i + 1]], axis=1)
            valid = jnp.concatenate([at_pos < lens_ref[b0 + i], at_pos < lens_ref[b0 + i + 1]], axis=0)
            s2 = jnp.where(valid, s_buf[i * 16 : i * 16 + 32, :], lowest)
            top = jnp.max(s2, axis=-1, keepdims=True)
            p2 = jnp.where(valid, jnp.exp(s2 - top), 0.0)
            total = jnp.sum(p2, axis=-1, keepdims=True)
            o2 = jnp.dot(p2.astype(jnp.bfloat16), v2, preferred_element_type=jnp.float32)
            for e in range(2):
                part = slice(e * 16, e * 16 + 16)
                stat = jnp.where(pick_m, top[part], 0.0) + jnp.where(pick_l, total[part], 0.0)
                stat = jnp.sum(stat, axis=0, keepdims=True)
                o_buf[(i + e) * 16 : (i + e) * 16 + 16, :] = jnp.where(row == heads, stat, o2[part, e * hd : (e + 1) * hd])
        for n in range(heads + 1):
            part_buf[pl.ds(b0, seqs), n * hd : (n + 1) * hd] = o_buf[pl.ds(n, seqs, stride=16), :]

    sends = []

    def remote(src, dst, ssem, rsem, peer):
        return pltpu.make_async_remote_copy(
            src_ref=src, dst_ref=dst, send_sem=ssem, recv_sem=rsem, device_id=peer, device_id_type=MESH
        )

    def send(*args):
        copy = remote(*args)
        copy.start()
        sends.append(copy)
        return copy

    def part_at(i):
        return pl.ds(pl.multiple_of(block_row(i), rows), rows)

    def of_part(i):
        return lambda n: part_buf[part_at(i), n * hd : (n + 1) * hd]

    def of(ref):
        return lambda n: ref[:, n * hd : (n + 1) * hd]

    pair = [remote(part_buf.at[part_at(2 * k), :], pair_buf.at[k], pair_send.at[k], pair_recv.at[k], to_pair) for k in range(4)]
    x_o = remote(pair_buf.at[0], x_buf.at[0], x_send.at[0], x_recv.at[0], to_x_fwd)
    x_b = remote(pair_buf.at[1], x_buf.at[1], x_send.at[1], x_recv.at[1], to_x_bwd)
    x_a = remote(pair_buf.at[2], x_buf.at[2], x_send.at[2], x_recv.at[2], to_x_fwd)
    sends.extend(pair + [x_o, x_b, x_a])

    def after_block(i):
        slot = i // 2
        if i % 2 == 0:
            pair[slot].start()
            return
        pair[slot].wait_recv()
        merge_into(pair_buf.at[slot], of_part(i), of(pair_buf.at[slot]), heads)
        if slot == 0:
            x_o.start()
        elif slot == 1:
            x_b.start()
        elif slot == 2:
            x_o.wait_recv()
            merge_into(pair_buf.at[2], of(pair_buf.at[2]), of(x_buf.at[0]), heads)
            x_a.start()

    pl.semaphore_wait(barrier, 5)
    score(0, s_buf0)

    def two_blocks(t, _):
        c = t * 2
        score(c + 1, s_buf1)
        combine(c, s_buf0)
        for j in range(3):
            pl.when(t == j)(functools.partial(after_block, 2 * j))
        score(c + 2, s_buf0)
        combine(c + 1, s_buf1)
        for j in range(3):
            pl.when(t == j)(functools.partial(after_block, 2 * j + 1))
        return 0

    lax.fori_loop(0, steps // 2 - 1, two_blocks, 0)
    score(steps - 1, s_buf1)
    combine(steps - 2, s_buf0)
    after_block(6)
    combine(steps - 1, s_buf1)

    own = pl.multiple_of(sq * rows, rows)
    k_new, v_new = kv_buf[0, pl.ds(own, rows), :], kv_buf[1, pl.ds(own, rows), :]
    new_lane = lax.broadcasted_iota(jnp.int32, (rows, hd), 1)
    new_stat = jnp.where((new_lane >= 64) & (new_lane < 64 + heads), 1.0, 0.0)
    for n in range(heads):
        s_new = jnp.sum(q_buf[pl.ds(own * 16 + n, rows, stride=16), :] * k_new, axis=-1, keepdims=True) * scale
        new_stat = jnp.where(new_lane == n, s_new, new_stat)

    after_block(7)
    total = pair_buf.at[3]
    merge_into(total, of(total), lambda n: new_stat if n == heads else v_new, heads)
    x_b.wait_recv()
    merge_into(total, of(total), of(x_buf.at[1]), heads)
    x_a.wait_recv()
    merge_into(total, of(total), of(x_buf.at[2]), heads)
    stat = total[:, depth:]
    for n in range(heads):
        block = slice(n * hd, (n + 1) * hd)
        att_buf[:, block] = (total[:, block] / stat[:, 64 + n : 65 + n]).astype(jnp.bfloat16)

    def project(k, h):
        w_block = w_buf[(k % 2) * depth : (k % 2 + 1) * depth, h * half : (h + 1) * half]
        return jnp.dot(att_buf[...], w_block, preferred_element_type=jnp.float32)

    y_o, y_b, y_a = [None, None], [None, None], [None, None]
    for k in range(4):
        wo_copy(k).wait()
        for h in range(2):
            part = project(k, h)
            if k < 2:
                proj_buf[k, h] = part
                copy = send(proj_buf.at[k, h], y_buf.at[k, h], y_send.at[k, h], y_recv.at[k, h], (to_y_fwd, to_y_bwd)[k])
                (y_o, y_b)[k][h] = copy
            elif k == 2:
                proj_buf[2, h] = part
            else:
                if h == 0:
                    hid_copy.wait()
                own_cols = pl.ds(pl.multiple_of(y * cols + h * half, half), half)
                proj_buf[3, h] = part + hid_buf[:, h * half : (h + 1) * half].astype(jnp.float32) + b_out_ref[:, own_cols]
        if k < 2:
            wo_copy(k + 2).start()
        if k == 2:
            for h in range(2):
                y_o[h].wait_recv()
                proj_buf[2, h] = proj_buf[2, h] + y_buf[0, h]
                y_a[h] = send(proj_buf.at[2, h], y_buf.at[2, h], y_send.at[2, h], y_recv.at[2, h], to_y_fwd)

    def place(xt, yt, ct, h):
        row = pl.multiple_of((xt * 2 + ct) * rows, rows)
        col = pl.multiple_of(yt * cols + h * half, half)
        return pl.ds(row, rows), pl.ds(col, half)

    xs = (x, x_bwd, x_fwd, x_opp)
    ys = (y, y_bwd, y_fwd, y_opp)
    x_peers, y_peers = (to_x_fwd, to_x_bwd), (to_y_fwd, to_y_bwd)
    gathers = {}
    pairs = {}

    def spot(h, first, second, ct=None):
        ct = core if ct is None else ct
        if h == 0:
            return place(xs[first], ys[second], ct, h)
        return place(xs[second], ys[first], ct, h)

    def piece(h, first, second):
        return gather_buf.at[spot(h, first, second)]

    def ring_send(h, first, second, slot, phase):
        peers = (x_peers, y_peers) if h == 0 else (y_peers, x_peers)
        peer = peers[phase][1 if slot == 2 else 0]
        index = slot - 1 if phase == 0 else 3 + first * 3 + slot - 1
        key = (h, phase, first if phase else 0, slot)
        ref = piece(h, first, second)
        gathers[key] = send(ref, ref, g_send.at[h, index], g_recv.at[h, index], peer)

    def pair_forward(h, first, second):
        ref = piece(h, first, second)
        index = first * 4 + second
        pairs[(h, first, second)] = send(ref, ref, d_send.at[h, index], d_recv.at[h, index], to_pair)

    def convert(where):
        out_ref[where] = gather_buf[where].astype(jnp.bfloat16)

    def mirrored(slot):
        return (0, 2, 1, 3)[slot]

    todo = []

    def drain(limit):
        while len(todo) > limit:
            h, first, second = todo.pop(0)
            pairs[(h, first, second)].wait_recv()
            convert(spot(h, mirrored(first), mirrored(second), 1 - core))

    def have(h, first, second):
        pair_forward(h, first, second)
        convert(spot(h, first, second))
        todo.append((h, first, second))
        drain(6)

    for h in range(2):
        y_b[h].wait_recv()
        part = proj_buf[3, h] + y_buf[1, h]
        y_a[h].wait_recv()
        gather_buf[spot(h, 0, 0)] = part + y_buf[2, h]
        ring_send(h, 0, 0, 1, 0)
        ring_send(h, 0, 0, 2, 0)
        pair_forward(h, 0, 0)
    for h in range(2):
        ring_send(h, 0, 0, 1, 1)
        ring_send(h, 0, 0, 2, 1)
        convert(spot(h, 0, 0))
        todo.append((h, 0, 0))

    def arrived(h, first, second):
        if second == 0:
            gathers[(h, 0, 0, first)].wait_recv()
            if first == 1:
                ring_send(h, 1, 0, 3, 0)
            ring_send(h, first, 0, 1, 1)
            ring_send(h, first, 0, 2, 1)
        else:
            gathers[(h, 1, first, second)].wait_recv()
            if second == 1:
                ring_send(h, first, 1, 3, 1)
        have(h, first, second)

    order = [(1, 0), (2, 0), (0, 1), (0, 2), (1, 1), (3, 0), (1, 2), (2, 1), (0, 3), (2, 2), (3, 1), (1, 3), (3, 2), (2, 3), (3, 3)]
    for first, second in order:
        for h in range(2):
            arrived(h, first, second)
    drain(0)
    for copy in sends:
        copy.wait_send()


def store_kernel(lens_ref, y_ref, kv_ref, cache_ref, y_out_ref, cache_buf, k_out_ref, v_out_ref, y_sem, out_sem):
    k_buf, v_buf = cache_buf.at[0], cache_buf.at[1]
    batch, pos_local, hd = k_buf.shape
    first_pos = lax.axis_index("sq") * pos_local
    row = lax.broadcasted_iota(jnp.int32, (16, hd), 0)
    pairs = ((k_buf, k_out_ref), (v_buf, v_out_ref))

    def write(c):
        at = pl.ds(pl.multiple_of(c * STORE_SEQS, STORE_SEQS), STORE_SEQS)
        return [pltpu.make_async_copy(buf.at[at], out.at[at], out_sem.at[w, c]) for w, (buf, out) in enumerate(pairs)]

    def replace(c, _):
        for i in range(STORE_SEQS):
            b = c * STORE_SEQS + i
            pos = lens_ref[b] - first_pos
            base = pl.multiple_of(lax.div(jnp.clip(pos, 0, pos_local - 1), 16) * 16, 16)
            here = row + base == pos
            for which, (buf, _) in enumerate(pairs):
                old = buf[b, pl.ds(base, 16), :].astype(jnp.float32)
                new = kv_ref[which, pl.ds(b, 1), :]
                buf[b, pl.ds(base, 16), :] = jnp.where(here, new, old).astype(jnp.bfloat16)
        for copy in write(c):
            copy.start()
        return 0

    def drain(c, _):
        for copy in write(c):
            copy.wait()
        return 0

    y_copy = pltpu.make_async_copy(y_ref, y_out_ref, y_sem)
    y_copy.start()
    lax.fori_loop(0, batch // STORE_SEQS, replace, 0)
    lax.fori_loop(0, batch // STORE_SEQS, drain, 0)
    y_copy.wait()


def solution(mesh):
    nx, ny = mesh.shape["sq"] // 2, mesh.shape["tp"]

    def local_step(hidden, cache_lens, k_cache, v_cache, ln_gain, ln_bias, w_query, b_query, w_kv, b_kv, w_out, b_out):
        batch, pos_local, hd = k_cache.shape
        d_model, depth = w_query.shape
        heads = depth // hd
        rows, cols = batch // (2 * nx), d_model // ny
        width = depth + hd
        half = cols // 2
        f32, bf16, dma, vmem_buf = jnp.float32, jnp.bfloat16, pltpu.SemaphoreType.DMA, pltpu.VMEM
        smem, vmem, hbm = (pl.BlockSpec(memory_space=m) for m in (pltpu.SMEM, pltpu.VMEM, pl.ANY))
        out_hidden, key_val, caches = pl.pallas_call(
            functools.partial(decode_kernel, (nx, ny, heads, rows, cols, pos_local)),
            out_shape=[
                vmem_buf((batch, d_model), bf16),
                vmem_buf((2, batch, hd), f32),
                vmem_buf((2,) + k_cache.shape, bf16),
            ],
            in_specs=[smem] + [vmem] * 5 + [hbm] * 6,
            out_specs=[vmem] * 3,
            scratch_shapes=[
                vmem_buf((W_SLOTS * TALL, depth), bf16),
                vmem_buf((W_SLOTS, TALL, 2 * hd), bf16),
                vmem_buf((batch * 16, hd), f32),
                vmem_buf((batch, width), f32),
                vmem_buf((SEQS * 16, hd), f32),
                vmem_buf((SEQS * 16, pos_local), f32),
                vmem_buf((SEQS * 16, pos_local), f32),
                vmem_buf((batch, hd), f32),
                vmem_buf((batch, hd), f32),
                vmem_buf((4, rows, width), f32),
                vmem_buf((3, rows, width), f32),
                vmem_buf((rows, depth), bf16),
                vmem_buf((4, 2, rows, half), f32),
                vmem_buf((3, 2, rows, half), f32),
                vmem_buf((rows, cols), bf16),
                vmem_buf((batch, d_model), f32),
                dma((4,)),
                dma((2, d_model // TALL)),
                dma((2, batch // SEQS)),
                dma((4,)),
                dma,
                dma((4,)),
                dma((4,)),
                dma((3,)),
                dma((3,)),
                dma((3, 2)),
                dma((3, 2)),
                dma((2, 15)),
                dma((2, 15)),
                dma((2, 16)),
                dma((2, 16)),
            ],
            compiler_params=pltpu.CompilerParams(collective_id=0, has_side_effects=True, vmem_limit_bytes=28 * 1024 * 1024),
            name="decode",
        )(
            cache_lens,
            ln_gain.reshape(1, d_model),
            ln_bias.reshape(1, d_model),
            b_query,
            b_kv.reshape(1, 2 * hd),
            b_out.reshape(1, d_model),
            hidden,
            w_query,
            w_kv,
            w_out,
            k_cache,
            v_cache,
        )
        out_hidden, _, key_new, val_new = pl.pallas_call(
            store_kernel,
            out_shape=[
                jax.ShapeDtypeStruct((batch, d_model), bf16),
                vmem_buf((2,) + k_cache.shape, bf16),
                jax.ShapeDtypeStruct(k_cache.shape, bf16),
                jax.ShapeDtypeStruct(v_cache.shape, bf16),
            ],
            in_specs=[smem] + [vmem] * 3,
            out_specs=[hbm, vmem, hbm, hbm],
            input_output_aliases={3: 1},
            scratch_shapes=[dma, dma((2, batch // STORE_SEQS))],
            compiler_params=pltpu.CompilerParams(vmem_limit_bytes=1 * 1024 * 1024),
            name="store",
        )(cache_lens, out_hidden, key_val, caches)
        return out_hidden, key_new, val_new

    cache_spec = P("dp", "sq", None)
    row_spec = P("dp", None)
    in_specs = (row_spec, P("dp"), cache_spec, cache_spec, P(None), P(None), P(None, "tp"), P("tp"), P(None, None), P(None), P("tp", None), P(None))
    out_specs = (row_spec, cache_spec, cache_spec)
    return jax.shard_map(local_step, mesh=mesh, in_specs=in_specs, out_specs=out_specs, check_vma=False)
```
